32 devices in a mesh: seq: 8 (over y, x, core), head: 4 (over z).
Axes of the slice: x: 2, y: 2, z: 4, core: 2. Of those that a mesh axis runs over, the one named last changes fastest.
Arguments:
- query: bfloat16 [2, 1024, 4096], P(None, 'seq', 'head'), may hold values from -5 to 5
- keys: bfloat16 [2, 1024, 1024], P(None, 'seq', 'head'), may hold values from -5 to 5
- values: bfloat16 [2, 1024, 1024], P(None, 'seq', 'head'), may hold values from -12 to 12
- norm_gain: float32 [4096], P('head'), may hold values from 0.25 to 1.75
- in_b: bfloat16 [2048, 128], P('seq'), may hold values from -0.25 to 0.25
- out_c: bfloat16 [2048, 128], P('seq'), may hold values from -0.25 to 0.25
- step: float32 [64, 2048], P('head', 'seq'), may hold values from 0.2 to 1
- log_decay: float32 [64, 2048], P('head', 'seq'), may hold values from -2 to 0
- skip: float32 [64], P('head'), may hold values from 0.5 to 1.5
Outputs:
- mixed: bfloat16 [2048, 4096], P('seq', 'head')
The draws below stay inside these ranges and needn't reach their ends.
All inputs are finite; a program needn't handle non-finite values.
Results may differ from the reference program's by a relative error of at most 0.012.
Values may be sent and summed in bfloat16 or wider, within the bound.
No kernel may reach another device: no remote copies, remote signals or barrier semaphores. Data moves between devices by JAX's collectives and lax.ppermute only.
A program may use at most 128 MiB of HBM per device.

```python
import math
import jax
import jax.numpy as jnp
from jax import lax

HEADS = 32
KVH = 8
HDIM = 128
SHEADS = 64
SDIM = 64
STATE = 128
SPAN = 256
TOKEN_COUNT = 2048
BLK = 128
WIN = 256


def qk_pair(key):
    baseline_rate = jax.random.fold_in(key, 11)
    key_query, key_keys = jax.random.split(baseline_rate, 2)
    queries = jnp.clip(jax.random.normal(key_query, (TOKEN_COUNT, HEADS * HDIM), jnp.float32), -4.0, 4.0)
    keyvals = jnp.clip(jax.random.normal(key_keys, (TOKEN_COUNT, KVH * HDIM), jnp.float32), -4.0, 4.0)
    queries = queries.reshape(2, TOKEN_COUNT // 2, HEADS * HDIM).astype(jnp.bfloat16)
    keyvals = keyvals.reshape(2, TOKEN_COUNT // 2, KVH * HDIM).astype(jnp.bfloat16)
    return (queries, keyvals)


def draw_query(key, part):
    return qk_pair(key)[0]


def draw_keys(key, part):
    return qk_pair(key)[1]


def draw_values(key, part):
    baseline_rate = jax.random.fold_in(key, 23)
    head_scale = 3.0 ** (jnp.arange(KVH, dtype=jnp.float32) / (KVH - 1))
    raw_values = jnp.clip(jax.random.normal(baseline_rate, (TOKEN_COUNT, KVH, HDIM), jnp.float32), -4.0, 4.0)
    scaled = raw_values * head_scale[None, :, None]
    return scaled.reshape(2, TOKEN_COUNT // 2, KVH * HDIM).astype(jnp.bfloat16)


def draw_log_decay(key, part):
    baseline_rate = jax.random.fold_in(key, 31)
    gradual_key, rate_key, quick_key, noise_key, spike_key, depth_key = jax.random.split(baseline_rate, 6)
    slow_share = 0.5
    slow_heads = jax.random.bernoulli(gradual_key, slow_share, (SHEADS,))
    slow_rate = jnp.exp(jax.random.uniform(rate_key, (SHEADS,), jnp.float32, jnp.log(0.1), jnp.log(0.6))) / TOKEN_COUNT
    fast_rate = jax.random.uniform(quick_key, (SHEADS,), jnp.float32, 1.0 / 50.0, 1.0 / 30.0)
    decay_speeds = jnp.where(slow_heads, slow_rate, fast_rate)
    random_noise = jnp.exp(jax.random.uniform(noise_key, (SHEADS, TOKEN_COUNT), jnp.float32, jnp.log(0.5), jnp.log(2.0)))
    spike_position = jax.random.randint(spike_key, (3,), 0, TOKEN_COUNT)
    spike_depth = jax.random.uniform(depth_key, (3,), jnp.float32, 0.22, 0.5)
    token_location = jnp.arange(TOKEN_COUNT)
    spike_events = jnp.sum(jnp.where(token_location[None, :] == spike_position[:, None], spike_depth[:, None], 0.0), axis=0)
    return -(decay_speeds[:, None] * random_noise + spike_events[None, :])


def block_levels(own_key, extent, cuts, least, largest):
    loudness = 1.0
    for dim, shards_of in cuts:
        heights = jax.random.uniform(jax.random.fold_in(jax.random.fold_in(own_key, 6), dim), (shards_of,), jnp.float32, least / len(cuts), largest / len(cuts))
        loudness = loudness * jnp.repeat(jnp.exp(heights), extent[dim] // shards_of).reshape((-1,) + (1,) * (len(extent) - 1 - dim))
    return loudness


def scatter_about(own_key, extent, spread, reach, cuts=(), kind=jnp.bfloat16):
    array = spread * jax.random.normal(own_key, extent, jnp.float32)
    if cuts:
        array = array * block_levels(own_key, extent, cuts, -0.22, 0.18)
    return jnp.clip(array, -reach, reach).astype(kind)


def setup_inputs(seed: int = 0) -> dict:
    key_list = jax.random.split(jax.random.key(seed), 10)
    query = draw_query(jax.random.fold_in(key_list[9], 71), 0)
    keys = draw_keys(jax.random.fold_in(key_list[9], 71), 0)
    values = draw_values(jax.random.fold_in(key_list[9], 71), 0)
    norm_gain = jnp.clip(1.0 + 0.15 * jax.random.normal(key_list[3], (HEADS * HDIM,), jnp.float32), 0.25, 1.75)
    in_b = scatter_about(key_list[4], (TOKEN_COUNT, STATE), 0.04, 0.25, ((0, 8),))
    out_c = scatter_about(key_list[5], (TOKEN_COUNT, STATE), 0.04, 0.25, ((0, 8),))
    step = jnp.clip(jnp.exp(math.log(1.0) - 1.609438 * jax.random.uniform(key_list[6], (SHEADS, TOKEN_COUNT), jnp.float32) ** block_levels(key_list[6], (SHEADS, TOKEN_COUNT), ((0, 4), (1, 8)), -0.2, 0.2)), 0.2, 1.0)
    log_decay = draw_log_decay(jax.random.fold_in(key_list[9], 71), 0)
    skip = jnp.clip(0.5 + 1.0 * jax.random.uniform(key_list[8], (SHEADS,), jnp.float32) ** block_levels(key_list[8], (SHEADS,), ((0, 4),), -0.2, 0.2), 0.5, 1.5)
    return {"query": query, "keys": keys, "values": values, "norm_gain": norm_gain, "in_b": in_b, "out_c": out_c, "step": step, "log_decay": log_decay, "skip": skip}


def attention_all(query, keys, values):
    group_size = HEADS // KVH
    queries = query.reshape(TOKEN_COUNT, KVH, group_size, HDIM)
    key_pad = jnp.concatenate([jnp.zeros((WIN, KVH, HDIM), jnp.bfloat16), keys.reshape(TOKEN_COUNT, KVH, HDIM)], 0)
    val_pad = jnp.concatenate([jnp.zeros((WIN, KVH, HDIM), jnp.bfloat16), values.reshape(TOKEN_COUNT, KVH, HDIM)], 0)
    score_scale = 1.0 / math.sqrt(HDIM)

    def attend_block(block_no):
        start = (block_no * BLK).astype(jnp.int32)
        query_rows = lax.dynamic_slice_in_dim(queries, start, BLK, 0).astype(jnp.float32)
        key_rows = lax.dynamic_slice_in_dim(key_pad, start, WIN + BLK, 0).astype(jnp.float32)
        val_rows = lax.dynamic_slice_in_dim(val_pad, start, WIN + BLK, 0).astype(jnp.float32)
        query_pos = start + jnp.arange(BLK, dtype=jnp.int32)
        key_pos = start - WIN + jnp.arange(WIN + BLK, dtype=jnp.int32)
        allowed = (key_pos[None, :] <= query_pos[:, None]) & (key_pos[None, :] > query_pos[:, None] - WIN) & (key_pos[None, :] >= 0)
        scores = jnp.einsum('qgjd,kgd->gjqk', query_rows, key_rows) * score_scale
        scores = jnp.where(allowed, scores, -jnp.inf)
        row_peak = lax.optimization_barrier(jnp.max(scores, axis=-1, keepdims=True))
        exp_terms = jnp.exp(scores - row_peak)
        row_total = lax.optimization_barrier(jnp.sum(exp_terms, axis=-1))
        weights = exp_terms.astype(jnp.bfloat16).astype(jnp.float32)
        result = jnp.einsum('gjqk,kgd->qgjd', weights, val_rows)
        result = result / jnp.transpose(row_total, (2, 0, 1))[..., None]
        return result.reshape(BLK, HEADS * HDIM).astype(jnp.bfloat16)
    blocks = lax.map(attend_block, jnp.arange(TOKEN_COUNT // BLK, dtype=jnp.int32))
    return blocks.reshape(TOKEN_COUNT, HEADS * HDIM)

def reference(query, keys, values, norm_gain, in_b, out_c, step, log_decay, skip):
    attended = attention_all(query, keys, values)
    widened = attended.astype(jnp.float32)
    meansq = lax.optimization_barrier(jnp.mean(widened * widened, axis=-1))
    normed = (widened * norm_gain[None, :] * lax.rsqrt(meansq + 1e-06)[:, None]).astype(jnp.bfloat16)
    span_count = TOKEN_COUNT // SPAN
    inputs = normed.astype(jnp.float32).reshape(span_count, SPAN, SHEADS, SDIM)
    in_rows = in_b.astype(jnp.float32).reshape(span_count, SPAN, STATE)
    out_rows = out_c.astype(jnp.float32).reshape(span_count, SPAN, STATE)
    step_rows = step.reshape(SHEADS, span_count, SPAN).transpose(1, 0, 2)
    decay_rows = log_decay.reshape(SHEADS, span_count, SPAN).transpose(1, 0, 2)
    causal = jnp.arange(SPAN)[:, None] >= jnp.arange(SPAN)[None, :]
    highest = lax.Precision.HIGHEST

    def advance(carried, pieces):
        x_rows, b_rows, c_rows, dt_rows, log_rows = pieces
        cum_log = jnp.cumsum(log_rows, axis=1)
        decay_mat = jnp.exp(jnp.where(causal[None], cum_log[:, :, None] - cum_log[:, None, :], -jnp.inf))
        cross_terms = jnp.dot(c_rows, b_rows.T, precision=highest)
        mixing = decay_mat * cross_terms[None] * dt_rows[:, None, :]
        mixing = mixing.astype(jnp.bfloat16).astype(jnp.float32)
        result = jnp.einsum('htu,uhe->the', mixing, x_rows, precision=highest)
        entry_term = jnp.einsum('tn,hen->the', c_rows, carried, precision=highest)
        result = result + entry_term * jnp.exp(cum_log).T[:, :, None]
        result = result + skip[None, :, None] * x_rows
        end_weights = jnp.exp(cum_log[:, -1:] - cum_log) * dt_rows
        weighted = end_weights.T[:, :, None] * x_rows
        carried = jnp.exp(cum_log[:, -1])[:, None, None] * carried + jnp.einsum('uhe,un->hen', weighted, b_rows, precision=highest)
        return (carried, result)
    initial = jnp.zeros((SHEADS, SDIM, STATE), jnp.float32)
    final_state, outputs = lax.scan(advance, initial, (inputs, in_rows, out_rows, step_rows, decay_rows))
    return outputs.reshape(TOKEN_COUNT, SHEADS * SDIM).astype(jnp.bfloat16)
```

```python
import functools
import math

import jax
import jax.numpy as jnp
from jax import lax
from jax.experimental import pallas as pl
from jax.experimental.pallas import tpu as pltpu
from jax.sharding import PartitionSpec as P


HEADS = 32
HDIM = 128
SDIM = 64
STATE = 128

F32 = jnp.float32
BF16 = jnp.bfloat16
VMEM = pltpu.VMEM
GRANT = 12 << 20


def dot(a, b, contract=(1, 0), precision=None):
    return lax.dot_general(
        a,
        b,
        (((contract[0],), (contract[1],)), ((), ())),
        precision=precision,
        preferred_element_type=F32,
    )


def call(kernel, outs, args, flops=1, spaces=None):
    spaces = spaces or [VMEM] * len(args)
    return pl.pallas_call(
        kernel,
        out_shape=[jax.ShapeDtypeStruct(s, d) for s, d in outs],
        in_specs=[pl.BlockSpec(memory_space=m) for m in spaces],
        out_specs=[pl.BlockSpec(memory_space=VMEM)] * len(outs),
        compiler_params=pltpu.CompilerParams(vmem_limit_bytes=GRANT),
        cost_estimate=pl.CostEstimate(flops=flops, bytes_accessed=1 << 20, transcendentals=0),
    )(*args)


def pack_kernel(k_ref, v_ref, out_ref):
    width = k_ref.shape[2]

    def inner(sems):
        copies = [
            pltpu.make_async_copy(ref, out_ref.at[:, :, i * width : (i + 1) * width], sems.at[i])
            for i, ref in enumerate((k_ref, v_ref))
        ]
        for copy in copies:
            copy.start()
        for copy in copies:
            copy.wait()

    pl.run_scoped(inner, pltpu.SemaphoreType.DMA((2,)))


def prepare_kernel(step_ref, log_ref, b_ref, c_ref, skip_ref, mix_ref, bw_ref, scale_ref, tot_ref, pass_ref):
    heads, toks = step_ref.shape
    half = toks // 2
    highest = lax.Precision.HIGHEST
    log = log_ref[...]
    step = step_ref[...]
    rows = lax.broadcasted_iota(jnp.int32, (toks, toks), 0)
    cols = lax.broadcasted_iota(jnp.int32, (toks, toks), 1)
    lower = (rows >= cols).astype(F32)
    cum = dot(log, lower, (1, 1), highest)
    cum_cols = dot(lower, log, (1, 1), highest)
    total = cum[:, toks - 1 :]
    weight = jnp.exp(total - cum) * step
    cross = dot(c_ref[...], b_ref[...], (1, 1))
    b_t = jnp.transpose(b_ref[...].astype(F32))
    causal = (
        lax.broadcasted_iota(jnp.int32, (half, half), 0)
        >= lax.broadcasted_iota(jnp.int32, (half, half), 1)
    )
    lanes = lax.broadcasted_iota(jnp.int32, (toks, HDIM), 1)
    for pair in range(heads // 2):
        for side in range(2):
            k = 2 * pair + side
            at = side * toks
            for r in range(2):
                for c in range(2):
                    dst = (pair, slice(r * half, (r + 1) * half), slice(at + c * half, at + (c + 1) * half))
                    if c > r:
                        mix_ref[dst] = jnp.zeros((half, half), BF16)
                        continue
                    rs, cs = slice(r * half, (r + 1) * half), slice(c * half, (c + 1) * half)
                    gap = cum_cols[rs, k : k + 1] - cum[k : k + 1, cs]
                    if r == c:
                        gap = jnp.where(causal, gap, -jnp.inf)
                    mix_ref[dst] = (jnp.exp(gap) * cross[rs, cs] * step[k : k + 1, cs]).astype(BF16)
            bw_ref[pair, :, at : at + toks] = (b_t * weight[k : k + 1, :]).astype(BF16)
        both = jnp.where(
            lanes < SDIM,
            cum_cols[:, 2 * pair : 2 * pair + 1],
            cum_cols[:, 2 * pair + 1 : 2 * pair + 2],
        )
        both = jnp.exp(both)
        scale_ref[:, pair * HDIM : (pair + 1) * HDIM] = both
        tot_ref[:, pair * HDIM : (pair + 1) * HDIM] = both[toks - 1 :, :]
        pass_ref[:, pair * HDIM : (pair + 1) * HDIM] = jnp.where(
            lanes[:1] < SDIM, skip_ref[2 * pair], skip_ref[2 * pair + 1]
        )


def attention_kernel(second, q_ref, kv_ref, near_ref, far_even_ref, far_odd_ref, *refs):
    if second:
        before_ref, out_ref, sums_ref = refs
    else:
        out_ref, sums_ref = refs
    me, count = lax.axis_index("seq"), lax.axis_size("seq")
    blk, feat = q_ref.shape[1:]
    kv_local = kv_ref.shape[2] // (2 * HDIM)
    group = feat // HDIM // kv_local
    odd = me % 2
    slot = 1 - odd if second else odd
    near_slot = jnp.where(me < 1, 0, slot)
    far_slot = jnp.where(me < 2, 0, slot)
    block = slot * count + me
    rows = lax.broadcasted_iota(jnp.int32, (group * blk, blk), 0) % blk
    cols = lax.broadcasted_iota(jnp.int32, (group * blk, blk), 1)
    own_ok = cols <= rows
    far_ok = (cols > rows) & (block >= 2)
    near_ok = (cols >= 0) & (block >= 1)
    factor = math.log2(math.e) / math.sqrt(HDIM)
    squares = jnp.zeros((blk, 1), F32)

    def take(column):
        at = slice(column * HDIM, (column + 1) * HDIM)
        far = jnp.where(odd == 1, far_odd_ref[far_slot, :, at], far_even_ref[far_slot, :, at])
        return jnp.concatenate([far, near_ref[near_slot, :, at], kv_ref[slot, :, at]], 0)

    for g in range(kv_local):
        heads = [
            q_ref[slot, :, (g * group + i) * HDIM : (g * group + i + 1) * HDIM] for i in range(group)
        ]
        query = jnp.concatenate(heads, 0)
        score = dot(query, take(g), (1, 1))
        ok = jnp.concatenate([far_ok, near_ok, own_ok], 1)
        score = jnp.where(ok, score, -jnp.inf)
        peak = jnp.max(score, axis=1, keepdims=True)
        terms = jnp.exp2((score - peak) * factor)
        total = jnp.sum(terms, axis=1, keepdims=True)
        result = dot(terms.astype(BF16), take(kv_local + g)) / total
        result = result.astype(BF16)
        wide = result.astype(F32)
        part = jnp.sum(wide * wide, axis=1, keepdims=True)
        for i in range(group):
            out_ref[:, (g * group + i) * HDIM : (g * group + i + 1) * HDIM] = result[
                i * blk : (i + 1) * blk
            ]
            squares = squares + part[i * blk : (i + 1) * blk]
    turned = jnp.transpose(jnp.broadcast_to(squares, (blk, blk)))[:8]
    if second:
        sums_ref[:8] = before_ref[...]
        sums_ref[8:] = turned
    else:
        sums_ref[...] = turned


def home_kernel(xa_ref, xb_ref, ra_ref, rb_ref, gain_ref, bw_ref, x_ref, keep_ref, send_ref):
    me, count = lax.axis_index("seq"), lax.axis_size("seq")
    blk, feat = xa_ref.shape
    upper = me >= count // 2
    pairs = feat // HDIM
    mine = me % 2
    gain = gain_ref[...]
    for part in range(2):
        swap = upper if part == 0 else jnp.logical_not(upper)
        sums = jnp.where(swap, rb_ref[...], ra_ref[...])
        mean = jnp.transpose(jnp.broadcast_to(sums[:1], (blk, blk))) / (HEADS * HDIM)
        inv = lax.rsqrt(mean + 1e-06)[:, :1]
        rows = jnp.where(swap, xb_ref[...], xa_ref[...]).astype(F32)
        x_ref[part * blk : (part + 1) * blk, :] = (rows * gain * inv).astype(BF16)
    lanes = lax.broadcasted_iota(jnp.int32, (2 * blk, HDIM), 1)
    zero = jnp.zeros((2 * blk, HDIM), BF16)
    for p in range(pairs):
        x = x_ref[:, p * HDIM : (p + 1) * HDIM]
        spread = jnp.concatenate([jnp.where(lanes < SDIM, x, zero), jnp.where(lanes < SDIM, zero, x)], 0)
        state = dot(bw_ref[p], spread)
        side = 0 if p < pairs // 2 else 1
        at = (p % (pairs // 2)) * HDIM

        @pl.when(mine == side)
        def _():
            keep_ref[:, at : at + HDIM] = state

        @pl.when(mine != side)
        def _():
            send_ref[:, at : at + HDIM] = state.astype(BF16)


def local_kernel(x_ref, mix_ref, skip_ref, out_ref):
    toks, feat = x_ref.shape
    lanes = lax.broadcasted_iota(jnp.int32, (toks, HDIM), 1)
    zero = jnp.zeros((toks, HDIM), BF16)
    for p in range(feat // HDIM):
        at = slice(p * HDIM, (p + 1) * HDIM)
        x = x_ref[:, at]
        spread = jnp.concatenate([jnp.where(lanes < SDIM, x, zero), jnp.where(lanes < SDIM, zero, x)], 0)
        out_ref[:, at] = dot(mix_ref[p], spread) + skip_ref[:, at] * x.astype(F32)


def final_kernel(local_ref, scale_ref, c_ref, own_ref, other_ref, out_ref):
    mine = lax.axis_index("seq") % 2
    half = own_ref.shape[1]
    for ref, side in ((own_ref, mine), (other_ref, 1 - mine)):
        at = pl.ds(pl.multiple_of(side * half, half), half)
        part = dot(c_ref[...], ref[...])
        out_ref[:, at] = (local_ref[:, at] + part * scale_ref[:, at]).astype(BF16)


def add_kernel(a_ref, b_ref, *out_refs):
    rows = a_ref.shape[0] // len(out_refs)
    for i, ref in enumerate(out_refs):
        at = slice(i * rows, (i + 1) * rows)
        ref[...] = a_ref[at] + b_ref[at]


def half_of(ref, side):
    half = ref.shape[1] // 2
    return ref[:, pl.ds(pl.multiple_of(side * half, half), half)]


def decay_kernel(tot_ref, core_ref, out_ref):
    mine = lax.axis_index("seq") % 2
    out_ref[...] = half_of(tot_ref, mine) * half_of(core_ref, mine)


def times_kernel(a_ref, b_ref, out_ref):
    out_ref[...] = a_ref[...] * b_ref[...]


def chip_kernel(keep_ref, got_ref, tot_ref, core_ref, early_ref, total_ref, low_ref):
    mine = lax.axis_index("seq") % 2
    late = mine == 1
    keep, got = keep_ref[...], got_ref[...].astype(F32)
    second = jnp.where(late, half_of(tot_ref, mine), half_of(core_ref, mine))
    early = jnp.where(late, got, keep)
    total = second * early + jnp.where(late, keep, got)
    early_ref[...] = early
    total_ref[...] = total
    low_ref[...] = total.astype(BF16)


def stage_kernel(bit, total_ref, theirs_ref, mine_ref, decay_ref, enter_in_ref, carried_in_ref, *outs):
    upper = (lax.axis_index("seq") >> bit) % 2 == 1
    theirs = theirs_ref[...].astype(F32)
    enter_ref, carried_ref, next_ref, low_ref = outs
    carried = carried_in_ref[...]
    enter_ref[...] = enter_in_ref[...] + jnp.where(upper, carried * theirs, 0.0)
    carried_ref[...] = jnp.where(upper, carried * decay_ref[...], carried)
    total = total_ref[...]
    total = jnp.where(upper, mine_ref[...] * theirs + total, decay_ref[...] * total + theirs)
    next_ref[...] = total
    low_ref[...] = total.astype(BF16)


def last_kernel(bit, theirs_ref, enter_in_ref, carried_ref, early_ref, tot_ref, core_ref, own_ref, give_ref):
    me = lax.axis_index("seq")
    mine = me % 2
    late = mine == 1
    upper = (me >> bit) % 2 == 1
    enter = enter_in_ref[...]
    enter = enter + jnp.where(upper, carried_ref[...] * theirs_ref[...].astype(F32), 0.0)
    first = jnp.where(late, half_of(core_ref, mine), half_of(tot_ref, mine))
    after = first * enter + early_ref[...]
    own_ref[...] = jnp.where(late, after, enter).astype(BF16)
    give_ref[...] = jnp.where(late, enter, after).astype(BF16)


def layer(query, keys, values, norm_gain, in_b, out_c, step, log_decay, skip):
    seq_count = lax.axis_size("seq")
    head_count = lax.axis_size("head")
    blk, feat = query.shape[1:]
    heads, toks = step.shape
    kv_width = keys.shape[2]
    pairs = heads // 2
    half = feat // 2
    every = range(seq_count)
    any_space = pltpu.HBM

    def swap(block, bit):
        return lax.ppermute(block, "seq", [(i, i ^ (1 << bit)) for i in every])

    (kv,) = call(pack_kernel, [((2, blk, 2 * kv_width), BF16)], (keys, values), spaces=[any_space] * 2)
    near = lax.ppermute(kv, "seq", [(i, (i + 1) % seq_count) for i in every])
    far_even = lax.ppermute(kv, "seq", [(i, (i + 2) % seq_count) for i in every if i % 2 == 0])
    far_odd = lax.ppermute(near, "seq", [(i, i + 1) for i in every if i % 2 == 0])

    mix, b_weighted, scale, tot, skip_row = call(
        prepare_kernel,
        [
            ((pairs, toks, 2 * toks), BF16),
            ((pairs, STATE, 2 * toks), BF16),
            ((toks, feat), F32),
            ((1, feat), F32),
            ((1, feat), F32),
        ],
        (step, log_decay, in_b, out_c, skip),
        flops=1 << 30,
        spaces=[VMEM] * 4 + [pltpu.SMEM],
    )
    bits = seq_count.bit_length() - 1
    core = swap(tot, 0)
    (chip,) = call(decay_kernel, [((1, half), F32)], (tot, core))

    args = (query, kv, near, far_even, far_odd)
    first, sums = call(
        functools.partial(attention_kernel, False), [((blk, feat), BF16), ((8, blk), F32)], args, flops=1 << 28
    )
    to_a = [(i, i // 2 + (i % 2) * (seq_count // 2)) for i in every]
    to_b = [(i, i // 2 + (1 - i % 2) * (seq_count // 2)) for i in every]
    home_a = lax.ppermute(first, "seq", to_a)
    second, sums = call(
        functools.partial(attention_kernel, True),
        [((blk, feat), BF16), ((16, blk), F32)],
        args + (sums,),
        flops=1 << 28,
    )
    home_b = lax.ppermute(second, "seq", to_b)
    z_bits = head_count.bit_length() - 1
    for bit in range(z_bits):
        other = lax.ppermute(sums, "head", [(i, i ^ (1 << bit)) for i in range(head_count)])
        parts = 2 if bit == z_bits - 1 else 1
        added = call(add_kernel, [((16 // parts, blk), F32)] * parts, (sums, other))
        sums = added[0]
    sums_a = lax.ppermute(added[0], "seq", to_a)
    sums_b = lax.ppermute(added[1], "seq", to_b)
    decays = []
    running = [chip]
    for bit in range(1, bits - 1):
        decays.append(swap(running[-1], bit))
        if bit < bits - 2:
            running += call(times_kernel, [((1, half), F32)], (running[-1], decays[-1]))

    x, keep, send = call(
        home_kernel,
        [((toks, feat), BF16), ((STATE, half), F32), ((STATE, half), BF16)],
        (home_a, home_b, sums_a, sums_b, norm_gain[None, :], b_weighted),
        flops=1 << 28,
    )
    (local,) = call(local_kernel, [((toks, feat), F32)], (x, mix, skip_row), flops=1 << 29)
    got = swap(send, 0)
    state = ((STATE, half), F32)
    row = ((1, half), F32)
    early, total, low = call(chip_kernel, [state, state, ((STATE, half), BF16)], (keep, got, tot, core))
    enter, carried = jnp.zeros(*state), jnp.ones(*row)
    for bit in range(1, bits):
        theirs = swap(low, bit)
        if bit < bits - 1:
            enter, carried, total, low = call(
                functools.partial(stage_kernel, bit),
                [state, row, state, ((STATE, half), BF16)],
                (total, theirs, running[bit - 1], decays[bit - 1], enter, carried),
            )
    own, give = call(
        functools.partial(last_kernel, bits - 1),
        [((STATE, half), BF16)] * 2,
        (theirs, enter, carried, early, tot, core),
    )
    other = swap(give, 0)
    (out,) = call(final_kernel, [((toks, feat), BF16)], (local, scale, out_c, own, other), flops=1 << 28)
    return out


def solution(mesh):
    placed = (
        P(None, "seq", "head"),
        P(None, "seq", "head"),
        P(None, "seq", "head"),
        P("head"),
        P("seq", None),
        P("seq", None),
        P("head", "seq"),
        P("head", "seq"),
        P("head"),
    )
    return jax.shard_map(layer, mesh=mesh, in_specs=placed, out_specs=P("seq", "head"), check_vma=False)
```

```python
import functools
import math

import jax
import jax.numpy as jnp
from jax import lax
from jax.experimental import pallas as pl
from jax.experimental.pallas import tpu as pltpu
from jax.sharding import PartitionSpec as P


HEADS = 32
HDIM = 128
SDIM = 64
STATE = 128

F32 = jnp.float32
BF16 = jnp.bfloat16
VMEM = pltpu.VMEM
GRANT = 12 << 20


def dot(a, b, contract=(1, 0), precision=None):
    return lax.dot_general(
        a,
        b,
        (((contract[0],), (contract[1],)), ((), ())),
        precision=precision,
        preferred_element_type=F32,
    )


def call(kernel, outs, args, flops=1, spaces=None):
    spaces = spaces or [VMEM] * len(args)
    return pl.pallas_call(
        kernel,
        out_shape=[jax.ShapeDtypeStruct(s, d) for s, d in outs],
        in_specs=[pl.BlockSpec(memory_space=m) for m in spaces],
        out_specs=[pl.BlockSpec(memory_space=VMEM)] * len(outs),
        compiler_params=pltpu.CompilerParams(vmem_limit_bytes=GRANT),
        cost_estimate=pl.CostEstimate(flops=flops, bytes_accessed=1 << 20, transcendentals=0),
    )(*[pltpu.with_memory_space_constraint(a, m) if m == pltpu.HBM else a for a, m in zip(args, spaces)])


def pack_kernel(k_ref, v_ref, out_ref):
    width = k_ref.shape[2]

    def inner(sems):
        copies = [
            pltpu.make_async_copy(ref, out_ref.at[:, :, i * width : (i + 1) * width], sems.at[i])
            for i, ref in enumerate((k_ref, v_ref))
        ]
        for copy in copies:
            copy.start()
        for copy in copies:
            copy.wait()

    pl.run_scoped(inner, pltpu.SemaphoreType.DMA((2,)))


def prepare_kernel(*refs):
    def inner(sems, *inside):
        copies = [
            pltpu.make_async_copy(src, dst, sems.at[i])
            for i, (src, dst) in enumerate(zip(refs[:5], inside))
        ]
        for copy in copies:
            copy.start()
        for copy in copies:
            copy.wait()
        prepare(*inside, *refs[5:])

    pl.run_scoped(
        inner,
        pltpu.SemaphoreType.DMA((5,)),
        *[VMEM(r.shape, r.dtype) for r in refs[:4]],
        pltpu.SMEM(refs[4].shape, refs[4].dtype),
    )


def prepare(step_ref, log_ref, b_ref, c_ref, skip_ref, mix_ref, bw_ref, scale_ref, tot_ref, pass_ref):
    heads, toks = step_ref.shape
    half = toks // 2
    highest = lax.Precision.HIGHEST
    log = log_ref[...]
    step = step_ref[...]
    rows = lax.broadcasted_iota(jnp.int32, (toks, toks), 0)
    cols = lax.broadcasted_iota(jnp.int32, (toks, toks), 1)
    lower = (rows >= cols).astype(F32)
    cum = dot(log, lower, (1, 1), highest)
    cum_cols = dot(lower, log, (1, 1), highest)
    total = cum[:, toks - 1 :]
    weight = jnp.exp(total - cum) * step
    cross = dot(c_ref[...], b_ref[...], (1, 1))
    b_t = jnp.transpose(b_ref[...].astype(F32))
    causal = (
        lax.broadcasted_iota(jnp.int32, (half, half), 0)
        >= lax.broadcasted_iota(jnp.int32, (half, half), 1)
    )
    lanes = lax.broadcasted_iota(jnp.int32, (toks, HDIM), 1)
    for pair in range(heads // 2):
        for side in range(2):
            k = 2 * pair + side
            at = side * toks
            for r in range(2):
                for c in range(2):
                    dst = (pair, slice(r * half, (r + 1) * half), slice(at + c * half, at + (c + 1) * half))
                    if c > r:
                        mix_ref[dst] = jnp.zeros((half, half), BF16)
                        continue
                    rs, cs = slice(r * half, (r + 1) * half), slice(c * half, (c + 1) * half)
                    gap = cum_cols[rs, k : k + 1] - cum[k : k + 1, cs]
                    if r == c:
                        gap = jnp.where(causal, gap, -jnp.inf)
                    mix_ref[dst] = (jnp.exp(gap) * cross[rs, cs] * step[k : k + 1, cs]).astype(BF16)
            bw_ref[pair, :, at : at + toks] = (b_t * weight[k : k + 1, :]).astype(BF16)
        both = jnp.where(
            lanes < SDIM,
            cum_cols[:, 2 * pair : 2 * pair + 1],
            cum_cols[:, 2 * pair + 1 : 2 * pair + 2],
        )
        both = jnp.exp(both)
        scale_ref[:, pair * HDIM : (pair + 1) * HDIM] = both
        tot_ref[:, pair * HDIM : (pair + 1) * HDIM] = both[toks - 1 :, :]
        pass_ref[:, pair * HDIM : (pair + 1) * HDIM] = jnp.where(
            lanes[:1] < SDIM, skip_ref[2 * pair], skip_ref[2 * pair + 1]
        )


def attention_kernel(second, q_ref, kv_ref, near_ref, far_even_ref, far_odd_ref, *refs):
    if second:
        before_ref, out_ref, sums_ref = refs
    else:
        out_ref, sums_ref = refs
    me, count = lax.axis_index("seq"), lax.axis_size("seq")
    blk, feat = q_ref.shape[1:]
    kv_local = kv_ref.shape[2] // (2 * HDIM)
    group = feat // HDIM // kv_local
    odd = me % 2
    slot = 1 - odd if second else odd
    near_slot = jnp.where(me < 1, 0, slot)
    far_slot = jnp.where(me < 2, 0, slot)
    block = slot * count + me
    rows = lax.broadcasted_iota(jnp.int32, (group * blk, blk), 0) % blk
    cols = lax.broadcasted_iota(jnp.int32, (group * blk, blk), 1)
    own_ok = cols <= rows
    far_ok = (cols > rows) & (block >= 2)
    near_ok = (cols >= 0) & (block >= 1)
    factor = math.log2(math.e) / math.sqrt(HDIM)
    squares = jnp.zeros((blk, 1), F32)

    def take(column):
        at = slice(column * HDIM, (column + 1) * HDIM)
        far = jnp.where(odd == 1, far_odd_ref[far_slot, :, at], far_even_ref[far_slot, :, at])
        return jnp.concatenate([far, near_ref[near_slot, :, at], kv_ref[slot, :, at]], 0)

    for g in range(kv_local):
        heads = [
            q_ref[slot, :, (g * group + i) * HDIM : (g * group + i + 1) * HDIM] for i in range(group)
        ]
        query = jnp.concatenate(heads, 0)
        score = dot(query, take(g), (1, 1))
        ok = jnp.concatenate([far_ok, near_ok, own_ok], 1)
        score = jnp.where(ok, score, -jnp.inf)
        peak = jnp.max(score, axis=1, keepdims=True)
        terms = jnp.exp2((score - peak) * factor)
        total = jnp.sum(terms, axis=1, keepdims=True)
        result = dot(terms.astype(BF16), take(kv_local + g)) / total
        result = result.astype(BF16)
        wide = result.astype(F32)
        part = jnp.sum(wide * wide, axis=1, keepdims=True)
        for i in range(group):
            out_ref[:, (g * group + i) * HDIM : (g * group + i + 1) * HDIM] = result[
                i * blk : (i + 1) * blk
            ]
            squares = squares + part[i * blk : (i + 1) * blk]
    turned = jnp.transpose(jnp.broadcast_to(squares, (blk, blk)))[:8]
    if second:
        sums_ref[:8] = before_ref[...]
        sums_ref[8:] = turned
    else:
        sums_ref[...] = turned


def home_kernel(xa_ref, xb_ref, ra_ref, rb_ref, gain_ref, bw_ref, x_ref, keep_ref, send_ref):
    me, count = lax.axis_index("seq"), lax.axis_size("seq")
    blk, feat = xa_ref.shape
    upper = me >= count // 2
    pairs = feat // HDIM
    mine = me % 2
    gain = gain_ref[...]
    for part in range(2):
        swap = upper if part == 0 else jnp.logical_not(upper)
        sums = jnp.where(swap, rb_ref[...], ra_ref[...])
        mean = jnp.transpose(jnp.broadcast_to(sums[:1], (blk, blk))) / (HEADS * HDIM)
        inv = lax.rsqrt(mean + 1e-06)[:, :1]
        rows = jnp.where(swap, xb_ref[...], xa_ref[...]).astype(F32)
        x_ref[part * blk : (part + 1) * blk, :] = (rows * gain * inv).astype(BF16)
    lanes = lax.broadcasted_iota(jnp.int32, (2 * blk, HDIM), 1)
    zero = jnp.zeros((2 * blk, HDIM), BF16)
    for p in range(pairs):
        x = x_ref[:, p * HDIM : (p + 1) * HDIM]
        spread = jnp.concatenate([jnp.where(lanes < SDIM, x, zero), jnp.where(lanes < SDIM, zero, x)], 0)
        state = dot(bw_ref[p], spread)
        side = 0 if p < pairs // 2 else 1
        at = (p % (pairs // 2)) * HDIM

        @pl.when(mine == side)
        def _():
            keep_ref[:, at : at + HDIM] = state

        @pl.when(mine != side)
        def _():
            send_ref[:, at : at + HDIM] = state.astype(BF16)


def local_kernel(x_ref, mix_ref, skip_ref, out_ref):
    toks, feat = x_ref.shape
    lanes = lax.broadcasted_iota(jnp.int32, (toks, HDIM), 1)
    zero = jnp.zeros((toks, HDIM), BF16)
    for p in range(feat // HDIM):
        at = slice(p * HDIM, (p + 1) * HDIM)
        x = x_ref[:, at]
        spread = jnp.concatenate([jnp.where(lanes < SDIM, x, zero), jnp.where(lanes < SDIM, zero, x)], 0)
        out_ref[:, at] = dot(mix_ref[p], spread) + skip_ref[:, at] * x.astype(F32)


def final_kernel(local_ref, scale_ref, c_ref, own_ref, other_ref, out_ref):
    mine = lax.axis_index("seq") % 2
    half = own_ref.shape[1]
    for ref, side in ((own_ref, mine), (other_ref, 1 - mine)):
        at = pl.ds(pl.multiple_of(side * half, half), half)
        part = dot(c_ref[...], ref[...])
        out_ref[:, at] = (local_ref[:, at] + part * scale_ref[:, at]).astype(BF16)


def add_kernel(a_ref, b_ref, *out_refs):
    rows = a_ref.shape[0] // len(out_refs)
    for i, ref in enumerate(out_refs):
        at = slice(i * rows, (i + 1) * rows)
        ref[...] = a_ref[at] + b_ref[at]


def half_of(ref, side):
    half = ref.shape[1] // 2
    return ref[:, pl.ds(pl.multiple_of(side * half, half), half)]


def decay_kernel(tot_ref, core_ref, out_ref):
    mine = lax.axis_index("seq") % 2
    out_ref[...] = half_of(tot_ref, mine) * half_of(core_ref, mine)


def times_kernel(a_ref, b_ref, out_ref):
    out_ref[...] = a_ref[...] * b_ref[...]


def chip_kernel(keep_ref, got_ref, tot_ref, core_ref, early_ref, total_ref, low_ref):
    mine = lax.axis_index("seq") % 2
    late = mine == 1
    keep, got = keep_ref[...], got_ref[...].astype(F32)
    second = jnp.where(late, half_of(tot_ref, mine), half_of(core_ref, mine))
    early = jnp.where(late, got, keep)
    total = second * early + jnp.where(late, keep, got)
    early_ref[...] = early
    total_ref[...] = total
    low_ref[...] = total.astype(BF16)


def arrive(bit, theirs_ref, decay_ref, entered):
    upper = (lax.axis_index("seq") >> bit) % 2 == 1
    theirs = theirs_ref[...].astype(F32)
    enter, carried = (None, None) if entered is None else (entered[0][...], entered[1][...])
    step = theirs if carried is None else carried * theirs
    step = jnp.where(upper, step, 0.0)
    enter = step if enter is None else enter + step
    if decay_ref is None:
        return upper, theirs, enter, None
    ahead = decay_ref[...] if carried is None else carried * decay_ref[...]
    stay = jnp.ones_like(ahead) if carried is None else carried
    return upper, theirs, enter, jnp.where(upper, ahead, stay)


def stage_kernel(bit, first, total_ref, theirs_ref, mine_ref, decay_ref, *refs):
    entered, outs = (None, refs) if first else (refs[:2], refs[2:])
    enter_ref, carried_ref, low_ref = outs[:3]
    upper, theirs, enter, carried = arrive(bit, theirs_ref, decay_ref, entered)
    enter_ref[...] = enter
    carried_ref[...] = carried
    total = total_ref[...]
    total = jnp.where(upper, mine_ref[...] * theirs + total, decay_ref[...] * total + theirs)
    low_ref[...] = total.astype(BF16)
    if len(outs) == 4:
        outs[3][...] = total


def last_kernel(bit, theirs_ref, early_ref, tot_ref, core_ref, *refs):
    own_ref, give_ref = refs[-2:]
    mine = lax.axis_index("seq") % 2
    late = mine == 1
    enter = arrive(bit, theirs_ref, None, refs[:-2] or None)[2]
    first = jnp.where(late, half_of(core_ref, mine), half_of(tot_ref, mine))
    after = first * enter + early_ref[...]
    own_ref[...] = jnp.where(late, after, enter).astype(BF16)
    give_ref[...] = jnp.where(late, enter, after).astype(BF16)


def layer(query, keys, values, norm_gain, in_b, out_c, step, log_decay, skip):
    seq_count = lax.axis_size("seq")
    head_count = lax.axis_size("head")
    blk, feat = query.shape[1:]
    heads, toks = step.shape
    kv_width = keys.shape[2]
    pairs = heads // 2
    half = feat // 2
    every = range(seq_count)

    def swap(block, bit):
        return lax.ppermute(block, "seq", [(i, i ^ (1 << bit)) for i in every])

    (kv,) = call(
        pack_kernel, [((2, blk, 2 * kv_width), BF16)], (keys, values), spaces=[pltpu.HBM] * 2
    )
    near = lax.ppermute(kv, "seq", [(i, (i + 1) % seq_count) for i in every])
    far_even = lax.ppermute(kv, "seq", [(i, (i + 2) % seq_count) for i in every if i % 2 == 0])
    far_odd = lax.ppermute(near, "seq", [(i, i + 1) for i in every if i % 2 == 0])

    mix, b_weighted, scale, tot, skip_row = call(
        prepare_kernel,
        [
            ((pairs, toks, 2 * toks), BF16),
            ((pairs, STATE, 2 * toks), BF16),
            ((toks, feat), F32),
            ((1, feat), F32),
            ((1, feat), F32),
        ],
        (step, log_decay, in_b, out_c, skip),
        flops=1 << 30,
        spaces=[pltpu.HBM] * 5,
    )
    bits = seq_count.bit_length() - 1
    core = swap(tot, 0)
    (chip,) = call(decay_kernel, [((1, half), F32)], (tot, core))

    args = (query, kv, near, far_even, far_odd)
    first, sums = call(
        functools.partial(attention_kernel, False),
        [((blk, feat), BF16), ((8, blk), F32)],
        args,
        flops=1 << 28,
    )
    to_a = [(i, i // 2 + (i % 2) * (seq_count // 2)) for i in every]
    to_b = [(i, i // 2 + (1 - i % 2) * (seq_count // 2)) for i in every]
    home_a = lax.ppermute(first, "seq", to_a)
    second, sums = call(
        functools.partial(attention_kernel, True),
        [((blk, feat), BF16), ((16, blk), F32)],
        args + (sums,),
        flops=1 << 28,
    )
    home_b = lax.ppermute(second, "seq", to_b)
    z_bits = head_count.bit_length() - 1
    for bit in range(z_bits):
        other = lax.ppermute(sums, "head", [(i, i ^ (1 << bit)) for i in range(head_count)])
        parts = 2 if bit == z_bits - 1 else 1
        added = call(add_kernel, [((16 // parts, blk), F32)] * parts, (sums, other))
        sums = added[0]
    sums_a = lax.ppermute(added[0], "seq", to_a)
    sums_b = lax.ppermute(added[1], "seq", to_b)
    decays = []
    running = [chip]
    for bit in range(1, bits - 1):
        decays.append(swap(running[-1], bit))
        if bit < bits - 2:
            running += call(times_kernel, [((1, half), F32)], (running[-1], decays[-1]))

    x, keep, send = call(
        home_kernel,
        [((toks, feat), BF16), ((STATE, half), F32), ((STATE, half), BF16)],
        (home_a, home_b, sums_a, sums_b, norm_gain[None, :], b_weighted),
        flops=1 << 28,
    )
    (local,) = call(local_kernel, [((toks, feat), F32)], (x, mix, skip_row), flops=1 << 29)
    got = swap(send, 0)
    state = ((STATE, half), F32)
    row = ((1, half), F32)
    early, total, low = call(
        chip_kernel, [state, state, ((STATE, half), BF16)], (keep, got, tot, core)
    )
    entered = ()
    for bit in range(1, bits):
        theirs = swap(low, bit)
        if bit < bits - 1:
            outs = call(
                functools.partial(stage_kernel, bit, bit == 1),
                [state, row, ((STATE, half), BF16)] + [state] * (bit < bits - 2),
                (total, theirs, running[bit - 1], decays[bit - 1], *entered),
            )
            entered, low, total = outs[:2], outs[2], outs[-1]
    own, give = call(
        functools.partial(last_kernel, bits - 1),
        [((STATE, half), BF16)] * 2,
        (theirs, early, tot, core, *entered),
    )
    other = swap(give, 0)
    (out,) = call(
        final_kernel, [((toks, feat), BF16)], (local, scale, out_c, own, other), flops=1 << 28
    )
    return out


def solution(mesh):
    placed = (
        P(None, "seq", "head"),
        P(None, "seq", "head"),
        P(None, "seq", "head"),
        P("head"),
        P("seq", None),
        P("seq", None),
        P("head", "seq"),
        P("head", "seq"),
        P("head"),
    )
    return jax.shard_map(
        layer, mesh=mesh, in_specs=placed, out_specs=P("seq", "head"), check_vma=False
    )
```

```python
import functools
import math

import jax
import jax.numpy as jnp
from jax import lax
from jax.experimental import pallas as pl
from jax.experimental.pallas import tpu as pltpu
from jax.sharding import PartitionSpec as P


HEADS = 32
HDIM = 128
SDIM = 64
STATE = 128

F32 = jnp.float32
BF16 = jnp.bfloat16
VMEM = pltpu.VMEM
GRANT = 12 << 20


def dot(a, b, contract=(1, 0), precision=None):
    return lax.dot_general(
        a,
        b,
        (((contract[0],), (contract[1],)), ((), ())),
        precision=precision,
        preferred_element_type=F32,
    )


def call(kernel, outs, args, flops=1, spaces=None):
    spaces = spaces or [VMEM] * len(args)
    return pl.pallas_call(
        kernel,
        out_shape=[jax.ShapeDtypeStruct(s, d) for s, d in outs],
        in_specs=[pl.BlockSpec(memory_space=m) for m in spaces],
        out_specs=[pl.BlockSpec(memory_space=VMEM)] * len(outs),
        compiler_params=pltpu.CompilerParams(vmem_limit_bytes=GRANT),
        cost_estimate=pl.CostEstimate(flops=flops, bytes_accessed=1 << 20, transcendentals=0),
    )(*[pltpu.with_memory_space_constraint(a, m) if m == pltpu.HBM else a for a, m in zip(args, spaces)])


def pack_kernel(q_ref, k_ref, v_ref, *refs):
    width = k_ref.shape[2]
    mine = lax.axis_index("seq") % 2
    copies = []

    def inner(sems):
        for i, (kv_ref, q_out_ref) in enumerate((refs[:2], refs[2:])):
            slot = mine if i == 0 else 1 - mine
            for j, (src, dst) in enumerate(
                ((k_ref, kv_ref.at[:, :width]), (v_ref, kv_ref.at[:, width:]), (q_ref, q_out_ref))
            ):
                copies.append(pltpu.make_async_copy(src.at[slot], dst, sems.at[i, j]))
        for copy in copies:
            copy.start()
        for copy in copies:
            copy.wait()

    pl.run_scoped(inner, pltpu.SemaphoreType.DMA((2, 3)))


def prepare_kernel(*refs):
    def inner(sems, *inside):
        copies = [
            pltpu.make_async_copy(src, dst, sems.at[i])
            for i, (src, dst) in enumerate(zip(refs[:5], inside))
        ]
        for copy in copies:
            copy.start()
        for copy in copies:
            copy.wait()
        prepare(*inside, *refs[5:])

    pl.run_scoped(
        inner,
        pltpu.SemaphoreType.DMA((5,)),
        *[VMEM(r.shape, r.dtype) for r in refs[:4]],
        pltpu.SMEM(refs[4].shape, refs[4].dtype),
    )


def prepare(step_ref, log_ref, b_ref, c_ref, skip_ref, mix_ref, bw_ref, scale_ref, tot_ref, pass_ref):
    heads, toks = step_ref.shape
    half = toks // 2
    highest = lax.Precision.HIGHEST
    log = log_ref[...]
    step = step_ref[...]
    rows = lax.broadcasted_iota(jnp.int32, (toks, toks), 0)
    cols = lax.broadcasted_iota(jnp.int32, (toks, toks), 1)
    lower = (rows >= cols).astype(F32)
    cum = dot(log, lower, (1, 1), highest)
    cum_cols = dot(lower, log, (1, 1), highest)
    total = cum[:, toks - 1 :]
    weight = jnp.exp(total - cum) * step
    cross = dot(c_ref[...], b_ref[...], (1, 1))
    b_t = jnp.transpose(b_ref[...].astype(F32))
    causal = (
        lax.broadcasted_iota(jnp.int32, (half, half), 0)
        >= lax.broadcasted_iota(jnp.int32, (half, half), 1)
    )
    lanes = lax.broadcasted_iota(jnp.int32, (toks, HDIM), 1)
    for pair in range(heads // 2):
        for side in range(2):
            k = 2 * pair + side
            at = side * toks
            for r in range(2):
                for c in range(2):
                    dst = (pair, slice(r * half, (r + 1) * half), slice(at + c * half, at + (c + 1) * half))
                    if c > r:
                        mix_ref[dst] = jnp.zeros((half, half), BF16)
                        continue
                    rs, cs = slice(r * half, (r + 1) * half), slice(c * half, (c + 1) * half)
                    gap = cum_cols[rs, k : k + 1] - cum[k : k + 1, cs]
                    if r == c:
                        gap = jnp.where(causal, gap, -jnp.inf)
                    mix_ref[dst] = (jnp.exp(gap) * cross[rs, cs] * step[k : k + 1, cs]).astype(BF16)
            bw_ref[pair, :, at : at + toks] = (b_t * weight[k : k + 1, :]).astype(BF16)
        both = jnp.where(
            lanes < SDIM,
            cum_cols[:, 2 * pair : 2 * pair + 1],
            cum_cols[:, 2 * pair + 1 : 2 * pair + 2],
        )
        both = jnp.exp(both)
        scale_ref[:, pair * HDIM : (pair + 1) * HDIM] = both
        tot_ref[:, pair * HDIM : (pair + 1) * HDIM] = both[toks - 1 :, :]
        pass_ref[:, pair * HDIM : (pair + 1) * HDIM] = jnp.where(
            lanes[:1] < SDIM, skip_ref[2 * pair], skip_ref[2 * pair + 1]
        )


def attention_kernel(
    q_keep_ref, q_got_ref, kv_keep_ref, kv_got_ref, old_keep_ref, old_got_ref, out_ref, sums_ref
):
    me = lax.axis_index("seq")
    blk, feat = q_keep_ref.shape
    kv_local = kv_keep_ref.shape[1] // (2 * HDIM)
    group = feat // HDIM // kv_local
    late = me % 2 == 1
    old_late = jnp.where(me < 2, me % 2 == 0, late)
    has_old = me > 0
    rows = lax.broadcasted_iota(jnp.int32, (group * blk, blk), 0) % blk
    cols = lax.broadcasted_iota(jnp.int32, (group * blk, blk), 1)
    own_ok = cols <= rows
    far_ok = cols > rows
    near_ok = cols >= 0
    factor = math.log2(math.e) / math.sqrt(HDIM)

    def pick(keep_ref, got_ref, swapped, column):
        at = slice(column * HDIM, (column + 1) * HDIM)
        keep, got = keep_ref[:, at], got_ref[:, at]
        return jnp.where(swapped, got, keep), jnp.where(swapped, keep, got)

    squares = [jnp.zeros((blk, 1), F32)] * 2
    for g in range(kv_local):
        keys = pick(old_keep_ref, old_got_ref, old_late, g) + pick(kv_keep_ref, kv_got_ref, late, g)
        c = kv_local + g
        vals = pick(old_keep_ref, old_got_ref, old_late, c) + pick(kv_keep_ref, kv_got_ref, late, c)
        heads = [pick(q_keep_ref, q_got_ref, late, g * group + i) for i in range(group)]
        for part in range(2):
            query = jnp.concatenate([h[part] for h in heads], 0)
            score = dot(query, jnp.concatenate(keys[part : part + 3], 0), (1, 1))
            ok = (
                [far_ok & has_old, near_ok & has_old, own_ok]
                if part == 0
                else [far_ok & has_old, near_ok, own_ok]
            )
            score = jnp.where(jnp.concatenate(ok, 1), score, -jnp.inf)
            peak = jnp.max(score, axis=1, keepdims=True)
            terms = jnp.exp2((score - peak) * factor)
            total = jnp.sum(terms, axis=1, keepdims=True)
            values = jnp.concatenate(vals[part : part + 3], 0)
            result = (dot(terms.astype(BF16), values) / total).astype(BF16)
            wide = result.astype(F32)
            square = jnp.sum(wide * wide, axis=1, keepdims=True)
            for i in range(group):
                at = slice((g * group + i) * HDIM, (g * group + i + 1) * HDIM)
                out_ref[part * blk : (part + 1) * blk, at] = result[i * blk : (i + 1) * blk]
                squares[part] = squares[part] + square[i * blk : (i + 1) * blk]
    for part in range(2):
        turned = jnp.transpose(jnp.broadcast_to(squares[part], (blk, blk)))
        sums_ref[part * 8 : part * 8 + 8] = turned[:8]


def home_kernel(rows_ref, sums_ref, gain_ref, bw_ref, x_ref, keep_ref, send_ref):
    mine = lax.axis_index("seq") % 2
    toks, feat = rows_ref.shape
    blk = toks // 2
    pairs = feat // HDIM
    gain = gain_ref[...]
    for part in range(2):
        at = slice(part * blk, (part + 1) * blk)
        sums = sums_ref[part * 8 : part * 8 + 1]
        mean = jnp.transpose(jnp.broadcast_to(sums, (blk, blk))) / (HEADS * HDIM)
        inv = lax.rsqrt(mean + 1e-06)[:, :1]
        x_ref[at, :] = (rows_ref[at, :].astype(F32) * gain * inv).astype(BF16)
    lanes = lax.broadcasted_iota(jnp.int32, (toks, HDIM), 1)
    zero = jnp.zeros((toks, HDIM), BF16)
    for p in range(pairs):
        x = x_ref[:, p * HDIM : (p + 1) * HDIM]
        spread = jnp.concatenate([jnp.where(lanes < SDIM, x, zero), jnp.where(lanes < SDIM, zero, x)], 0)
        state = dot(bw_ref[p], spread)
        side = 0 if p < pairs // 2 else 1
        at = (p % (pairs // 2)) * HDIM

        @pl.when(mine == side)
        def _():
            keep_ref[:, at : at + HDIM] = state

        @pl.when(mine != side)
        def _():
            send_ref[:, at : at + HDIM] = state.astype(BF16)


def local_kernel(x_ref, mix_ref, skip_ref, out_ref):
    toks, feat = x_ref.shape
    lanes = lax.broadcasted_iota(jnp.int32, (toks, HDIM), 1)
    zero = jnp.zeros((toks, HDIM), BF16)
    for p in range(feat // HDIM):
        at = slice(p * HDIM, (p + 1) * HDIM)
        x = x_ref[:, at]
        spread = jnp.concatenate([jnp.where(lanes < SDIM, x, zero), jnp.where(lanes < SDIM, zero, x)], 0)
        out_ref[:, at] = dot(mix_ref[p], spread) + skip_ref[:, at] * x.astype(F32)


def final_kernel(local_ref, scale_ref, c_ref, own_ref, other_ref, out_ref):
    mine = lax.axis_index("seq") % 2
    half = own_ref.shape[1]
    for ref, side in ((own_ref, mine), (other_ref, 1 - mine)):
        at = pl.ds(pl.multiple_of(side * half, half), half)
        part = dot(c_ref[...], ref[...])
        out_ref[:, at] = (local_ref[:, at] + part * scale_ref[:, at]).astype(BF16)


def add_kernel(a_ref, b_ref, out_ref):
    out_ref[...] = a_ref[...] + b_ref[...]


def half_of(ref, side):
    half = ref.shape[1] // 2
    return ref[:, pl.ds(pl.multiple_of(side * half, half), half)]


def decay_kernel(tot_ref, core_ref, out_ref):
    mine = lax.axis_index("seq") % 2
    out_ref[...] = half_of(tot_ref, mine) * half_of(core_ref, mine)


def times_kernel(a_ref, b_ref, out_ref):
    out_ref[...] = a_ref[...] * b_ref[...]


def chip_kernel(keep_ref, got_ref, tot_ref, core_ref, early_ref, total_ref, low_ref):
    mine = lax.axis_index("seq") % 2
    late = mine == 1
    keep, got = keep_ref[...], got_ref[...].astype(F32)
    second = jnp.where(late, half_of(tot_ref, mine), half_of(core_ref, mine))
    early = jnp.where(late, got, keep)
    total = second * early + jnp.where(late, keep, got)
    early_ref[...] = early
    total_ref[...] = total
    low_ref[...] = total.astype(BF16)


def arrive(bit, theirs_ref, decay_ref, entered):
    upper = (lax.axis_index("seq") >> bit) % 2 == 1
    theirs = theirs_ref[...].astype(F32)
    enter, carried = (None, None) if entered is None else (entered[0][...], entered[1][...])
    step = theirs if carried is None else carried * theirs
    step = jnp.where(upper, step, 0.0)
    enter = step if enter is None else enter + step
    if decay_ref is None:
        return upper, theirs, enter, None
    ahead = decay_ref[...] if carried is None else carried * decay_ref[...]
    stay = jnp.ones_like(ahead) if carried is None else carried
    return upper, theirs, enter, jnp.where(upper, ahead, stay)


def stage_kernel(bit, first, total_ref, theirs_ref, mine_ref, decay_ref, *refs):
    entered, outs = (None, refs) if first else (refs[:2], refs[2:])
    enter_ref, carried_ref, low_ref = outs[:3]
    upper, theirs, enter, carried = arrive(bit, theirs_ref, decay_ref, entered)
    enter_ref[...] = enter
    carried_ref[...] = carried
    total = total_ref[...]
    total = jnp.where(upper, mine_ref[...] * theirs + total, decay_ref[...] * total + theirs)
    low_ref[...] = total.astype(BF16)
    if len(outs) == 4:
        outs[3][...] = total


def last_kernel(bit, theirs_ref, early_ref, tot_ref, core_ref, *refs):
    own_ref, give_ref = refs[-2:]
    mine = lax.axis_index("seq") % 2
    late = mine == 1
    enter = arrive(bit, theirs_ref, None, refs[:-2] or None)[2]
    first = jnp.where(late, half_of(core_ref, mine), half_of(tot_ref, mine))
    after = first * enter + early_ref[...]
    own_ref[...] = jnp.where(late, after, enter).astype(BF16)
    give_ref[...] = jnp.where(late, enter, after).astype(BF16)


def layer(query, keys, values, norm_gain, in_b, out_c, step, log_decay, skip):
    seq_count = lax.axis_size("seq")
    head_count = lax.axis_size("head")
    blk, feat = query.shape[1:]
    heads, toks = step.shape
    kv_width = keys.shape[2]
    pairs = heads // 2
    half = feat // 2
    every = range(seq_count)

    def swap(block, bit):
        return lax.ppermute(block, "seq", [(i, i ^ (1 << bit)) for i in every])

    width = 2 * kv_width
    kv_keep, q_keep, kv_send, q_send = call(
        pack_kernel,
        [((blk, width), BF16), ((blk, feat), BF16)] * 2,
        (query, keys, values),
        spaces=[pltpu.HBM] * 3,
    )
    chips = seq_count // 2
    onward = [(i, i + 2) for i in range(seq_count - 2)] + [(seq_count - 2, 1)]
    kv_got = swap(kv_send, 0)
    old_keep = lax.ppermute(kv_keep, "seq", onward)
    old_got = lax.ppermute(kv_got, "seq", onward)
    q_got = swap(q_send, 0)

    mix, b_weighted, scale, tot, skip_row = call(
        prepare_kernel,
        [
            ((pairs, toks, 2 * toks), BF16),
            ((pairs, STATE, 2 * toks), BF16),
            ((toks, feat), F32),
            ((1, feat), F32),
            ((1, feat), F32),
        ],
        (step, log_decay, in_b, out_c, skip),
        flops=1 << 30,
        spaces=[pltpu.HBM] * 5,
    )
    bits = seq_count.bit_length() - 1
    core = swap(tot, 0)
    (chip,) = call(decay_kernel, [((1, half), F32)], (tot, core))

    attended, sums = call(
        attention_kernel,
        [((toks, feat), BF16), ((16, blk), F32)],
        (q_keep, q_got, kv_keep, kv_got, old_keep, old_got),
        flops=1 << 29,
    )
    to_home = [(i, i // 2 + (i % 2) * chips) for i in every]
    sums = lax.ppermute(sums, "seq", to_home)
    rows = lax.ppermute(attended, "seq", to_home)
    for bit in range(head_count.bit_length() - 1):
        other = lax.ppermute(sums, "head", [(i, i ^ (1 << bit)) for i in range(head_count)])
        (sums,) = call(add_kernel, [((16, blk), F32)], (sums, other))
    decays = []
    running = [chip]
    for bit in range(1, bits - 1):
        decays.append(swap(running[-1], bit))
        if bit < bits - 2:
            running += call(times_kernel, [((1, half), F32)], (running[-1], decays[-1]))

    x, keep, send = call(
        home_kernel,
        [((toks, feat), BF16), ((STATE, half), F32), ((STATE, half), BF16)],
        (rows, sums, norm_gain[None, :], b_weighted),
        flops=1 << 28,
    )
    (local,) = call(local_kernel, [((toks, feat), F32)], (x, mix, skip_row), flops=1 << 29)
    got = swap(send, 0)
    state = ((STATE, half), F32)
    row = ((1, half), F32)
    early, total, low = call(
        chip_kernel, [state, state, ((STATE, half), BF16)], (keep, got, tot, core)
    )
    entered = ()
    for bit in range(1, bits):
        theirs = swap(low, bit)
        if bit < bits - 1:
            outs = call(
                functools.partial(stage_kernel, bit, bit == 1),
                [state, row, ((STATE, half), BF16)] + [state] * (bit < bits - 2),
                (total, theirs, running[bit - 1], decays[bit - 1], *entered),
            )
            entered, low, total = outs[:2], outs[2], outs[-1]
    own, give = call(
        functools.partial(last_kernel, bits - 1),
        [((STATE, half), BF16)] * 2,
        (theirs, early, tot, core, *entered),
    )
    other = swap(give, 0)
    (out,) = call(
        final_kernel, [((toks, feat), BF16)], (local, scale, out_c, own, other), flops=1 << 28
    )
    return out


def solution(mesh):
    placed = (
        P(None, "seq", "head"),
        P(None, "seq", "head"),
        P(None, "seq", "head"),
        P("head"),
        P("seq", None),
        P("seq", None),
        P("head", "seq"),
        P("head", "seq"),
        P("head"),
    )
    return jax.shard_map(
        layer, mesh=mesh, in_specs=placed, out_specs=P("seq", "head"), check_vma=False
    )
```

```python
import functools
import math

import jax
import jax.numpy as jnp
from jax import lax
from jax.experimental import pallas as pl
from jax.experimental.pallas import tpu as pltpu
from jax.sharding import PartitionSpec as P


HEADS = 32
HDIM = 128
SDIM = 64
STATE = 128

F32 = jnp.float32
BF16 = jnp.bfloat16
VMEM = pltpu.VMEM
GRANT = 12 << 20


def dot(a, b, contract=(1, 0), precision=None):
    return lax.dot_general(
        a,
        b,
        (((contract[0],), (contract[1],)), ((), ())),
        precision=precision,
        preferred_element_type=F32,
    )


def call(kernel, outs, args, flops=1, spaces=None):
    spaces = spaces or [VMEM] * len(args)
    return pl.pallas_call(
        kernel,
        out_shape=[jax.ShapeDtypeStruct(s, d) for s, d in outs],
        in_specs=[pl.BlockSpec(memory_space=m) for m in spaces],
        out_specs=[pl.BlockSpec(memory_space=VMEM)] * len(outs),
        compiler_params=pltpu.CompilerParams(vmem_limit_bytes=GRANT),
        cost_estimate=pl.CostEstimate(flops=flops, bytes_accessed=1 << 20, transcendentals=0),
    )(*[pltpu.with_memory_space_constraint(a, m) if m == pltpu.HBM else a for a, m in zip(args, spaces)])


def pack_kernel(q_ref, k_ref, v_ref, *refs):
    width = k_ref.shape[2]
    mine = lax.axis_index("seq") % 2
    copies = []

    def inner(sems):
        for i, (kv_ref, q_out_ref) in enumerate((refs[:2], refs[2:])):
            slot = 1 - mine if i == 0 else mine
            for j, (src, dst) in enumerate(
                ((k_ref, kv_ref.at[:, :width]), (v_ref, kv_ref.at[:, width:]), (q_ref, q_out_ref))
            ):
                copies.append(pltpu.make_async_copy(src.at[slot], dst, sems.at[i, j]))
        for copy in copies:
            copy.start()
        for copy in copies:
            copy.wait()

    pl.run_scoped(inner, pltpu.SemaphoreType.DMA((2, 3)))


def prepare_kernel(*refs):
    def inner(sems, *inside):
        copies = [
            pltpu.make_async_copy(src, dst, sems.at[i])
            for i, (src, dst) in enumerate(zip(refs[:5], inside))
        ]
        for copy in copies:
            copy.start()
        for copy in copies:
            copy.wait()
        prepare(*inside, *refs[5:])

    pl.run_scoped(
        inner,
        pltpu.SemaphoreType.DMA((5,)),
        *[VMEM(r.shape, r.dtype) for r in refs[:4]],
        pltpu.SMEM(refs[4].shape, refs[4].dtype),
    )


def prepare(step_ref, log_ref, b_ref, c_ref, skip_ref, mix_ref, bw_ref, scale_ref, tot_ref, pass_ref):
    heads, toks = step_ref.shape
    half = toks // 2
    highest = lax.Precision.HIGHEST
    log = log_ref[...]
    step = step_ref[...]
    rows = lax.broadcasted_iota(jnp.int32, (toks, toks), 0)
    cols = lax.broadcasted_iota(jnp.int32, (toks, toks), 1)
    lower = (rows >= cols).astype(F32)
    cum = dot(log, lower, (1, 1), highest)
    cum_cols = dot(lower, log, (1, 1), highest)
    total = cum[:, toks - 1 :]
    weight = jnp.exp(total - cum) * step
    cross = dot(c_ref[...], b_ref[...], (1, 1))
    b_t = jnp.transpose(b_ref[...].astype(F32))
    causal = (
        lax.broadcasted_iota(jnp.int32, (half, half), 0)
        >= lax.broadcasted_iota(jnp.int32, (half, half), 1)
    )
    lanes = lax.broadcasted_iota(jnp.int32, (toks, HDIM), 1)
    for pair in range(heads // 2):
        for side in range(2):
            k = 2 * pair + side
            at = side * toks
            for r in range(2):
                for c in range(2):
                    dst = (pair, slice(r * half, (r + 1) * half), slice(at + c * half, at + (c + 1) * half))
                    if c > r:
                        mix_ref[dst] = jnp.zeros((half, half), BF16)
                        continue
                    rs, cs = slice(r * half, (r + 1) * half), slice(c * half, (c + 1) * half)
                    gap = cum_cols[rs, k : k + 1] - cum[k : k + 1, cs]
                    if r == c:
                        gap = jnp.where(causal, gap, -jnp.inf)
                    mix_ref[dst] = (jnp.exp(gap) * cross[rs, cs] * step[k : k + 1, cs]).astype(BF16)
            bw_ref[pair, :, at : at + toks] = (b_t * weight[k : k + 1, :]).astype(BF16)
        both = jnp.where(
            lanes < SDIM,
            cum_cols[:, 2 * pair : 2 * pair + 1],
            cum_cols[:, 2 * pair + 1 : 2 * pair + 2],
        )
        both = jnp.exp(both)
        scale_ref[:, pair * HDIM : (pair + 1) * HDIM] = both
        tot_ref[:, pair * HDIM : (pair + 1) * HDIM] = both[toks - 1 :, :]
        pass_ref[:, pair * HDIM : (pair + 1) * HDIM] = jnp.where(
            lanes[:1] < SDIM, skip_ref[2 * pair], skip_ref[2 * pair + 1]
        )


def attention_kernel(
    q_keep_ref, q_got_ref, kv_keep_ref, kv_got_ref, old_keep_ref, old_got_ref, out_ref, sums_ref
):
    me = lax.axis_index("seq")
    blk, feat = q_keep_ref.shape
    kv_local = kv_keep_ref.shape[1] // (2 * HDIM)
    group = feat // HDIM // kv_local
    late = me % 2 == 1
    old_late = jnp.where(me < 2, me % 2 == 0, late)
    has_old = me != 1
    rows = lax.broadcasted_iota(jnp.int32, (group * blk, blk), 0) % blk
    cols = lax.broadcasted_iota(jnp.int32, (group * blk, blk), 1)
    own_ok = cols <= rows
    far_ok = cols > rows
    near_ok = cols >= 0
    factor = math.log2(math.e) / math.sqrt(HDIM)

    def pick(keep_ref, got_ref, swapped, column):
        at = slice(column * HDIM, (column + 1) * HDIM)
        keep, got = keep_ref[:, at], got_ref[:, at]
        return jnp.where(swapped, got, keep), jnp.where(swapped, keep, got)

    squares = [jnp.zeros((blk, 1), F32)] * 2
    for g in range(kv_local):
        keys = pick(old_keep_ref, old_got_ref, old_late, g) + pick(kv_keep_ref, kv_got_ref, late, g)
        c = kv_local + g
        vals = pick(old_keep_ref, old_got_ref, old_late, c) + pick(kv_keep_ref, kv_got_ref, late, c)
        heads = [pick(q_keep_ref, q_got_ref, late, g * group + i) for i in range(group)]
        for part in range(2):
            query = jnp.concatenate([h[part] for h in heads], 0)
            score = dot(query, jnp.concatenate(keys[part : part + 3], 0), (1, 1))
            ok = (
                [far_ok & has_old, near_ok & has_old, own_ok]
                if part == 0
                else [far_ok & has_old, near_ok, own_ok]
            )
            score = jnp.where(jnp.concatenate(ok, 1), score, -jnp.inf)
            peak = jnp.max(score, axis=1, keepdims=True)
            terms = jnp.exp2((score - peak) * factor)
            total = jnp.sum(terms, axis=1, keepdims=True)
            values = jnp.concatenate(vals[part : part + 3], 0)
            result = (dot(terms.astype(BF16), values) / total).astype(BF16)
            wide = result.astype(F32)
            square = jnp.sum(wide * wide, axis=1, keepdims=True)
            for i in range(group):
                at = slice((g * group + i) * HDIM, (g * group + i + 1) * HDIM)
                out_ref[part * blk : (part + 1) * blk, at] = result[i * blk : (i + 1) * blk]
                squares[part] = squares[part] + square[i * blk : (i + 1) * blk]
    for part in range(2):
        turned = jnp.transpose(jnp.broadcast_to(squares[part], (blk, blk)))
        sums_ref[part * 8 : part * 8 + 8] = turned[:8]


def home_kernel(rows_ref, sums_ref, gain_ref, bw_ref, x_ref, keep_ref, send_ref):
    mine = lax.axis_index("seq") % 2
    toks, feat = rows_ref.shape
    blk = toks // 2
    pairs = feat // HDIM
    gain = gain_ref[...]
    for part in range(2):
        at = slice(part * blk, (part + 1) * blk)
        sums = sums_ref[part * 8 : part * 8 + 1]
        mean = jnp.transpose(jnp.broadcast_to(sums, (blk, blk))) / (HEADS * HDIM)
        inv = lax.rsqrt(mean + 1e-06)[:, :1]
        x_ref[at, :] = (rows_ref[at, :].astype(F32) * gain * inv).astype(BF16)
    lanes = lax.broadcasted_iota(jnp.int32, (toks, HDIM), 1)
    zero = jnp.zeros((toks, HDIM), BF16)
    for p in range(pairs):
        x = x_ref[:, p * HDIM : (p + 1) * HDIM]
        spread = jnp.concatenate([jnp.where(lanes < SDIM, x, zero), jnp.where(lanes < SDIM, zero, x)], 0)
        state = dot(bw_ref[p], spread)
        side = 0 if p < pairs // 2 else 1
        at = (p % (pairs // 2)) * HDIM

        @pl.when(mine == side)
        def _():
            keep_ref[:, at : at + HDIM] = state

        @pl.when(mine != side)
        def _():
            send_ref[:, at : at + HDIM] = state.astype(BF16)


def local_kernel(x_ref, mix_ref, skip_ref, out_ref):
    toks, feat = x_ref.shape
    lanes = lax.broadcasted_iota(jnp.int32, (toks, HDIM), 1)
    zero = jnp.zeros((toks, HDIM), BF16)
    for p in range(feat // HDIM):
        at = slice(p * HDIM, (p + 1) * HDIM)
        x = x_ref[:, at]
        spread = jnp.concatenate([jnp.where(lanes < SDIM, x, zero), jnp.where(lanes < SDIM, zero, x)], 0)
        out_ref[:, at] = dot(mix_ref[p], spread) + skip_ref[:, at] * x.astype(F32)


def final_kernel(local_ref, scale_ref, c_ref, own_ref, other_ref, out_ref):
    mine = lax.axis_index("seq") % 2
    half = own_ref.shape[1]
    for ref, side in ((own_ref, mine), (other_ref, 1 - mine)):
        at = pl.ds(pl.multiple_of(side * half, half), half)
        part = dot(c_ref[...], ref[...])
        out_ref[:, at] = (local_ref[:, at] + part * scale_ref[:, at]).astype(BF16)


def add_kernel(a_ref, b_ref, out_ref):
    out_ref[...] = a_ref[...] + b_ref[...]


def half_of(ref, side):
    half = ref.shape[1] // 2
    return ref[:, pl.ds(pl.multiple_of(side * half, half), half)]


def decay_kernel(tot_ref, core_ref, out_ref):
    mine = lax.axis_index("seq") % 2
    out_ref[...] = half_of(tot_ref, mine) * half_of(core_ref, mine)


def times_kernel(a_ref, b_ref, out_ref):
    out_ref[...] = a_ref[...] * b_ref[...]


def chip_kernel(keep_ref, got_ref, tot_ref, core_ref, early_ref, total_ref, low_ref):
    mine = lax.axis_index("seq") % 2
    late = mine == 1
    keep, got = keep_ref[...], got_ref[...].astype(F32)
    second = jnp.where(late, half_of(tot_ref, mine), half_of(core_ref, mine))
    early = jnp.where(late, got, keep)
    total = second * early + jnp.where(late, keep, got)
    early_ref[...] = early
    total_ref[...] = total
    low_ref[...] = total.astype(BF16)


def arrive(bit, theirs_ref, decay_ref, entered):
    upper = (lax.axis_index("seq") >> bit) % 2 == 1
    theirs = theirs_ref[...].astype(F32)
    enter, carried = (None, None) if entered is None else (entered[0][...], entered[1][...])
    step = theirs if carried is None else carried * theirs
    step = jnp.where(upper, step, 0.0)
    enter = step if enter is None else enter + step
    if decay_ref is None:
        return upper, theirs, enter, None
    ahead = decay_ref[...] if carried is None else carried * decay_ref[...]
    stay = jnp.ones_like(ahead) if carried is None else carried
    return upper, theirs, enter, jnp.where(upper, ahead, stay)


def stage_kernel(bit, first, total_ref, theirs_ref, mine_ref, decay_ref, *refs):
    entered, outs = (None, refs) if first else (refs[:2], refs[2:])
    enter_ref, carried_ref, low_ref = outs[:3]
    upper, theirs, enter, carried = arrive(bit, theirs_ref, decay_ref, entered)
    enter_ref[...] = enter
    carried_ref[...] = carried
    total = total_ref[...]
    total = jnp.where(upper, mine_ref[...] * theirs + total, decay_ref[...] * total + theirs)
    low_ref[...] = total.astype(BF16)
    if len(outs) == 4:
        outs[3][...] = total


def last_kernel(bit, theirs_ref, early_ref, tot_ref, core_ref, *refs):
    own_ref, give_ref = refs[-2:]
    mine = lax.axis_index("seq") % 2
    late = mine == 1
    enter = arrive(bit, theirs_ref, None, refs[:-2] or None)[2]
    first = jnp.where(late, half_of(core_ref, mine), half_of(tot_ref, mine))
    after = first * enter + early_ref[...]
    own_ref[...] = jnp.where(late, after, enter).astype(BF16)
    give_ref[...] = jnp.where(late, enter, after).astype(BF16)


def layer(query, keys, values, norm_gain, in_b, out_c, step, log_decay, skip):
    seq_count = lax.axis_size("seq")
    head_count = lax.axis_size("head")
    blk, feat = query.shape[1:]
    heads, toks = step.shape
    kv_width = keys.shape[2]
    pairs = heads // 2
    half = feat // 2
    every = range(seq_count)

    def swap(block, bit):
        return lax.ppermute(block, "seq", [(i, i ^ (1 << bit)) for i in every])

    width = 2 * kv_width
    kv_keep, q_keep, kv_send, q_send = call(
        pack_kernel,
        [((blk, width), BF16), ((blk, feat), BF16)] * 2,
        (query, keys, values),
        spaces=[pltpu.HBM] * 3,
    )
    chips = seq_count // 2
    onward = [(i, i + 2) for i in range(seq_count - 2)] + [(seq_count - 2, 1), (seq_count - 1, 0)]
    kv_got = swap(kv_send, 0)
    old_keep = lax.ppermute(kv_keep, "seq", onward)
    old_got = lax.ppermute(kv_got, "seq", onward)
    q_got = swap(q_send, 0)

    mix, b_weighted, scale, tot, skip_row = call(
        prepare_kernel,
        [
            ((pairs, toks, 2 * toks), BF16),
            ((pairs, STATE, 2 * toks), BF16),
            ((toks, feat), F32),
            ((1, feat), F32),
            ((1, feat), F32),
        ],
        (step, log_decay, in_b, out_c, skip),
        flops=1 << 30,
        spaces=[pltpu.HBM] * 5,
    )
    bits = seq_count.bit_length() - 1
    core = swap(tot, 0)
    (chip,) = call(decay_kernel, [((1, half), F32)], (tot, core))

    attended, sums = call(
        attention_kernel,
        [((toks, feat), BF16), ((16, blk), F32)],
        (q_keep, q_got, kv_keep, kv_got, old_keep, old_got),
        flops=1 << 29,
    )
    to_home = [(i, i // 2 + (1 - i % 2) * chips) for i in every]
    sums = lax.ppermute(sums, "seq", to_home)
    rows = lax.ppermute(attended, "seq", to_home)
    for bit in range(head_count.bit_length() - 1):
        other = lax.ppermute(sums, "head", [(i, i ^ (1 << bit)) for i in range(head_count)])
        (sums,) = call(add_kernel, [((16, blk), F32)], (sums, other))
    decays = []
    running = [chip]
    for bit in range(1, bits - 1):
        decays.append(swap(running[-1], bit))
        if bit < bits - 2:
            running += call(times_kernel, [((1, half), F32)], (running[-1], decays[-1]))

    x, keep, send = call(
        home_kernel,
        [((toks, feat), BF16), ((STATE, half), F32), ((STATE, half), BF16)],
        (rows, sums, norm_gain[None, :], b_weighted),
        flops=1 << 28,
    )
    (local,) = call(local_kernel, [((toks, feat), F32)], (x, mix, skip_row), flops=1 << 29)
    got = swap(send, 0)
    state = ((STATE, half), F32)
    row = ((1, half), F32)
    early, total, low = call(
        chip_kernel, [state, state, ((STATE, half), BF16)], (keep, got, tot, core)
    )
    entered = ()
    for bit in range(1, bits):
        theirs = swap(low, bit)
        if bit < bits - 1:
            outs = call(
                functools.partial(stage_kernel, bit, bit == 1),
                [state, row, ((STATE, half), BF16)] + [state] * (bit < bits - 2),
                (total, theirs, running[bit - 1], decays[bit - 1], *entered),
            )
            entered, low, total = outs[:2], outs[2], outs[-1]
    own, give = call(
        functools.partial(last_kernel, bits - 1),
        [((STATE, half), BF16)] * 2,
        (theirs, early, tot, core, *entered),
    )
    other = swap(give, 0)
    (out,) = call(
        final_kernel, [((toks, feat), BF16)], (local, scale, out_c, own, other), flops=1 << 28
    )
    return out


def solution(mesh):
    placed = (
        P(None, "seq", "head"),
        P(None, "seq", "head"),
        P(None, "seq", "head"),
        P("head"),
        P("seq", None),
        P("seq", None),
        P("head", "seq"),
        P("head", "seq"),
        P("head"),
    )
    return jax.shard_map(
        layer, mesh=mesh, in_specs=placed, out_specs=P("seq", "head"), check_vma=False
    )
```

```python
import functools
import math

import jax
import jax.numpy as jnp
from jax import lax
from jax.experimental import pallas as pl
from jax.experimental.pallas import tpu as pltpu
from jax.sharding import PartitionSpec as P


HEADS = 32
HDIM = 128
SDIM = 64
STATE = 128

F32 = jnp.float32
BF16 = jnp.bfloat16
VMEM = pltpu.VMEM
GRANT = 12 << 20


def dot(a, b, contract=(1, 0), precision=None):
    return lax.dot_general(
        a,
        b,
        (((contract[0],), (contract[1],)), ((), ())),
        precision=precision,
        preferred_element_type=F32,
    )


def call(kernel, outs, args, flops=1, spaces=None):
    spaces = spaces or [VMEM] * len(args)
    return pl.pallas_call(
        kernel,
        out_shape=[jax.ShapeDtypeStruct(s, d) for s, d in outs],
        in_specs=[pl.BlockSpec(memory_space=m) for m in spaces],
        out_specs=[pl.BlockSpec(memory_space=VMEM)] * len(outs),
        compiler_params=pltpu.CompilerParams(vmem_limit_bytes=GRANT),
        cost_estimate=pl.CostEstimate(flops=flops, bytes_accessed=1 << 20, transcendentals=0),
    )(*[pltpu.with_memory_space_constraint(a, m) if m == pltpu.HBM else a for a, m in zip(args, spaces)])


def pack_kernel(q_ref, k_ref, v_ref, *refs):
    width = k_ref.shape[2]
    mine = lax.axis_index("seq") % 2
    copies = []

    def inner(sems):
        for i, (kv_ref, q_out_ref) in enumerate((refs[:2], refs[2:])):
            slot = 1 - mine if i == 0 else mine
            for j, (src, dst) in enumerate(
                ((k_ref, kv_ref.at[:, :width]), (v_ref, kv_ref.at[:, width:]), (q_ref, q_out_ref))
            ):
                copies.append(pltpu.make_async_copy(src.at[slot], dst, sems.at[i, j]))
        for copy in copies:
            copy.start()
        for copy in copies:
            copy.wait()

    pl.run_scoped(inner, pltpu.SemaphoreType.DMA((2, 3)))


def prepare_kernel(*refs):
    def inner(sems, *inside):
        copies = [
            pltpu.make_async_copy(src, dst, sems.at[i])
            for i, (src, dst) in enumerate(zip(refs[:5], inside))
        ]
        for copy in copies:
            copy.start()
        for copy in copies:
            copy.wait()
        prepare(*inside, *refs[5:])

    pl.run_scoped(
        inner,
        pltpu.SemaphoreType.DMA((5,)),
        *[VMEM(r.shape, r.dtype) for r in refs[:4]],
        pltpu.SMEM(refs[4].shape, refs[4].dtype),
    )


def prepare(step_ref, log_ref, b_ref, c_ref, skip_ref, mix_ref, bw_ref, scale_ref, tot_ref, pass_ref):
    heads, toks = step_ref.shape
    half = toks // 2
    highest = lax.Precision.HIGHEST
    log = log_ref[...]
    step = step_ref[...]
    rows = lax.broadcasted_iota(jnp.int32, (toks, toks), 0)
    cols = lax.broadcasted_iota(jnp.int32, (toks, toks), 1)
    lower = (rows >= cols).astype(F32)
    cum = dot(log, lower, (1, 1), highest)
    cum_cols = dot(lower, log, (1, 1), highest)
    total = cum[:, toks - 1 :]
    weight = jnp.exp(total - cum) * step
    cross = dot(c_ref[...], b_ref[...], (1, 1))
    b_t = jnp.transpose(b_ref[...].astype(F32))
    causal = (
        lax.broadcasted_iota(jnp.int32, (half, half), 0)
        >= lax.broadcasted_iota(jnp.int32, (half, half), 1)
    )
    lanes = lax.broadcasted_iota(jnp.int32, (toks, HDIM), 1)
    for pair in range(heads // 2):
        for side in range(2):
            k = 2 * pair + side
            at = side * toks
            for r in range(2):
                for c in range(2):
                    dst = (pair, slice(r * half, (r + 1) * half), slice(at + c * half, at + (c + 1) * half))
                    if c > r:
                        mix_ref[dst] = jnp.zeros((half, half), BF16)
                        continue
                    rs, cs = slice(r * half, (r + 1) * half), slice(c * half, (c + 1) * half)
                    gap = cum_cols[rs, k : k + 1] - cum[k : k + 1, cs]
                    if r == c:
                        gap = jnp.where(causal, gap, -jnp.inf)
                    mix_ref[dst] = (jnp.exp(gap) * cross[rs, cs] * step[k : k + 1, cs]).astype(BF16)
            bw_ref[pair, :, at : at + toks] = (b_t * weight[k : k + 1, :]).astype(BF16)
        both = jnp.where(
            lanes < SDIM,
            cum_cols[:, 2 * pair : 2 * pair + 1],
            cum_cols[:, 2 * pair + 1 : 2 * pair + 2],
        )
        both = jnp.exp(both)
        scale_ref[:, pair * HDIM : (pair + 1) * HDIM] = both
        tot_ref[:, pair * HDIM : (pair + 1) * HDIM] = both[toks - 1 :, :]
        pass_ref[:, pair * HDIM : (pair + 1) * HDIM] = jnp.where(
            lanes[:1] < SDIM, skip_ref[2 * pair], skip_ref[2 * pair + 1]
        )


def attention_kernel(
    q_keep_ref, q_got_ref, kv_keep_ref, kv_got_ref, old_keep_ref, old_got_ref, out_ref, sums_ref
):
    me = lax.axis_index("seq")
    blk, feat = q_keep_ref.shape
    kv_local = kv_keep_ref.shape[1] // (2 * HDIM)
    group = feat // HDIM // kv_local
    late = me % 2 == 1
    old_late = jnp.where(me < 2, me % 2 == 0, late)
    has_old = me != 1
    rows = lax.broadcasted_iota(jnp.int32, (group * blk, blk), 0) % blk
    cols = lax.broadcasted_iota(jnp.int32, (group * blk, blk), 1)
    own_ok = cols <= rows
    far_ok = cols > rows
    near_ok = cols >= 0
    factor = math.log2(math.e) / math.sqrt(HDIM)

    def pick(keep_ref, got_ref, swapped, column):
        at = slice(column * HDIM, (column + 1) * HDIM)
        keep, got = keep_ref[:, at], got_ref[:, at]
        return jnp.where(swapped, got, keep), jnp.where(swapped, keep, got)

    squares = [jnp.zeros((blk, 1), F32)] * 2
    for g in range(kv_local):
        keys = pick(old_keep_ref, old_got_ref, old_late, g) + pick(kv_keep_ref, kv_got_ref, late, g)
        c = kv_local + g
        vals = pick(old_keep_ref, old_got_ref, old_late, c) + pick(kv_keep_ref, kv_got_ref, late, c)
        heads = [pick(q_keep_ref, q_got_ref, late, g * group + i) for i in range(group)]
        for part in range(2):
            query = jnp.concatenate([h[part] for h in heads], 0)
            score = dot(query, jnp.concatenate(keys[part : part + 3], 0), (1, 1))
            ok = (
                [far_ok & has_old, near_ok & has_old, own_ok]
                if part == 0
                else [far_ok & has_old, near_ok, own_ok]
            )
            score = jnp.where(jnp.concatenate(ok, 1), score, -jnp.inf)
            peak = jnp.max(score, axis=1, keepdims=True)
            terms = jnp.exp2((score - peak) * factor)
            total = jnp.sum(terms, axis=1, keepdims=True)
            values = jnp.concatenate(vals[part : part + 3], 0)
            result = (dot(terms.astype(BF16), values) / total).astype(BF16)
            wide = result.astype(F32)
            square = jnp.sum(wide * wide, axis=1, keepdims=True)
            for i in range(group):
                at = slice((g * group + i) * HDIM, (g * group + i + 1) * HDIM)
                out_ref[part * blk : (part + 1) * blk, at] = result[i * blk : (i + 1) * blk]
                squares[part] = squares[part] + square[i * blk : (i + 1) * blk]
    for part in range(2):
        turned = jnp.transpose(jnp.broadcast_to(squares[part], (blk, blk)))
        sums_ref[part * 8 : part * 8 + 8] = turned[:8]


def home_kernel(rows_ref, sums_ref, gain_ref, bw_ref, x_ref, keep_ref, send_ref):
    mine = lax.axis_index("seq") % 2
    toks, feat = rows_ref.shape
    blk = toks // 2
    pairs = feat // HDIM
    gain = gain_ref[...]
    for part in range(2):
        at = slice(part * blk, (part + 1) * blk)
        sums = sums_ref[part * 8 : part * 8 + 1]
        mean = jnp.transpose(jnp.broadcast_to(sums, (blk, blk))) / (HEADS * HDIM)
        inv = lax.rsqrt(mean + 1e-06)[:, :1]
        x_ref[at, :] = (rows_ref[at, :].astype(F32) * gain * inv).astype(BF16)
    lanes = lax.broadcasted_iota(jnp.int32, (toks, HDIM), 1)
    zero = jnp.zeros((toks, HDIM), BF16)
    for p in range(pairs):
        x = x_ref[:, p * HDIM : (p + 1) * HDIM]
        spread = jnp.concatenate([jnp.where(lanes < SDIM, x, zero), jnp.where(lanes < SDIM, zero, x)], 0)
        state = dot(bw_ref[p], spread)
        side = 0 if p < pairs // 2 else 1
        at = (p % (pairs // 2)) * HDIM

        @pl.when(mine == side)
        def _():
            keep_ref[:, at : at + HDIM] = state

        @pl.when(mine != side)
        def _():
            send_ref[:, at : at + HDIM] = state.astype(BF16)


def local_kernel(x_ref, mix_ref, skip_ref, out_ref):
    toks, feat = x_ref.shape
    lanes = lax.broadcasted_iota(jnp.int32, (toks, HDIM), 1)
    zero = jnp.zeros((toks, HDIM), BF16)
    for p in range(feat // HDIM):
        at = slice(p * HDIM, (p + 1) * HDIM)
        x = x_ref[:, at]
        spread = jnp.concatenate([jnp.where(lanes < SDIM, x, zero), jnp.where(lanes < SDIM, zero, x)], 0)
        out_ref[:, at] = dot(mix_ref[p], spread) + skip_ref[:, at] * x.astype(F32)


def final_kernel(local_ref, scale_ref, c_ref, own_ref, other_ref, out_ref):
    mine = lax.axis_index("seq") % 2
    half = own_ref.shape[1]
    for ref, side in ((own_ref, mine), (other_ref, 1 - mine)):
        at = pl.ds(pl.multiple_of(side * half, half), half)
        part = dot(c_ref[...], ref[...])
        out_ref[:, at] = (local_ref[:, at] + part * scale_ref[:, at]).astype(BF16)


def add_kernel(a_ref, b_ref, out_ref):
    out_ref[...] = a_ref[...] + b_ref[...]


def half_of(ref, side):
    half = ref.shape[1] // 2
    return ref[:, pl.ds(pl.multiple_of(side * half, half), half)]


def decay_kernel(tot_ref, core_ref, out_ref):
    mine = lax.axis_index("seq") % 2
    out_ref[...] = half_of(tot_ref, mine) * half_of(core_ref, mine)


def times_kernel(a_ref, b_ref, out_ref):
    out_ref[...] = a_ref[...] * b_ref[...]


def chip_kernel(keep_ref, got_ref, tot_ref, core_ref, early_ref, total_ref, low_ref):
    mine = lax.axis_index("seq") % 2
    late = mine == 1
    keep, got = keep_ref[...], got_ref[...].astype(F32)
    second = jnp.where(late, half_of(tot_ref, mine), half_of(core_ref, mine))
    early = jnp.where(late, got, keep)
    total = second * early + jnp.where(late, keep, got)
    early_ref[...] = early
    total_ref[...] = total
    low_ref[...] = total.astype(BF16)


def stage_kernel(bit, first, total_ref, theirs_ref, mine_ref, decay_ref, *refs):
    upper = (lax.axis_index("seq") >> bit) % 2 == 1
    enter_ref, carried_ref, low_ref, next_ref = refs[-4:]
    theirs, decay, total = theirs_ref[...].astype(F32), decay_ref[...], total_ref[...]
    if first:
        enter_ref[...] = jnp.where(upper, theirs, 0.0)
        carried_ref[...] = jnp.where(upper, decay, 1.0)
    else:
        carried = refs[1][...]
        enter_ref[...] = refs[0][...] + jnp.where(upper, carried * theirs, 0.0)
        carried_ref[...] = jnp.where(upper, carried * decay, carried)
    total = jnp.where(upper, mine_ref[...] * theirs + total, decay * total + theirs)
    low_ref[...] = total.astype(BF16)
    next_ref[...] = total


def middle_kernel(shift, total_ref, first_ref, mine_ref, near_ref, low_ref):
    me = lax.axis_index("seq")
    quarter, late = me >> shift, me % 2 == 1
    upper = quarter % 2 == 1
    mine, near = mine_ref[...], near_ref[...]
    one, zero = jnp.ones_like(mine), jnp.zeros_like(mine)
    theirs = jnp.where(
        late,
        jnp.where(upper, one, jnp.where(quarter == 2, mine * near, zero)),
        jnp.where(upper, mine, one),
    )
    own = jnp.where(late, jnp.where(upper, zero, one), jnp.where(upper, one, near))
    low_ref[...] = (theirs * first_ref[...].astype(F32) + own * total_ref[...]).astype(BF16)


def last_kernel(
    shift, first_ref, second_ref, near_ref, early_ref, tot_ref, core_ref, *refs
):
    own_ref, give_ref = refs[-2:]
    me = lax.axis_index("seq")
    side = me % 2
    quarter, late = me >> shift, side == 1
    near = near_ref[...]
    one, zero = jnp.ones_like(near), jnp.zeros_like(near)
    a = jnp.where(
        late,
        jnp.where(quarter >= 2, near, zero),
        jnp.where(quarter % 2 == 1, one, zero),
    )
    b = jnp.where(
        late,
        jnp.where(quarter >= 1, one, zero),
        jnp.where(quarter == 3, near, jnp.where(quarter == 2, one, zero)),
    )
    enter = a * first_ref[...].astype(F32) + b * second_ref[...].astype(F32)
    if len(refs) == 4:
        enter = refs[0][...] + refs[1][...] * enter
    ahead = jnp.where(late, half_of(core_ref, side), half_of(tot_ref, side))
    after = ahead * enter + early_ref[...]
    own_ref[...] = jnp.where(late, after, enter).astype(BF16)
    give_ref[...] = jnp.where(late, enter, after).astype(BF16)


def layer(query, keys, values, norm_gain, in_b, out_c, step, log_decay, skip):
    seq_count = lax.axis_size("seq")
    head_count = lax.axis_size("head")
    blk, feat = query.shape[1:]
    heads, toks = step.shape
    kv_width = keys.shape[2]
    pairs = heads // 2
    half = feat // 2
    every = range(seq_count)

    def swap(block, bit):
        return lax.ppermute(block, "seq", [(i, i ^ (1 << bit)) for i in every])

    width = 2 * kv_width
    kv_keep, q_keep, kv_send, q_send = call(
        pack_kernel,
        [((blk, width), BF16), ((blk, feat), BF16)] * 2,
        (query, keys, values),
        spaces=[pltpu.HBM] * 3,
    )
    chips = seq_count // 2
    onward = [(i, i + 2) for i in range(seq_count - 2)] + [(seq_count - 2, 1), (seq_count - 1, 0)]
    kv_got = swap(kv_send, 0)
    old_keep = lax.ppermute(kv_keep, "seq", onward)
    old_got = lax.ppermute(kv_got, "seq", onward)
    q_got = swap(q_send, 0)

    mix, b_weighted, scale, tot, skip_row = call(
        prepare_kernel,
        [
            ((pairs, toks, 2 * toks), BF16),
            ((pairs, STATE, 2 * toks), BF16),
            ((toks, feat), F32),
            ((1, feat), F32),
            ((1, feat), F32),
        ],
        (step, log_decay, in_b, out_c, skip),
        flops=1 << 30,
        spaces=[pltpu.HBM] * 5,
    )
    bits = seq_count.bit_length() - 1
    core = swap(tot, 0)
    (chip,) = call(decay_kernel, [((1, half), F32)], (tot, core))

    attended, sums = call(
        attention_kernel,
        [((toks, feat), BF16), ((16, blk), F32)],
        (q_keep, q_got, kv_keep, kv_got, old_keep, old_got),
        flops=1 << 29,
    )
    to_home = [(i, i // 2 + (1 - i % 2) * chips) for i in every]
    sums = lax.ppermute(sums, "seq", to_home)
    rows = lax.ppermute(attended, "seq", to_home)
    for bit in range(head_count.bit_length() - 1):
        other = lax.ppermute(sums, "head", [(i, i ^ (1 << bit)) for i in range(head_count)])
        (sums,) = call(add_kernel, [((16, blk), F32)], (sums, other))
    decays = []
    running = chip
    for bit in range(1, bits - 2):
        theirs = swap(running, bit)
        decays.append((running, theirs))
        (running,) = call(times_kernel, [((1, half), F32)], (running, theirs))
    inner, outer = bits - 2, bits - 1
    near = lax.ppermute(
        running,
        "seq",
        [(i, (i + (1 << inner)) % seq_count if i % 2 else i ^ (1 << inner)) for i in every],
    )

    x, keep, send = call(
        home_kernel,
        [((toks, feat), BF16), ((STATE, half), F32), ((STATE, half), BF16)],
        (rows, sums, norm_gain[None, :], b_weighted),
        flops=1 << 28,
    )
    (local,) = call(local_kernel, [((toks, feat), F32)], (x, mix, skip_row), flops=1 << 29)
    got = swap(send, 0)
    state = ((STATE, half), F32)
    row = ((1, half), F32)
    early, total, low = call(
        chip_kernel, [state, state, ((STATE, half), BF16)], (keep, got, tot, core)
    )
    entered = ()
    for bit in range(1, bits - 2):
        theirs = swap(low, bit)
        *entered, low, total = call(
            functools.partial(stage_kernel, bit, bit == 1),
            [state, row, ((STATE, half), BF16), state],
            (total, theirs, *decays[bit - 1], *entered),
        )
    by_core = [[(i, i ^ (1 << (outer if i % 2 == turn else inner))) for i in every] for turn in (1, 0)]
    first = lax.ppermute(low, "seq", by_core[0])
    (low,) = call(
        functools.partial(middle_kernel, inner),
        [((STATE, half), BF16)],
        (total, first, running, near),
    )
    second = lax.ppermute(low, "seq", by_core[1])
    own, give = call(
        functools.partial(last_kernel, inner),
        [((STATE, half), BF16)] * 2,
        (first, second, near, early, tot, core, *entered),
    )
    other = swap(give, 0)
    (out,) = call(
        final_kernel, [((toks, feat), BF16)], (local, scale, out_c, own, other), flops=1 << 28
    )
    return out


def solution(mesh):
    placed = (
        P(None, "seq", "head"),
        P(None, "seq", "head"),
        P(None, "seq", "head"),
        P("head"),
        P("seq", None),
        P("seq", None),
        P("head", "seq"),
        P("head", "seq"),
        P("head"),
    )
    return jax.shard_map(
        layer, mesh=mesh, in_specs=placed, out_specs=P("seq", "head"), check_vma=False
    )
```

```python
import functools
import math

import jax
import jax.numpy as jnp
from jax import lax
from jax.experimental import pallas as pl
from jax.experimental.pallas import tpu as pltpu
from jax.sharding import PartitionSpec as P


HEADS = 32
HDIM = 128
SDIM = 64
STATE = 128
TAIL = 16

F32 = jnp.float32
BF16 = jnp.bfloat16
VMEM = pltpu.VMEM
GRANT = 12 << 20


def dot(a, b, contract=(1, 0), precision=None):
    return lax.dot_general(
        a,
        b,
        (((contract[0],), (contract[1],)), ((), ())),
        precision=precision,
        preferred_element_type=F32,
    )


def call(kernel, outs, args, flops=1, spaces=None):
    spaces = spaces or [VMEM] * len(args)
    return pl.pallas_call(
        kernel,
        out_shape=[jax.ShapeDtypeStruct(s, d) for s, d in outs],
        in_specs=[pl.BlockSpec(memory_space=m) for m in spaces],
        out_specs=[pl.BlockSpec(memory_space=VMEM)] * len(outs),
        compiler_params=pltpu.CompilerParams(vmem_limit_bytes=GRANT),
        cost_estimate=pl.CostEstimate(flops=flops, bytes_accessed=1 << 20, transcendentals=0),
    )(*[pltpu.with_memory_space_constraint(a, m) if m == pltpu.HBM else a for a, m in zip(args, spaces)])


def gather(copies, sems):
    started = [pltpu.make_async_copy(a, b, sems.at[i]) for i, (a, b) in enumerate(copies)]
    for copy in started:
        copy.start()
    for copy in started:
        copy.wait()


def part_kernel(kv_ref, k_ref, v_ref):
    width = k_ref.shape[1]
    k_ref[...] = kv_ref[:, :width]
    v_ref[...] = kv_ref[:, width:]


def pack_kv_kernel(k_ref, v_ref, keep_ref, send_ref):
    width = k_ref.shape[2]
    mine = lax.axis_index("seq") % 2
    copies = []
    for slot, out_ref in ((1 - mine, keep_ref), (mine, send_ref)):
        copies.append((k_ref.at[slot], out_ref.at[:, :width]))
        copies.append((v_ref.at[slot], out_ref.at[:, width:]))
    pl.run_scoped(functools.partial(gather, copies), pltpu.SemaphoreType.DMA((4,)))


def pack_q_kernel(q_ref, keep_ref, send_ref):
    mine = lax.axis_index("seq") % 2
    copies = [(q_ref.at[1 - mine], keep_ref), (q_ref.at[mine], send_ref)]
    pl.run_scoped(functools.partial(gather, copies), pltpu.SemaphoreType.DMA((2,)))


def prepare_kernel(*refs):
    def inner(sems, *inside):
        copies = [
            pltpu.make_async_copy(src, dst, sems.at[i])
            for i, (src, dst) in enumerate(zip(refs[:5], inside))
        ]
        for copy in copies:
            copy.start()
        for copy in copies:
            copy.wait()
        prepare(*inside, *refs[5:])

    pl.run_scoped(
        inner,
        pltpu.SemaphoreType.DMA((5,)),
        *[VMEM(r.shape, r.dtype) for r in refs[:4]],
        pltpu.SMEM(refs[4].shape, refs[4].dtype),
    )


def prepare(step_ref, log_ref, b_ref, c_ref, skip_ref, mix_ref, bw_ref, scale_ref, tot_ref, pass_ref):
    heads, toks = step_ref.shape
    half = toks // 2
    highest = lax.Precision.HIGHEST
    log = log_ref[...]
    step = step_ref[...]
    rows = lax.broadcasted_iota(jnp.int32, (toks, toks), 0)
    cols = lax.broadcasted_iota(jnp.int32, (toks, toks), 1)
    lower = (rows >= cols).astype(F32)
    cum = dot(log, lower, (1, 1), highest)
    cum_cols = dot(lower, log, (1, 1), highest)
    total = cum[:, toks - 1 :]
    weight = jnp.exp(total - cum) * step
    cross = dot(c_ref[...], b_ref[...], (1, 1))
    b_t = jnp.transpose(b_ref[...].astype(F32))
    causal = (
        lax.broadcasted_iota(jnp.int32, (half, half), 0)
        >= lax.broadcasted_iota(jnp.int32, (half, half), 1)
    )
    lanes = lax.broadcasted_iota(jnp.int32, (toks, HDIM), 1)
    for pair in range(heads // 2):
        for side in range(2):
            k = 2 * pair + side
            at = side * toks
            for r in range(2):
                for c in range(2):
                    dst = (pair, slice(r * half, (r + 1) * half), slice(at + c * half, at + (c + 1) * half))
                    if c > r:
                        mix_ref[dst] = jnp.zeros((half, half), BF16)
                        continue
                    rs, cs = slice(r * half, (r + 1) * half), slice(c * half, (c + 1) * half)
                    gap = cum_cols[rs, k : k + 1] - cum[k : k + 1, cs]
                    if r == c:
                        gap = jnp.where(causal, gap, -jnp.inf)
                    mix_ref[dst] = (jnp.exp(gap) * cross[rs, cs] * step[k : k + 1, cs]).astype(BF16)
            bw_ref[pair, :, at : at + toks] = (b_t * weight[k : k + 1, :]).astype(BF16)
        both = jnp.where(
            lanes < SDIM,
            cum_cols[:, 2 * pair : 2 * pair + 1],
            cum_cols[:, 2 * pair + 1 : 2 * pair + 2],
        )
        both = jnp.exp(both)
        scale_ref[:, pair * HDIM : (pair + 1) * HDIM] = both
        tot_ref[:, pair * HDIM : (pair + 1) * HDIM] = both[toks - 1 :, :]
        pass_ref[:, pair * HDIM : (pair + 1) * HDIM] = jnp.where(
            lanes[:1] < SDIM, skip_ref[2 * pair], skip_ref[2 * pair + 1]
        )


def pick(keep_ref, got_ref, swapped, column, got_column=None):
    keep, got = [
        ref[:, c * HDIM : (c + 1) * HDIM]
        for ref, c in ((keep_ref, column), (got_ref, column if got_column is None else got_column))
    ]
    return jnp.where(swapped, got, keep), jnp.where(swapped, keep, got)


def places():
    me = lax.axis_index("seq")
    late = me % 2 == 1
    return late, jnp.where(me < 2, me % 2 == 0, late), me != 1


def score_kernel(
    q_keep_ref, q_got_ref, kv_keep_ref, kv_got_ref, old_keep_ref, old_got_ref, weight_ref, scale_ref
):
    blk, feat = q_keep_ref.shape
    kv_local = kv_keep_ref.shape[1] // (2 * HDIM)
    group = feat // HDIM // kv_local
    late, old_late, has_old = places()
    rows = lax.broadcasted_iota(jnp.int32, (group * blk, blk), 0) % blk
    cols = lax.broadcasted_iota(jnp.int32, (group * blk, blk), 1)
    own_ok = cols <= rows
    far_ok = (cols > rows) & has_old
    near_ok = (cols >= 0) & has_old
    factor = math.log2(math.e) / math.sqrt(HDIM)
    for g in range(kv_local):
        keys = pick(old_keep_ref, old_got_ref, old_late, g) + pick(kv_keep_ref, kv_got_ref, late, g)
        heads = [pick(q_keep_ref, q_got_ref, late, g * group + i) for i in range(group)]
        for part in range(2):
            query = jnp.concatenate([h[part] for h in heads], 0)
            score = dot(query, jnp.concatenate(keys[part : part + 3], 0), (1, 1))
            near = score[:, blk : 2 * blk]
            if part == 0:
                near = jnp.where(near_ok, near, -jnp.inf)
            far = jnp.where(far_ok, score[:, :blk], -jnp.inf)
            score = jnp.concatenate([far, near, jnp.where(own_ok, score[:, 2 * blk :], -jnp.inf)], 1)
            peak = jnp.max(score, axis=1, keepdims=True)
            terms = jnp.exp2((score - peak) * factor)
            total = pl.reciprocal(jnp.sum(terms, axis=1, keepdims=True))
            weight_ref[2 * g + part] = terms.astype(BF16)
            scale_ref[2 * g + part] = jnp.broadcast_to(total, (group * blk, HDIM))


def value_kernel(
    weight_ref, scale_ref, kv_keep_ref, kv_got_ref, old_keep_ref, old_got_ref, out_ref, sums_ref
):
    blk = kv_keep_ref.shape[0]
    kv_local = kv_keep_ref.shape[1] // (2 * HDIM)
    group = out_ref.shape[1] // HDIM // kv_local
    late, old_late, _ = places()
    squares = [jnp.zeros((blk, 1), F32)] * 2
    for g in range(kv_local):
        c = kv_local + g
        vals = pick(old_keep_ref, old_got_ref, old_late, c, g) + pick(kv_keep_ref, kv_got_ref, late, c)
        for part in range(2):
            values = jnp.concatenate(vals[part : part + 3], 0)
            result = dot(weight_ref[2 * g + part], values) * scale_ref[2 * g + part]
            result = result.astype(BF16)
            wide = result.astype(F32)
            square = jnp.sum(wide * wide, axis=1, keepdims=True)
            for i in range(group):
                at = slice((g * group + i) * HDIM, (g * group + i + 1) * HDIM)
                out_ref[part * blk : (part + 1) * blk, at] = result[i * blk : (i + 1) * blk]
                squares[part] = squares[part] + square[i * blk : (i + 1) * blk]
    for part in range(2):
        turned = jnp.transpose(jnp.broadcast_to(squares[part], (blk, blk)))
        sums_ref[part * 8 : part * 8 + 8] = turned[:8]


def spread(x):
    lanes = lax.broadcasted_iota(jnp.int32, x.shape, 1)
    zero = jnp.zeros_like(x)
    return jnp.concatenate([jnp.where(lanes < SDIM, x, zero), jnp.where(lanes < SDIM, zero, x)], 0)


def pack_state(ref, state, decay, at=slice(None)):
    ref[:STATE, at] = state.astype(BF16)
    high = decay.astype(BF16).astype(F32)
    row = lax.broadcasted_iota(jnp.int32, (TAIL, decay.shape[1]), 0)
    ref[STATE:, at] = jnp.where(row == 0, high, decay - high).astype(BF16)


def unpack_state(ref):
    tail = ref[STATE:].astype(F32)
    return ref[:STATE].astype(F32), tail[:1] + tail[1:2]


def home_kernel(keeps, rows_ref, sums_ref, gain_ref, bw_ref, tot_ref, x_ref, state_ref):
    mine = lax.axis_index("seq") % 2
    side = mine if keeps else 1 - mine
    toks, half = x_ref.shape
    blk = toks // 2
    pairs = half // HDIM
    lanes = pl.ds(pl.multiple_of(side * half, half), half)
    gain = gain_ref[:, lanes]
    for part in range(2):
        at = slice(part * blk, (part + 1) * blk)
        sums = sums_ref[part * 8 : part * 8 + 1]
        mean = jnp.transpose(jnp.broadcast_to(sums, (blk, blk))) / (HEADS * HDIM)
        inv = lax.rsqrt(mean + 1e-06)[:, :1]
        x_ref[at, :] = (rows_ref[at, lanes].astype(F32) * gain * inv).astype(BF16)
    for p in range(pairs):
        at = slice(p * HDIM, (p + 1) * HDIM)
        state = dot(bw_ref[side * pairs + p], spread(x_ref[:, at]))
        if keeps:
            state_ref[:, at] = state
        else:
            decay = tot_ref[:, pl.ds(pl.multiple_of(side * half + p * HDIM, HDIM), HDIM)]
            pack_state(state_ref, state, decay, at)


def local_kernel(x_keep_ref, x_send_ref, mix_ref, skip_ref, keep_ref, send_ref):
    mine = lax.axis_index("seq") % 2
    half = x_keep_ref.shape[1]
    pairs = half // HDIM
    for x_ref, out_ref, side in ((x_keep_ref, keep_ref, mine), (x_send_ref, send_ref, 1 - mine)):
        skip = skip_ref[:, pl.ds(pl.multiple_of(side * half, half), half)]
        for p in range(pairs):
            at = slice(p * HDIM, (p + 1) * HDIM)
            x = x_ref[:, at]
            out_ref[:, at] = dot(mix_ref[side * pairs + p], spread(x)) + skip[:, at] * x.astype(F32)


def final_kernel(keep_ref, send_ref, scale_ref, c_ref, own_ref, other_ref, out_ref):
    mine = lax.axis_index("seq") % 2
    half = keep_ref.shape[1]
    for local_ref, enter_ref, side in ((keep_ref, own_ref, mine), (send_ref, other_ref, 1 - mine)):
        lanes = pl.ds(pl.multiple_of(side * half, half), half)
        part = dot(c_ref[...], enter_ref[...])
        out_ref[:, lanes] = (local_ref[...] + part * scale_ref[:, lanes]).astype(BF16)


def add_kernel(a_ref, b_ref, out_ref):
    out_ref[...] = a_ref[...] + b_ref[...]


def half_of(ref, side):
    half = ref.shape[1] // 2
    return ref[:, pl.ds(pl.multiple_of(side * half, half), half)]


def chip_kernel(keep_ref, got_ref, tot_ref, early_ref, ahead_ref, low_ref, *refs):
    mine = lax.axis_index("seq") % 2
    late = mine == 1
    keep, here = keep_ref[...], half_of(tot_ref, mine)
    got, there = unpack_state(got_ref)
    early = jnp.where(late, got, keep)
    total = jnp.where(late, here, there) * early + jnp.where(late, keep, got)
    early_ref[...] = early
    ahead_ref[...] = jnp.where(late, there, here)
    pack_state(low_ref, total, here * there)
    if refs:
        refs[0][...] = total
        refs[1][...] = here * there


def stage_kernel(bit, first, total_ref, mine_ref, theirs_ref, *refs):
    upper = (lax.axis_index("seq") >> bit) % 2 == 1
    enter_ref, carried_ref, low_ref, next_ref, running_ref = refs[-5:]
    theirs, decay = unpack_state(theirs_ref)
    total, mine = total_ref[...], mine_ref[...]
    if first:
        enter_ref[...] = jnp.where(upper, theirs, 0.0)
        carried_ref[...] = jnp.where(upper, decay, 1.0)
    else:
        carried = refs[1][...]
        enter_ref[...] = refs[0][...] + jnp.where(upper, carried * theirs, 0.0)
        carried_ref[...] = jnp.where(upper, carried * decay, carried)
    total = jnp.where(upper, mine * theirs + total, decay * total + theirs)
    pack_state(low_ref, total, mine * decay)
    next_ref[...] = total
    running_ref[...] = mine * decay


def last_kernel(shift, inner_ref, outer_ref, both_ref, early_ref, ahead_ref, *refs):
    own_ref, give_ref = refs[-2:]
    me = lax.axis_index("seq")
    quarter, late = me >> shift, me % 2 == 1
    beside, by_inner = unpack_state(inner_ref)
    across, by_outer = unpack_state(outer_ref)
    diagonal, by_both = unpack_state(both_ref)
    one, zero = jnp.ones_like(by_inner), jnp.zeros_like(by_inner)

    def by_quarter(second, third, fourth):
        last = jnp.where(quarter == 3, fourth, zero)
        return jnp.where(quarter == 1, second, jnp.where(quarter == 2, third, last))

    enter = by_quarter(one, zero, one) * beside
    enter = enter + by_quarter(zero, by_both, by_inner) * across
    enter = enter + by_quarter(zero, one, by_inner * by_outer) * diagonal
    if len(refs) == 4:
        enter = refs[0][...] + refs[1][...] * enter
    after = ahead_ref[...] * enter + early_ref[...]
    own_ref[...] = jnp.where(late, after, enter).astype(BF16)
    give_ref[...] = jnp.where(late, enter, after).astype(BF16)


def layer(query, keys, values, norm_gain, in_b, out_c, step, log_decay, skip):
    seq_count = lax.axis_size("seq")
    head_count = lax.axis_size("head")
    blk, feat = query.shape[1:]
    heads, toks = step.shape
    kv_width = keys.shape[2]
    pairs = heads // 2
    half = feat // 2
    every = range(seq_count)

    def swap(block, bit):
        return lax.ppermute(block, "seq", [(i, i ^ (1 << bit)) for i in every])

    width = 2 * kv_width
    kv_keep, kv_send = call(
        pack_kv_kernel, [((blk, width), BF16)] * 2, (keys, values), spaces=[pltpu.HBM] * 2
    )
    q_keep, q_send = call(pack_q_kernel, [((blk, feat), BF16)] * 2, (query,), spaces=[pltpu.HBM])
    chips = seq_count // 2
    onward = [(i, i + 2) for i in range(seq_count - 2)] + [(seq_count - 2, 1), (seq_count - 1, 0)]
    kv_got = swap(kv_send, 0)
    old_keep = lax.ppermute(kv_keep, "seq", onward)
    got_k, got_v = call(part_kernel, [((blk, kv_width), BF16)] * 2, (kv_got,))
    old_k = lax.ppermute(got_k, "seq", onward)
    old_v = lax.ppermute(got_v, "seq", onward)
    q_got = swap(q_send, 0)

    mix, b_weighted, scale, tot, skip_row = call(
        prepare_kernel,
        [
            ((pairs, toks, 2 * toks), BF16),
            ((pairs, STATE, 2 * toks), BF16),
            ((toks, feat), F32),
            ((1, feat), F32),
            ((1, feat), F32),
        ],
        (step, log_decay, in_b, out_c, skip),
        flops=1 << 30,
        spaces=[pltpu.HBM] * 5,
    )
    bits = seq_count.bit_length() - 1
    rows_at_once = feat // kv_width * blk
    weights, scales = call(
        score_kernel,
        [((2 * kv_width // HDIM, rows_at_once, 3 * blk), BF16), ((2 * kv_width // HDIM, rows_at_once, HDIM), F32)],
        (q_keep, q_got, kv_keep, kv_got, old_keep, old_k),
        flops=1 << 28,
    )
    attended, sums = call(
        value_kernel,
        [((toks, feat), BF16), ((16, blk), F32)],
        (weights, scales, kv_keep, kv_got, old_keep, old_v),
        flops=1 << 28,
    )
    to_home = [(i, i // 2 + (1 - i % 2) * chips) for i in every]
    rows = lax.ppermute(attended, "seq", to_home)
    for bit in range(head_count.bit_length() - 1):
        other = lax.ppermute(sums, "head", [(i, i ^ (1 << bit)) for i in range(head_count)])
        (sums,) = call(add_kernel, [((16, blk), F32)], (sums, other))
    sums = lax.ppermute(sums, "seq", to_home)
    quarter = 1 << (bits - 2)

    def exchange(block, flip):
        return lax.ppermute(block, "seq", [(i, i ^ (flip * quarter)) for i in every])

    gain = norm_gain[None, :]
    state, row, packed = ((STATE, half), F32), ((1, half), F32), ((STATE + TAIL, half), BF16)
    x_send, send = call(
        functools.partial(home_kernel, False),
        [((toks, half), BF16), packed],
        (rows, sums, gain, b_weighted, tot),
        flops=1 << 27,
    )
    x_keep, keep = call(
        functools.partial(home_kernel, True),
        [((toks, half), BF16), state],
        (rows, sums, gain, b_weighted, tot),
        flops=1 << 27,
    )
    local_keep, local_send = call(
        local_kernel, [((toks, half), F32)] * 2, (x_keep, x_send, mix, skip_row), flops=1 << 29
    )
    got = swap(send, 0)
    stages = range(1, bits - 2)
    early, ahead, low, *held = call(
        chip_kernel, [state, row, packed] + [state, row] * bool(stages), (keep, got, tot)
    )
    entered = ()
    for bit in stages:
        theirs = swap(low, bit)
        *entered, low, total, running = call(
            functools.partial(stage_kernel, bit, bit == 1),
            [state, row, packed, state, row],
            (*held, theirs, *entered),
        )
        held = (total, running)
    both = exchange(low, 3)
    inner = exchange(low, 1)
    outer = exchange(low, 2)
    own, give = call(
        functools.partial(last_kernel, bits - 2),
        [((STATE, half), BF16)] * 2,
        (inner, outer, both, early, ahead, *entered),
    )
    other = swap(give, 0)
    (out,) = call(
        final_kernel,
        [((toks, feat), BF16)],
        (local_keep, local_send, scale, out_c, own, other),
        flops=1 << 28,
    )
    return out


def solution(mesh):
    placed = (
        P(None, "seq", "head"),
        P(None, "seq", "head"),
        P(None, "seq", "head"),
        P("head"),
        P("seq", None),
        P("seq", None),
        P("head", "seq"),
        P("head", "seq"),
        P("head"),
    )
    return jax.shard_map(
        layer, mesh=mesh, in_specs=placed, out_specs=P("seq", "head"), check_vma=False
    )
```

```python
import functools
import math

import jax
import jax.numpy as jnp
from jax import lax
from jax.experimental import pallas as pl
from jax.experimental.pallas import tpu as pltpu
from jax.sharding import PartitionSpec as P


HEADS = 32
HDIM = 128
SDIM = 64
STATE = 128
TAIL = 16

F32 = jnp.float32
BF16 = jnp.bfloat16
VMEM = pltpu.VMEM
GRANT = 12 << 20


def dot(a, b, contract=(1, 0), precision=None):
    return lax.dot_general(
        a,
        b,
        (((contract[0],), (contract[1],)), ((), ())),
        precision=precision,
        preferred_element_type=F32,
    )


def call(kernel, outs, args, flops=1, spaces=None):
    spaces = spaces or [VMEM] * len(args)
    return pl.pallas_call(
        kernel,
        out_shape=[jax.ShapeDtypeStruct(s, d) for s, d in outs],
        in_specs=[pl.BlockSpec(memory_space=m) for m in spaces],
        out_specs=[pl.BlockSpec(memory_space=VMEM)] * len(outs),
        compiler_params=pltpu.CompilerParams(vmem_limit_bytes=GRANT),
        cost_estimate=pl.CostEstimate(flops=flops, bytes_accessed=1 << 20, transcendentals=0),
    )(*[pltpu.with_memory_space_constraint(a, m) if m == pltpu.HBM else a for a, m in zip(args, spaces)])


def gather(copies, sems):
    started = [pltpu.make_async_copy(a, b, sems.at[i]) for i, (a, b) in enumerate(copies)]
    for copy in started:
        copy.start()
    for copy in started:
        copy.wait()


def part_kernel(kv_ref, k_ref, v_ref):
    width = k_ref.shape[1]
    k_ref[...] = kv_ref[:, :width]
    v_ref[...] = kv_ref[:, width:]


def pack_kv_kernel(k_ref, v_ref, keep_ref, send_ref):
    width = k_ref.shape[2]
    mine = lax.axis_index("seq") % 2
    copies = []
    for slot, out_ref in ((1 - mine, keep_ref), (mine, send_ref)):
        copies.append((k_ref.at[slot], out_ref.at[:, :width]))
        copies.append((v_ref.at[slot], out_ref.at[:, width:]))
    pl.run_scoped(functools.partial(gather, copies), pltpu.SemaphoreType.DMA((4,)))


def pack_q_kernel(q_ref, keep_ref, send_ref):
    mine = lax.axis_index("seq") % 2
    copies = [(q_ref.at[1 - mine], keep_ref), (q_ref.at[mine], send_ref)]
    pl.run_scoped(functools.partial(gather, copies), pltpu.SemaphoreType.DMA((2,)))


def prepare_kernel(*refs):
    def inner(sems, *inside):
        copies = [
            pltpu.make_async_copy(src, dst, sems.at[i])
            for i, (src, dst) in enumerate(zip(refs[:5], inside))
        ]
        for copy in copies:
            copy.start()
        for copy in copies:
            copy.wait()
        prepare(*inside, *refs[5:])

    pl.run_scoped(
        inner,
        pltpu.SemaphoreType.DMA((5,)),
        *[VMEM(r.shape, r.dtype) for r in refs[:4]],
        pltpu.SMEM(refs[4].shape, refs[4].dtype),
    )


def prepare(step_ref, log_ref, b_ref, c_ref, skip_ref, mix_ref, bw_ref, scale_ref, tot_ref, pass_ref):
    heads, toks = step_ref.shape
    half = toks // 2
    highest = lax.Precision.HIGHEST
    log = log_ref[...]
    step = step_ref[...]
    rows = lax.broadcasted_iota(jnp.int32, (toks, toks), 0)
    cols = lax.broadcasted_iota(jnp.int32, (toks, toks), 1)
    lower = (rows >= cols).astype(F32)
    cum = dot(log, lower, (1, 1), highest)
    cum_cols = dot(lower, log, (1, 1), highest)
    total = cum[:, toks - 1 :]
    weight = jnp.exp(total - cum) * step
    cross = dot(c_ref[...], b_ref[...], (1, 1))
    b_t = jnp.transpose(b_ref[...].astype(F32))
    causal = (
        lax.broadcasted_iota(jnp.int32, (half, half), 0)
        >= lax.broadcasted_iota(jnp.int32, (half, half), 1)
    )
    lanes = lax.broadcasted_iota(jnp.int32, (toks, HDIM), 1)
    for pair in range(heads // 2):
        for side in range(2):
            k = 2 * pair + side
            at = side * toks
            for r in range(2):
                for c in range(2):
                    dst = (pair, slice(r * half, (r + 1) * half), slice(at + c * half, at + (c + 1) * half))
                    if c > r:
                        mix_ref[dst] = jnp.zeros((half, half), BF16)
                        continue
                    rs, cs = slice(r * half, (r + 1) * half), slice(c * half, (c + 1) * half)
                    gap = cum_cols[rs, k : k + 1] - cum[k : k + 1, cs]
                    if r == c:
                        gap = jnp.where(causal, gap, -jnp.inf)
                    mix_ref[dst] = (jnp.exp(gap) * cross[rs, cs] * step[k : k + 1, cs]).astype(BF16)
            bw_ref[pair, :, at : at + toks] = (b_t * weight[k : k + 1, :]).astype(BF16)
        both = jnp.where(
            lanes < SDIM,
            cum_cols[:, 2 * pair : 2 * pair + 1],
            cum_cols[:, 2 * pair + 1 : 2 * pair + 2],
        )
        both = jnp.exp(both)
        scale_ref[:, pair * HDIM : (pair + 1) * HDIM] = both
        tot_ref[:, pair * HDIM : (pair + 1) * HDIM] = both[toks - 1 :, :]
        pass_ref[:, pair * HDIM : (pair + 1) * HDIM] = jnp.where(
            lanes[:1] < SDIM, skip_ref[2 * pair], skip_ref[2 * pair + 1]
        )


def pick(keep_ref, got_ref, swapped, column, got_column=None):
    keep, got = [
        ref[:, c * HDIM : (c + 1) * HDIM]
        for ref, c in ((keep_ref, column), (got_ref, column if got_column is None else got_column))
    ]
    return jnp.where(swapped, got, keep), jnp.where(swapped, keep, got)


def places():
    me = lax.axis_index("seq")
    late = me % 2 == 1
    return late, jnp.where(me < 2, me % 2 == 0, late), me != 1


def score_kernel(
    q_keep_ref, q_got_ref, kv_keep_ref, kv_got_ref, old_keep_ref, old_got_ref, weight_ref, scale_ref
):
    blk, feat = q_keep_ref.shape
    kv_local = kv_keep_ref.shape[1] // (2 * HDIM)
    group = feat // HDIM // kv_local
    late, old_late, has_old = places()
    rows = lax.broadcasted_iota(jnp.int32, (group * blk, blk), 0) % blk
    cols = lax.broadcasted_iota(jnp.int32, (group * blk, blk), 1)
    own_ok = cols <= rows
    far_ok = (cols > rows) & has_old
    near_ok = (cols >= 0) & has_old
    factor = math.log2(math.e) / math.sqrt(HDIM)
    for g in range(kv_local):
        keys = pick(old_keep_ref, old_got_ref, old_late, g) + pick(kv_keep_ref, kv_got_ref, late, g)
        heads = [pick(q_keep_ref, q_got_ref, late, g * group + i) for i in range(group)]
        for part in range(2):
            query = jnp.concatenate([h[part] for h in heads], 0)
            score = dot(query, jnp.concatenate(keys[part : part + 3], 0), (1, 1))
            near = score[:, blk : 2 * blk]
            if part == 0:
                near = jnp.where(near_ok, near, -jnp.inf)
            far = jnp.where(far_ok, score[:, :blk], -jnp.inf)
            score = jnp.concatenate([far, near, jnp.where(own_ok, score[:, 2 * blk :], -jnp.inf)], 1)
            peak = jnp.max(score, axis=1, keepdims=True)
            terms = jnp.exp2((score - peak) * factor)
            total = pl.reciprocal(jnp.sum(terms, axis=1, keepdims=True))
            weight_ref[2 * g + part] = terms.astype(BF16)
            scale_ref[2 * g + part] = jnp.broadcast_to(total, (group * blk, HDIM))


def value_kernel(
    weight_ref, scale_ref, kv_keep_ref, kv_got_ref, old_keep_ref, old_got_ref, out_ref, sums_ref
):
    blk = kv_keep_ref.shape[0]
    kv_local = kv_keep_ref.shape[1] // (2 * HDIM)
    group = out_ref.shape[1] // HDIM // kv_local
    late, old_late, _ = places()
    squares = [jnp.zeros((blk, 1), F32)] * 2
    for g in range(kv_local):
        c = kv_local + g
        vals = pick(old_keep_ref, old_got_ref, old_late, c, g) + pick(kv_keep_ref, kv_got_ref, late, c)
        for part in range(2):
            values = jnp.concatenate(vals[part : part + 3], 0)
            result = dot(weight_ref[2 * g + part], values) * scale_ref[2 * g + part]
            result = result.astype(BF16)
            wide = result.astype(F32)
            square = jnp.sum(wide * wide, axis=1, keepdims=True)
            for i in range(group):
                at = slice((g * group + i) * HDIM, (g * group + i + 1) * HDIM)
                out_ref[part * blk : (part + 1) * blk, at] = result[i * blk : (i + 1) * blk]
                squares[part] = squares[part] + square[i * blk : (i + 1) * blk]
    for part in range(2):
        turned = jnp.transpose(jnp.broadcast_to(squares[part], (blk, blk)))
        sums_ref[part * 8 : part * 8 + 8] = turned[:8]


def spread(x):
    lanes = lax.broadcasted_iota(jnp.int32, x.shape, 1)
    zero = jnp.zeros_like(x)
    return jnp.concatenate([jnp.where(lanes < SDIM, x, zero), jnp.where(lanes < SDIM, zero, x)], 0)


def pack_state(ref, state, decay, at=slice(None)):
    ref[:STATE, at] = state.astype(BF16)
    high = decay.astype(BF16).astype(F32)
    row = lax.broadcasted_iota(jnp.int32, (TAIL, decay.shape[1]), 0)
    ref[STATE:, at] = jnp.where(row == 0, high, decay - high).astype(BF16)


def unpack_state(ref):
    tail = ref[STATE:].astype(F32)
    return ref[:STATE].astype(F32), tail[:1] + tail[1:2]


def home_kernel(keeps, rows_ref, sums_ref, gain_ref, bw_ref, tot_ref, x_ref, state_ref):
    mine = lax.axis_index("seq") % 2
    side = mine if keeps else 1 - mine
    toks, half = x_ref.shape
    blk = toks // 2
    pairs = half // HDIM
    lanes = pl.ds(pl.multiple_of(side * half, half), half)
    gain = gain_ref[:, lanes]
    for part in range(2):
        at = slice(part * blk, (part + 1) * blk)
        sums = sums_ref[part * 8 : part * 8 + 1]
        mean = jnp.transpose(jnp.broadcast_to(sums, (blk, blk))) / (HEADS * HDIM)
        inv = lax.rsqrt(mean + 1e-06)[:, :1]
        x_ref[at, :] = (rows_ref[at, lanes].astype(F32) * gain * inv).astype(BF16)
    for p in range(pairs):
        at = slice(p * HDIM, (p + 1) * HDIM)
        state = dot(bw_ref[side * pairs + p], spread(x_ref[:, at]))
        if keeps:
            state_ref[:, at] = state
        else:
            decay = tot_ref[:, pl.ds(pl.multiple_of(side * half + p * HDIM, HDIM), HDIM)]
            pack_state(state_ref, state, decay, at)


def local_kernel(x_keep_ref, x_send_ref, mix_ref, skip_ref, keep_ref, send_ref):
    mine = lax.axis_index("seq") % 2
    half = x_keep_ref.shape[1]
    pairs = half // HDIM
    for x_ref, out_ref, side in ((x_keep_ref, keep_ref, mine), (x_send_ref, send_ref, 1 - mine)):
        skip = skip_ref[:, pl.ds(pl.multiple_of(side * half, half), half)]
        for p in range(pairs):
            at = slice(p * HDIM, (p + 1) * HDIM)
            x = x_ref[:, at]
            out_ref[:, at] = dot(mix_ref[side * pairs + p], spread(x)) + skip[:, at] * x.astype(F32)


def finish_kernel(keeps, local_ref, scale_ref, c_ref, enter_ref, *refs):
    mine = lax.axis_index("seq") % 2
    half = local_ref.shape[1]
    side = mine if keeps else 1 - mine
    lanes = pl.ds(pl.multiple_of(side * half, half), half)
    out = local_ref[...] + dot(c_ref[...], enter_ref[...]) * scale_ref[:, lanes]
    if keeps:
        refs[0][...] = out.astype(BF16)
    else:
        own_ref, out_ref = refs
        out_ref[:, lanes] = out.astype(BF16)
        out_ref[:, pl.ds(pl.multiple_of(mine * half, half), half)] = own_ref[...]


def add_kernel(a_ref, b_ref, out_ref):
    out_ref[...] = a_ref[...] + b_ref[...]


def half_of(ref, side):
    half = ref.shape[1] // 2
    return ref[:, pl.ds(pl.multiple_of(side * half, half), half)]


def chip_kernel(keep_ref, got_ref, tot_ref, early_ref, ahead_ref, low_ref, *refs):
    mine = lax.axis_index("seq") % 2
    late = mine == 1
    keep, here = keep_ref[...], half_of(tot_ref, mine)
    got, there = unpack_state(got_ref)
    early = jnp.where(late, got, keep)
    total = jnp.where(late, here, there) * early + jnp.where(late, keep, got)
    early_ref[...] = early
    ahead_ref[...] = jnp.where(late, there, here)
    pack_state(low_ref, total, here * there)
    if refs:
        refs[0][...] = total
        refs[1][...] = here * there


def stage_kernel(bit, first, total_ref, mine_ref, theirs_ref, *refs):
    upper = (lax.axis_index("seq") >> bit) % 2 == 1
    enter_ref, carried_ref, low_ref, next_ref, running_ref = refs[-5:]
    theirs, decay = unpack_state(theirs_ref)
    total, mine = total_ref[...], mine_ref[...]
    if first:
        enter_ref[...] = jnp.where(upper, theirs, 0.0)
        carried_ref[...] = jnp.where(upper, decay, 1.0)
    else:
        carried = refs[1][...]
        enter_ref[...] = refs[0][...] + jnp.where(upper, carried * theirs, 0.0)
        carried_ref[...] = jnp.where(upper, carried * decay, carried)
    total = jnp.where(upper, mine * theirs + total, decay * total + theirs)
    pack_state(low_ref, total, mine * decay)
    next_ref[...] = total
    running_ref[...] = mine * decay


def last_kernel(shift, inner_ref, outer_ref, both_ref, early_ref, ahead_ref, *refs):
    own_ref, give_ref = refs[-2:]
    me = lax.axis_index("seq")
    quarter, late = me >> shift, me % 2 == 1
    beside, by_inner = unpack_state(inner_ref)
    across, by_outer = unpack_state(outer_ref)
    diagonal, _ = unpack_state(both_ref)
    third, fourth = quarter == 2, quarter == 3
    one, zero = jnp.ones_like(by_inner), jnp.zeros_like(by_inner)
    enter = jnp.where(quarter > 0, one, zero) * beside
    enter = enter + jnp.where(third | fourth, by_inner, zero) * across
    enter = enter + jnp.where(fourth, by_inner * by_outer, zero) * diagonal
    if len(refs) == 4:
        enter = refs[0][...] + refs[1][...] * enter
    after = ahead_ref[...] * enter + early_ref[...]
    own_ref[...] = jnp.where(late, after, enter).astype(BF16)
    give_ref[...] = jnp.where(late, enter, after).astype(BF16)


def layer(query, keys, values, norm_gain, in_b, out_c, step, log_decay, skip):
    seq_count = lax.axis_size("seq")
    head_count = lax.axis_size("head")
    blk, feat = query.shape[1:]
    heads, toks = step.shape
    kv_width = keys.shape[2]
    pairs = heads // 2
    half = feat // 2
    every = range(seq_count)

    def swap(block, bit):
        return lax.ppermute(block, "seq", [(i, i ^ (1 << bit)) for i in every])

    width = 2 * kv_width
    kv_keep, kv_send = call(
        pack_kv_kernel, [((blk, width), BF16)] * 2, (keys, values), spaces=[pltpu.HBM] * 2
    )
    q_keep, q_send = call(pack_q_kernel, [((blk, feat), BF16)] * 2, (query,), spaces=[pltpu.HBM])
    chips = seq_count // 2
    onward = [(i, i + 2) for i in range(seq_count - 2)] + [(seq_count - 2, 1), (seq_count - 1, 0)]
    kv_got = swap(kv_send, 0)
    old_keep = lax.ppermute(kv_keep, "seq", onward)
    got_k, got_v = call(part_kernel, [((blk, kv_width), BF16)] * 2, (kv_got,))
    old_k = lax.ppermute(got_k, "seq", onward)
    old_v = lax.ppermute(got_v, "seq", onward)
    q_got = swap(q_send, 0)

    mix, b_weighted, scale, tot, skip_row = call(
        prepare_kernel,
        [
            ((pairs, toks, 2 * toks), BF16),
            ((pairs, STATE, 2 * toks), BF16),
            ((toks, feat), F32),
            ((1, feat), F32),
            ((1, feat), F32),
        ],
        (step, log_decay, in_b, out_c, skip),
        flops=1 << 30,
        spaces=[pltpu.HBM] * 5,
    )
    bits = seq_count.bit_length() - 1
    rows_at_once = feat // kv_width * blk
    weights, scales = call(
        score_kernel,
        [((2 * kv_width // HDIM, rows_at_once, 3 * blk), BF16), ((2 * kv_width // HDIM, rows_at_once, HDIM), F32)],
        (q_keep, q_got, kv_keep, kv_got, old_keep, old_k),
        flops=1 << 28,
    )
    attended, sums = call(
        value_kernel,
        [((toks, feat), BF16), ((16, blk), F32)],
        (weights, scales, kv_keep, kv_got, old_keep, old_v),
        flops=1 << 28,
    )
    to_home = [(i, i // 2 + (1 - i % 2) * chips) for i in every]
    rows = lax.ppermute(attended, "seq", to_home)
    for bit in range(head_count.bit_length() - 1):
        other = lax.ppermute(sums, "head", [(i, i ^ (1 << bit)) for i in range(head_count)])
        (sums,) = call(add_kernel, [((16, blk), F32)], (sums, other))
    sums = lax.ppermute(sums, "seq", to_home)
    quarter = 1 << (bits - 2)

    def hop(block, quarters):
        route = []
        for i in every:
            to = quarters[i // quarter]
            route.append((i, i ^ 1 if to is None else to * quarter + i % quarter))
        return lax.ppermute(block, "seq", route)

    gain = norm_gain[None, :]
    state, row, packed = ((STATE, half), F32), ((1, half), F32), ((STATE + TAIL, half), BF16)
    x_send, send = call(
        functools.partial(home_kernel, False),
        [((toks, half), BF16), packed],
        (rows, sums, gain, b_weighted, tot),
        flops=1 << 27,
    )
    x_keep, keep = call(
        functools.partial(home_kernel, True),
        [((toks, half), BF16), state],
        (rows, sums, gain, b_weighted, tot),
        flops=1 << 27,
    )
    local_keep, local_send = call(
        local_kernel, [((toks, half), F32)] * 2, (x_keep, x_send, mix, skip_row), flops=1 << 29
    )
    got = swap(send, 0)
    stages = range(1, bits - 2)
    early, ahead, low, *held = call(
        chip_kernel, [state, row, packed] + [state, row] * bool(stages), (keep, got, tot)
    )
    entered = ()
    for bit in stages:
        theirs = swap(low, bit)
        *entered, low, total, running = call(
            functools.partial(stage_kernel, bit, bit == 1),
            [state, row, packed, state, row],
            (*held, theirs, *entered),
        )
        held = (total, running)
    both = hop(low, (3, 0, None, 1))
    inner = hop(low, (1, 2, 3, 0))
    outer = hop(low, (2, 3, 0, 1))
    own, give = call(
        functools.partial(last_kernel, bits - 2),
        [((STATE, half), BF16)] * 2,
        (inner, outer, both, early, ahead, *entered),
    )
    other = swap(give, 0)
    (kept,) = call(
        functools.partial(finish_kernel, True),
        [((toks, half), BF16)],
        (local_keep, scale, out_c, own),
        flops=1 << 27,
    )
    (out,) = call(
        functools.partial(finish_kernel, False),
        [((toks, feat), BF16)],
        (local_send, scale, out_c, other, kept),
        flops=1 << 27,
    )
    return out


def solution(mesh):
    placed = (
        P(None, "seq", "head"),
        P(None, "seq", "head"),
        P(None, "seq", "head"),
        P("head"),
        P("seq", None),
        P("seq", None),
        P("head", "seq"),
        P("head", "seq"),
        P("head"),
    )
    return jax.shard_map(
        layer, mesh=mesh, in_specs=placed, out_specs=P("seq", "head"), check_vma=False
    )
```

```python
import functools
import math

import jax
import jax.numpy as jnp
from jax import lax
from jax.experimental import pallas as pl
from jax.experimental.pallas import tpu as pltpu
from jax.sharding import PartitionSpec as P


HEADS = 32
HDIM = 128
SDIM = 64
STATE = 128
TAIL = 8

F32 = jnp.float32
BF16 = jnp.bfloat16
VMEM = pltpu.VMEM
GRANT = 12 << 20


def dot(a, b, contract=(1, 0), precision=None):
    return lax.dot_general(
        a,
        b,
        (((contract[0],), (contract[1],)), ((), ())),
        precision=precision,
        preferred_element_type=F32,
    )


def call(kernel, outs, args, flops=1, spaces=None):
    spaces = spaces or [VMEM] * len(args)
    return pl.pallas_call(
        kernel,
        out_shape=[jax.ShapeDtypeStruct(s, d) for s, d in outs],
        in_specs=[pl.BlockSpec(memory_space=m) for m in spaces],
        out_specs=[pl.BlockSpec(memory_space=VMEM)] * len(outs),
        compiler_params=pltpu.CompilerParams(vmem_limit_bytes=GRANT),
        cost_estimate=pl.CostEstimate(flops=flops, bytes_accessed=1 << 20, transcendentals=0),
    )(*[pltpu.with_memory_space_constraint(a, m) if m == pltpu.HBM else a for a, m in zip(args, spaces)])


def gather(copies, sems):
    started = [pltpu.make_async_copy(a, b, sems.at[i]) for i, (a, b) in enumerate(copies)]
    for copy in started:
        copy.start()
    for copy in started:
        copy.wait()


def part_kernel(got_ref, keep_v_ref, k_ref, v_ref, both_ref):
    width = k_ref.shape[1]
    k_ref[...] = got_ref[:, :width]
    v_ref[...] = got_ref[:, width:]
    both_ref[:, :width] = keep_v_ref[...]
    both_ref[:, width:] = got_ref[:, width:]


def pack_kv_kernel(k_ref, v_ref, keep_k_ref, keep_v_ref, send_ref):
    width = k_ref.shape[2]
    mine = lax.axis_index("seq") % 2
    copies = [
        (k_ref.at[1 - mine], keep_k_ref),
        (k_ref.at[mine], send_ref.at[:, :width]),
        (v_ref.at[mine], send_ref.at[:, width:]),
        (v_ref.at[1 - mine], keep_v_ref),
    ]
    pl.run_scoped(functools.partial(gather, copies), pltpu.SemaphoreType.DMA((4,)))


def pack_q_kernel(q_ref, keep_ref, send_ref):
    mine = lax.axis_index("seq") % 2
    copies = [(q_ref.at[1 - mine], keep_ref), (q_ref.at[mine], send_ref)]
    pl.run_scoped(functools.partial(gather, copies), pltpu.SemaphoreType.DMA((2,)))


def prepare_kernel(*refs):
    def inner(sems, *inside):
        copies = [
            pltpu.make_async_copy(src, dst, sems.at[i])
            for i, (src, dst) in enumerate(zip(refs[:5], inside))
        ]
        for copy in copies:
            copy.start()
        for copy in copies:
            copy.wait()
        prepare(*inside, *refs[5:])

    pl.run_scoped(
        inner,
        pltpu.SemaphoreType.DMA((5,)),
        *[VMEM(r.shape, r.dtype) for r in refs[:4]],
        pltpu.SMEM(refs[4].shape, refs[4].dtype),
    )


def prepare(step_ref, log_ref, b_ref, c_ref, skip_ref, mix_ref, bw_ref, scale_ref, tot_ref, pass_ref):
    heads, toks = step_ref.shape
    half = toks // 2
    highest = lax.Precision.HIGHEST
    log = log_ref[...]
    step = step_ref[...]
    rows = lax.broadcasted_iota(jnp.int32, (toks, toks), 0)
    cols = lax.broadcasted_iota(jnp.int32, (toks, toks), 1)
    lower = (rows >= cols).astype(F32)
    cum = dot(log, lower, (1, 1), highest)
    cum_cols = dot(lower, log, (1, 1), highest)
    total = cum[:, toks - 1 :]
    weight = jnp.exp(total - cum) * step
    cross = dot(c_ref[...], b_ref[...], (1, 1))
    b_t = jnp.transpose(b_ref[...].astype(F32))
    causal = (
        lax.broadcasted_iota(jnp.int32, (half, half), 0)
        >= lax.broadcasted_iota(jnp.int32, (half, half), 1)
    )
    lanes = lax.broadcasted_iota(jnp.int32, (toks, HDIM), 1)
    for pair in range(heads // 2):
        for side in range(2):
            k = 2 * pair + side
            at = side * toks
            for r in range(2):
                for c in range(2):
                    dst = (pair, slice(r * half, (r + 1) * half), slice(at + c * half, at + (c + 1) * half))
                    if c > r:
                        mix_ref[dst] = jnp.zeros((half, half), BF16)
                        continue
                    rs, cs = slice(r * half, (r + 1) * half), slice(c * half, (c + 1) * half)
                    gap = cum_cols[rs, k : k + 1] - cum[k : k + 1, cs]
                    if r == c:
                        gap = jnp.where(causal, gap, -jnp.inf)
                    mix_ref[dst] = (jnp.exp(gap) * cross[rs, cs] * step[k : k + 1, cs]).astype(BF16)
            bw_ref[pair, :, at : at + toks] = (b_t * weight[k : k + 1, :]).astype(BF16)
        both = jnp.where(
            lanes < SDIM,
            cum_cols[:, 2 * pair : 2 * pair + 1],
            cum_cols[:, 2 * pair + 1 : 2 * pair + 2],
        )
        both = jnp.exp(both)
        scale_ref[:, pair * HDIM : (pair + 1) * HDIM] = both
        tot_ref[:, pair * HDIM : (pair + 1) * HDIM] = both[toks - 1 :, :]
        pass_ref[:, pair * HDIM : (pair + 1) * HDIM] = jnp.where(
            lanes[:1] < SDIM, skip_ref[2 * pair], skip_ref[2 * pair + 1]
        )


def pick(keep_ref, got_ref, swapped, column, got_column=None):
    keep, got = [
        ref[:, c * HDIM : (c + 1) * HDIM]
        for ref, c in ((keep_ref, column), (got_ref, column if got_column is None else got_column))
    ]
    return jnp.where(swapped, got, keep), jnp.where(swapped, keep, got)


def places():
    me = lax.axis_index("seq")
    late = me % 2 == 1
    return late, jnp.where(me < 2, me % 2 == 0, late), me != 1


def score_kernel(
    q_keep_ref, q_got_ref, keep_ref, got_ref, old_keep_ref, old_got_ref, weight_ref, scale_ref
):
    blk, feat = q_keep_ref.shape
    kv_local = keep_ref.shape[1] // HDIM
    group = feat // HDIM // kv_local
    late, old_late, has_old = places()
    rows = lax.broadcasted_iota(jnp.int32, (group * blk, blk), 0) % blk
    cols = lax.broadcasted_iota(jnp.int32, (group * blk, blk), 1)
    own_ok = cols <= rows
    far_ok = (cols > rows) & has_old
    near_ok = (cols >= 0) & has_old
    factor = math.log2(math.e) / math.sqrt(HDIM)
    for g in range(kv_local):
        keys = pick(old_keep_ref, old_got_ref, old_late, g) + pick(keep_ref, got_ref, late, g)
        heads = [pick(q_keep_ref, q_got_ref, late, g * group + i) for i in range(group)]
        for part in range(2):
            query = jnp.concatenate([h[part] for h in heads], 0)
            score = dot(query, jnp.concatenate(keys[part : part + 3], 0), (1, 1))
            near = score[:, blk : 2 * blk]
            if part == 0:
                near = jnp.where(near_ok, near, -jnp.inf)
            far = jnp.where(far_ok, score[:, :blk], -jnp.inf)
            score = jnp.concatenate([far, near, jnp.where(own_ok, score[:, 2 * blk :], -jnp.inf)], 1)
            peak = jnp.max(score, axis=1, keepdims=True)
            terms = jnp.exp2((score - peak) * factor)
            total = pl.reciprocal(jnp.sum(terms, axis=1, keepdims=True))
            weight_ref[2 * g + part] = terms.astype(BF16)
            scale_ref[2 * g + part] = jnp.broadcast_to(total, (group * blk, HDIM))


def own_value_kernel(weight_ref, keep_ref, got_ref, sum_ref):
    blk = keep_ref.shape[0]
    late = places()[0]
    for g in range(keep_ref.shape[1] // HDIM):
        vals = pick(keep_ref, got_ref, late, g)
        for part in range(2):
            values = jnp.concatenate(vals[: part + 1], 0)
            sum_ref[2 * g + part] = dot(weight_ref[2 * g + part, :, (2 - part) * blk :], values)


def value_kernel(weight_ref, scale_ref, sum_ref, old_ref, out_ref, sums_ref):
    blk = old_ref.shape[0]
    kv_local = old_ref.shape[1] // (2 * HDIM)
    group = out_ref.shape[1] // HDIM // kv_local
    old_late = places()[1]
    squares = [jnp.zeros((blk, 1), F32)] * 2
    for g in range(kv_local):
        vals = pick(old_ref, old_ref, old_late, g, kv_local + g)
        for part in range(2):
            at = 2 * g + part
            result = dot(weight_ref[at, :, : (2 - part) * blk], jnp.concatenate(vals[part:], 0))
            result = (result + sum_ref[at]) * scale_ref[at]
            result = result.astype(BF16)
            wide = result.astype(F32)
            square = jnp.sum(wide * wide, axis=1, keepdims=True)
            for i in range(group):
                at = slice((g * group + i) * HDIM, (g * group + i + 1) * HDIM)
                out_ref[part * blk : (part + 1) * blk, at] = result[i * blk : (i + 1) * blk]
                squares[part] = squares[part] + square[i * blk : (i + 1) * blk]
    for part in range(2):
        turned = jnp.transpose(jnp.broadcast_to(squares[part], (blk, blk)))
        sums_ref[part * 8 : part * 8 + 8] = turned[:8]


def spread(x):
    lanes = lax.broadcasted_iota(jnp.int32, x.shape, 1)
    zero = jnp.zeros_like(x)
    return jnp.concatenate([jnp.where(lanes < SDIM, x, zero), jnp.where(lanes < SDIM, zero, x)], 0)


def pack_state(ref, state, decay, at=slice(None)):
    ref[:STATE, at] = state.astype(BF16)
    high = decay.astype(BF16).astype(F32)
    row = lax.broadcasted_iota(jnp.int32, (TAIL, decay.shape[1]), 0)
    ref[STATE:, at] = jnp.where(row == 0, high, decay - high).astype(BF16)


def unpack_state(ref):
    tail = ref[STATE:].astype(F32)
    return ref[:STATE].astype(F32), tail[:1] + tail[1:2]


def home_kernel(keeps, rows_ref, sums_ref, gain_ref, bw_ref, tot_ref, x_ref, state_ref):
    mine = lax.axis_index("seq") % 2
    side = mine if keeps else 1 - mine
    toks, half = x_ref.shape
    blk = toks // 2
    pairs = half // HDIM
    lanes = pl.ds(pl.multiple_of(side * half, half), half)
    gain = gain_ref[:, lanes]
    for part in range(2):
        at = slice(part * blk, (part + 1) * blk)
        sums = sums_ref[part * 8 : part * 8 + 1]
        mean = jnp.transpose(jnp.broadcast_to(sums, (blk, blk))) / (HEADS * HDIM)
        inv = lax.rsqrt(mean + 1e-06)[:, :1]
        x_ref[at, :] = (rows_ref[at, lanes].astype(F32) * gain * inv).astype(BF16)
    for p in range(pairs):
        at = slice(p * HDIM, (p + 1) * HDIM)
        state = dot(bw_ref[side * pairs + p], spread(x_ref[:, at]))
        if keeps:
            state_ref[:, at] = state
        else:
            decay = tot_ref[:, pl.ds(pl.multiple_of(side * half + p * HDIM, HDIM), HDIM)]
            pack_state(state_ref, state, decay, at)


def local_kernel(x_keep_ref, x_send_ref, mix_ref, skip_ref, keep_ref, send_ref):
    mine = lax.axis_index("seq") % 2
    half = x_keep_ref.shape[1]
    pairs = half // HDIM
    for x_ref, out_ref, side in ((x_keep_ref, keep_ref, mine), (x_send_ref, send_ref, 1 - mine)):
        skip = skip_ref[:, pl.ds(pl.multiple_of(side * half, half), half)]
        for p in range(pairs):
            at = slice(p * HDIM, (p + 1) * HDIM)
            x = x_ref[:, at]
            out_ref[:, at] = dot(mix_ref[side * pairs + p], spread(x)) + skip[:, at] * x.astype(F32)


def finish_kernel(keeps, local_ref, scale_ref, c_ref, enter_ref, *refs):
    mine = lax.axis_index("seq") % 2
    half = local_ref.shape[1]
    side = mine if keeps else 1 - mine
    lanes = pl.ds(pl.multiple_of(side * half, half), half)
    out = local_ref[...] + dot(c_ref[...], enter_ref[...]) * scale_ref[:, lanes]
    if keeps:
        refs[0][...] = out.astype(BF16)
    else:
        own_ref, out_ref = refs
        out_ref[:, lanes] = out.astype(BF16)
        out_ref[:, pl.ds(pl.multiple_of(mine * half, half), half)] = own_ref[...]


def add_kernel(a_ref, b_ref, out_ref):
    out_ref[...] = a_ref[...] + b_ref[...]


def half_of(ref, side):
    half = ref.shape[1] // 2
    return ref[:, pl.ds(pl.multiple_of(side * half, half), half)]


def chip_kernel(keep_ref, got_ref, tot_ref, early_ref, ahead_ref, low_ref, *refs):
    mine = lax.axis_index("seq") % 2
    late = mine == 1
    keep, here = keep_ref[...], half_of(tot_ref, mine)
    got, there = unpack_state(got_ref)
    early = jnp.where(late, got, keep)
    total = jnp.where(late, here, there) * early + jnp.where(late, keep, got)
    early_ref[...] = early
    ahead_ref[...] = jnp.where(late, there, here)
    pack_state(low_ref, total, here * there)
    if refs:
        refs[0][...] = total
        refs[1][...] = here * there


def stage_kernel(bit, first, total_ref, mine_ref, theirs_ref, *refs):
    upper = (lax.axis_index("seq") >> bit) % 2 == 1
    enter_ref, carried_ref, low_ref, next_ref, running_ref = refs[-5:]
    theirs, decay = unpack_state(theirs_ref)
    total, mine = total_ref[...], mine_ref[...]
    if first:
        enter_ref[...] = jnp.where(upper, theirs, 0.0)
        carried_ref[...] = jnp.where(upper, decay, 1.0)
    else:
        carried = refs[1][...]
        enter_ref[...] = refs[0][...] + jnp.where(upper, carried * theirs, 0.0)
        carried_ref[...] = jnp.where(upper, carried * decay, carried)
    total = jnp.where(upper, mine * theirs + total, decay * total + theirs)
    pack_state(low_ref, total, mine * decay)
    next_ref[...] = total
    running_ref[...] = mine * decay


def last_kernel(shift, inner_ref, outer_ref, both_ref, early_ref, ahead_ref, *refs):
    own_ref, give_ref = refs[-2:]
    me = lax.axis_index("seq")
    quarter, late = me >> shift, me % 2 == 1
    beside, by_inner = unpack_state(inner_ref)
    across, by_outer = unpack_state(outer_ref)
    diagonal, _ = unpack_state(both_ref)
    third, fourth = quarter == 2, quarter == 3
    one, zero = jnp.ones_like(by_inner), jnp.zeros_like(by_inner)
    enter = jnp.where(quarter > 0, one, zero) * beside
    enter = enter + jnp.where(third | fourth, by_inner, zero) * across
    enter = enter + jnp.where(fourth, by_inner * by_outer, zero) * diagonal
    if len(refs) == 4:
        enter = refs[0][...] + refs[1][...] * enter
    after = ahead_ref[...] * enter + early_ref[...]
    own_ref[...] = jnp.where(late, after, enter).astype(BF16)
    give_ref[...] = jnp.where(late, enter, after).astype(BF16)


def layer(query, keys, values, norm_gain, in_b, out_c, step, log_decay, skip):
    seq_count = lax.axis_size("seq")
    head_count = lax.axis_size("head")
    blk, feat = query.shape[1:]
    heads, toks = step.shape
    kv_width = keys.shape[2]
    pairs = heads // 2
    half = feat // 2
    every = range(seq_count)

    def swap(block, bit):
        return lax.ppermute(block, "seq", [(i, i ^ (1 << bit)) for i in every])

    width = 2 * kv_width
    half_kv = ((blk, kv_width), BF16)
    keep_k, keep_v, kv_send = call(
        pack_kv_kernel,
        [half_kv, half_kv, ((blk, width), BF16)],
        (keys, values),
        spaces=[pltpu.HBM] * 2,
    )
    q_keep, q_send = call(pack_q_kernel, [((blk, feat), BF16)] * 2, (query,), spaces=[pltpu.HBM])
    chips = seq_count // 2
    onward = [(i, i + 2) for i in range(seq_count - 2)] + [(seq_count - 2, 1), (seq_count - 1, 0)]
    kv_got = swap(kv_send, 0)
    old_keep = lax.ppermute(keep_k, "seq", onward)
    got_k, got_v, both_v = call(
        part_kernel, [half_kv, half_kv, ((blk, width), BF16)], (kv_got, keep_v)
    )
    old_k = lax.ppermute(got_k, "seq", onward)
    old_v = lax.ppermute(both_v, "seq", onward)
    q_got = swap(q_send, 0)

    mix, b_weighted, scale, tot, skip_row = call(
        prepare_kernel,
        [
            ((pairs, toks, 2 * toks), BF16),
            ((pairs, STATE, 2 * toks), BF16),
            ((toks, feat), F32),
            ((1, feat), F32),
            ((1, feat), F32),
        ],
        (step, log_decay, in_b, out_c, skip),
        flops=1 << 30,
        spaces=[pltpu.HBM] * 5,
    )
    bits = seq_count.bit_length() - 1
    rows_at_once = feat // kv_width * blk
    weights, scales = call(
        score_kernel,
        [((2 * kv_width // HDIM, rows_at_once, 3 * blk), BF16), ((2 * kv_width // HDIM, rows_at_once, HDIM), F32)],
        (q_keep, q_got, keep_k, got_k, old_keep, old_k),
        flops=1 << 28,
    )
    (own_sum,) = call(
        own_value_kernel,
        [((2 * kv_width // HDIM, rows_at_once, HDIM), F32)],
        (weights, keep_v, got_v),
        flops=1 << 27,
    )
    attended, sums = call(
        value_kernel,
        [((toks, feat), BF16), ((16, blk), F32)],
        (weights, scales, own_sum, old_v),
        flops=1 << 28,
    )
    to_home = [(i, i // 2 + (1 - i % 2) * chips) for i in every]
    rows = lax.ppermute(attended, "seq", to_home)
    for bit in range(head_count.bit_length() - 1):
        other = lax.ppermute(sums, "head", [(i, i ^ (1 << bit)) for i in range(head_count)])
        (sums,) = call(add_kernel, [((16, blk), F32)], (sums, other))
    sums = lax.ppermute(sums, "seq", to_home)
    quarter = 1 << (bits - 2)

    def hop(block, quarters):
        route = []
        for i in every:
            to = quarters[i // quarter]
            route.append((i, i ^ 1 if to is None else to * quarter + i % quarter))
        return lax.ppermute(block, "seq", route)

    gain = norm_gain[None, :]
    state, row, packed = ((STATE, half), F32), ((1, half), F32), ((STATE + TAIL, half), BF16)
    x_send, send = call(
        functools.partial(home_kernel, False),
        [((toks, half), BF16), packed],
        (rows, sums, gain, b_weighted, tot),
        flops=1 << 27,
    )
    x_keep, keep = call(
        functools.partial(home_kernel, True),
        [((toks, half), BF16), state],
        (rows, sums, gain, b_weighted, tot),
        flops=1 << 27,
    )
    local_keep, local_send = call(
        local_kernel, [((toks, half), F32)] * 2, (x_keep, x_send, mix, skip_row), flops=1 << 29
    )
    got = swap(send, 0)
    stages = range(1, bits - 2)
    early, ahead, low, *held = call(
        chip_kernel, [state, row, packed] + [state, row] * bool(stages), (keep, got, tot)
    )
    entered = ()
    for bit in stages:
        theirs = swap(low, bit)
        *entered, low, total, running = call(
            functools.partial(stage_kernel, bit, bit == 1),
            [state, row, packed, state, row],
            (*held, theirs, *entered),
        )
        held = (total, running)
    both = hop(low, (3, 0, None, 1))
    inner = hop(low, (1, 2, 3, 0))
    outer = hop(low, (2, 3, 0, 1))
    own, give = call(
        functools.partial(last_kernel, bits - 2),
        [((STATE, half), BF16)] * 2,
        (inner, outer, both, early, ahead, *entered),
    )
    other = swap(give, 0)
    (kept,) = call(
        functools.partial(finish_kernel, True),
        [((toks, half), BF16)],
        (local_keep, scale, out_c, own),
        flops=1 << 27,
    )
    (out,) = call(
        functools.partial(finish_kernel, False),
        [((toks, feat), BF16)],
        (local_send, scale, out_c, other, kept),
        flops=1 << 27,
    )
    return out


def solution(mesh):
    placed = (
        P(None, "seq", "head"),
        P(None, "seq", "head"),
        P(None, "seq", "head"),
        P("head"),
        P("seq", None),
        P("seq", None),
        P("head", "seq"),
        P("head", "seq"),
        P("head"),
    )
    return jax.shard_map(
        layer, mesh=mesh, in_specs=placed, out_specs=P("seq", "head"), check_vma=False
    )
```

```python
import functools
import math

import jax
import jax.numpy as jnp
from jax import lax
from jax.experimental import pallas as pl
from jax.experimental.pallas import tpu as pltpu
from jax.sharding import PartitionSpec as P


HEADS = 32
HDIM = 128
SDIM = 64
STATE = 128
TAIL = 8

F32 = jnp.float32
BF16 = jnp.bfloat16
VMEM = pltpu.VMEM
GRANT = 12 << 20


def dot(a, b, contract=(1, 0), precision=None):
    return lax.dot_general(
        a,
        b,
        (((contract[0],), (contract[1],)), ((), ())),
        precision=precision,
        preferred_element_type=F32,
    )


def call(kernel, outs, args, flops=1, spaces=None):
    spaces = spaces or [VMEM] * len(args)
    return pl.pallas_call(
        kernel,
        out_shape=[jax.ShapeDtypeStruct(s, d) for s, d in outs],
        in_specs=[pl.BlockSpec(memory_space=m) for m in spaces],
        out_specs=[pl.BlockSpec(memory_space=VMEM)] * len(outs),
        compiler_params=pltpu.CompilerParams(vmem_limit_bytes=GRANT),
        cost_estimate=pl.CostEstimate(flops=flops, bytes_accessed=1 << 20, transcendentals=0),
    )(*[pltpu.with_memory_space_constraint(a, m) if m == pltpu.HBM else a for a, m in zip(args, spaces)])


def gather(copies, sems):
    started = [pltpu.make_async_copy(a, b, sems.at[i]) for i, (a, b) in enumerate(copies)]
    for copy in started:
        copy.start()
    for copy in started:
        copy.wait()


def part_kernel(got_ref, keep_v_ref, k_ref, v_ref, both_ref):
    width = k_ref.shape[1]
    k_ref[...] = got_ref[:, :width]
    v_ref[...] = got_ref[:, width:]
    both_ref[:, :width] = keep_v_ref[...]
    both_ref[:, width:] = got_ref[:, width:]


def pack_kv_kernel(k_ref, v_ref, keep_k_ref, keep_v_ref, send_ref):
    width = k_ref.shape[2]
    mine = lax.axis_index("seq") % 2
    copies = [
        (k_ref.at[1 - mine], keep_k_ref),
        (k_ref.at[mine], send_ref.at[:, :width]),
        (v_ref.at[mine], send_ref.at[:, width:]),
        (v_ref.at[1 - mine], keep_v_ref),
    ]
    pl.run_scoped(functools.partial(gather, copies), pltpu.SemaphoreType.DMA((4,)))


def pack_q_kernel(q_ref, keep_ref, send_ref):
    mine = lax.axis_index("seq") % 2
    copies = [(q_ref.at[1 - mine], keep_ref), (q_ref.at[mine], send_ref)]
    pl.run_scoped(functools.partial(gather, copies), pltpu.SemaphoreType.DMA((2,)))


def prepare_kernel(*refs):
    def inner(sems, *inside):
        copies = [
            pltpu.make_async_copy(src, dst, sems.at[i])
            for i, (src, dst) in enumerate(zip(refs[:5], inside))
        ]
        for copy in copies:
            copy.start()
        for copy in copies:
            copy.wait()
        prepare(*inside, *refs[5:])

    pl.run_scoped(
        inner,
        pltpu.SemaphoreType.DMA((5,)),
        *[VMEM(r.shape, r.dtype) for r in refs[:4]],
        pltpu.SMEM(refs[4].shape, refs[4].dtype),
    )


def prepare(step_ref, log_ref, b_ref, c_ref, skip_ref, mix_ref, bw_ref, scale_ref, tot_ref, pass_ref):
    heads, toks = step_ref.shape
    half = toks // 2
    highest = lax.Precision.HIGHEST
    log = log_ref[...]
    step = step_ref[...]
    rows = lax.broadcasted_iota(jnp.int32, (toks, toks), 0)
    cols = lax.broadcasted_iota(jnp.int32, (toks, toks), 1)
    lower = (rows >= cols).astype(F32)
    cum = dot(log, lower, (1, 1), highest)
    cum_cols = dot(lower, log, (1, 1), highest)
    total = cum[:, toks - 1 :]
    weight = jnp.exp(total - cum) * step
    cross = dot(c_ref[...], b_ref[...], (1, 1))
    b_t = jnp.transpose(b_ref[...].astype(F32))
    causal = (
        lax.broadcasted_iota(jnp.int32, (half, half), 0)
        >= lax.broadcasted_iota(jnp.int32, (half, half), 1)
    )
    lanes = lax.broadcasted_iota(jnp.int32, (toks, HDIM), 1)
    for pair in range(heads // 2):
        for side in range(2):
            k = 2 * pair + side
            at = side * toks
            for r in range(2):
                for c in range(2):
                    dst = (pair, slice(r * half, (r + 1) * half), slice(at + c * half, at + (c + 1) * half))
                    if c > r:
                        mix_ref[dst] = jnp.zeros((half, half), BF16)
                        continue
                    rs, cs = slice(r * half, (r + 1) * half), slice(c * half, (c + 1) * half)
                    gap = cum_cols[rs, k : k + 1] - cum[k : k + 1, cs]
                    if r == c:
                        gap = jnp.where(causal, gap, -jnp.inf)
                    mix_ref[dst] = (jnp.exp(gap) * cross[rs, cs] * step[k : k + 1, cs]).astype(BF16)
            bw_ref[pair, :, at : at + toks] = (b_t * weight[k : k + 1, :]).astype(BF16)
        both = jnp.where(
            lanes < SDIM,
            cum_cols[:, 2 * pair : 2 * pair + 1],
            cum_cols[:, 2 * pair + 1 : 2 * pair + 2],
        )
        both = jnp.exp(both)
        scale_ref[:, pair * HDIM : (pair + 1) * HDIM] = both
        tot_ref[:, pair * HDIM : (pair + 1) * HDIM] = both[toks - 1 :, :]
        pass_ref[:, pair * HDIM : (pair + 1) * HDIM] = jnp.where(
            lanes[:1] < SDIM, skip_ref[2 * pair], skip_ref[2 * pair + 1]
        )


def pick(keep_ref, got_ref, swapped, column, got_column=None):
    keep, got = [
        ref[:, c * HDIM : (c + 1) * HDIM]
        for ref, c in ((keep_ref, column), (got_ref, column if got_column is None else got_column))
    ]
    return jnp.where(swapped, got, keep), jnp.where(swapped, keep, got)


def places():
    me = lax.axis_index("seq")
    late = me % 2 == 1
    return late, jnp.where(me < 2, me % 2 == 0, late), me != 1


def score_kernel(
    q_keep_ref, q_got_ref, keep_ref, got_ref, old_keep_ref, old_got_ref, weight_ref, scale_ref
):
    blk, feat = q_keep_ref.shape
    kv_local = keep_ref.shape[1] // HDIM
    group = feat // HDIM // kv_local
    late, old_late, has_old = places()
    rows = lax.broadcasted_iota(jnp.int32, (group * blk, blk), 0) % blk
    cols = lax.broadcasted_iota(jnp.int32, (group * blk, blk), 1)
    own_ok = cols <= rows
    far_ok = (cols > rows) & has_old
    near_ok = (cols >= 0) & has_old
    factor = math.log2(math.e) / math.sqrt(HDIM)
    for g in range(kv_local):
        keys = pick(old_keep_ref, old_got_ref, old_late, g) + pick(keep_ref, got_ref, late, g)
        heads = [pick(q_keep_ref, q_got_ref, late, g * group + i) for i in range(group)]
        for part in range(2):
            query = jnp.concatenate([h[part] for h in heads], 0)
            score = dot(query, jnp.concatenate(keys[part : part + 3], 0), (1, 1))
            near = score[:, blk : 2 * blk]
            if part == 0:
                near = jnp.where(near_ok, near, -jnp.inf)
            far = jnp.where(far_ok, score[:, :blk], -jnp.inf)
            score = jnp.concatenate([far, near, jnp.where(own_ok, score[:, 2 * blk :], -jnp.inf)], 1)
            peak = jnp.max(score, axis=1, keepdims=True)
            terms = jnp.exp2((score - peak) * factor)
            total = pl.reciprocal(jnp.sum(terms, axis=1, keepdims=True))
            weight_ref[2 * g + part] = terms.astype(BF16)
            scale_ref[2 * g + part] = jnp.broadcast_to(total, (group * blk, HDIM))


def own_value_kernel(weight_ref, keep_ref, got_ref, sum_ref):
    blk = keep_ref.shape[0]
    late = places()[0]
    for g in range(keep_ref.shape[1] // HDIM):
        vals = pick(keep_ref, got_ref, late, g)
        for part in range(2):
            values = jnp.concatenate(vals[: part + 1], 0)
            sum_ref[2 * g + part] = dot(weight_ref[2 * g + part, :, (2 - part) * blk :], values)


def value_kernel(weight_ref, scale_ref, sum_ref, old_ref, out_ref):
    blk = old_ref.shape[0]
    kv_local = old_ref.shape[1] // (2 * HDIM)
    group = out_ref.shape[1] // HDIM // kv_local
    old_late = places()[1]
    for g in range(kv_local):
        vals = pick(old_ref, old_ref, old_late, g, kv_local + g)
        for part in range(2):
            at = 2 * g + part
            result = dot(weight_ref[at, :, : (2 - part) * blk], jnp.concatenate(vals[part:], 0))
            result = ((result + sum_ref[at]) * scale_ref[at]).astype(BF16)
            for i in range(group):
                lanes = slice((g * group + i) * HDIM, (g * group + i + 1) * HDIM)
                out_ref[part * blk : (part + 1) * blk, lanes] = result[i * blk : (i + 1) * blk]


def square_kernel(rows_ref, sums_ref):
    blk = rows_ref.shape[0] // 2
    for part in range(2):
        rows = rows_ref[part * blk : (part + 1) * blk].astype(F32)
        total = jnp.sum(rows * rows, axis=1, keepdims=True)
        turned = jnp.transpose(jnp.broadcast_to(total, (blk, blk)))
        sums_ref[part * 8 : part * 8 + 8] = turned[:8]


def spread(x):
    lanes = lax.broadcasted_iota(jnp.int32, x.shape, 1)
    zero = jnp.zeros_like(x)
    return jnp.concatenate([jnp.where(lanes < SDIM, x, zero), jnp.where(lanes < SDIM, zero, x)], 0)


def pack_state(ref, state, decay, at=slice(None)):
    ref[:STATE, at] = state.astype(BF16)
    high = decay.astype(BF16).astype(F32)
    row = lax.broadcasted_iota(jnp.int32, (TAIL, decay.shape[1]), 0)
    ref[STATE:, at] = jnp.where(row == 0, high, decay - high).astype(BF16)


def unpack_state(ref):
    tail = ref[STATE:].astype(F32)
    return ref[:STATE].astype(F32), tail[:1] + tail[1:2]


def home_kernel(keeps, rows_ref, sums_ref, gain_ref, bw_ref, tot_ref, x_ref, state_ref):
    mine = lax.axis_index("seq") % 2
    side = mine if keeps else 1 - mine
    toks, half = x_ref.shape
    blk = toks // 2
    pairs = half // HDIM
    lanes = pl.ds(pl.multiple_of(side * half, half), half)
    gain = gain_ref[:, lanes]
    for part in range(2):
        at = slice(part * blk, (part + 1) * blk)
        sums = sums_ref[part * 8 : part * 8 + 1]
        mean = jnp.transpose(jnp.broadcast_to(sums, (HDIM, blk))) / (HEADS * HDIM)
        inv = lax.rsqrt(mean + 1e-06)
        rows = rows_ref[at, lanes].astype(F32) * gain
        for p in range(pairs):
            tile = slice(p * HDIM, (p + 1) * HDIM)
            x_ref[at, tile] = (rows[:, tile] * inv).astype(BF16)
    for p in range(pairs):
        at = slice(p * HDIM, (p + 1) * HDIM)
        state = dot(bw_ref[side * pairs + p], spread(x_ref[:, at]))
        if keeps:
            state_ref[:, at] = state
        else:
            decay = tot_ref[:, pl.ds(pl.multiple_of(side * half + p * HDIM, HDIM), HDIM)]
            pack_state(state_ref, state, decay, at)


def local_kernel(x_keep_ref, x_send_ref, mix_ref, skip_ref, keep_ref, send_ref):
    mine = lax.axis_index("seq") % 2
    half = x_keep_ref.shape[1]
    pairs = half // HDIM
    for x_ref, out_ref, side in ((x_keep_ref, keep_ref, mine), (x_send_ref, send_ref, 1 - mine)):
        skip = skip_ref[:, pl.ds(pl.multiple_of(side * half, half), half)]
        for p in range(pairs):
            at = slice(p * HDIM, (p + 1) * HDIM)
            x = x_ref[:, at]
            out_ref[:, at] = dot(mix_ref[side * pairs + p], spread(x)) + skip[:, at] * x.astype(F32)


def finish_kernel(keeps, local_ref, scale_ref, c_ref, enter_ref, *refs):
    mine = lax.axis_index("seq") % 2
    half = local_ref.shape[1]
    side = mine if keeps else 1 - mine
    lanes = pl.ds(pl.multiple_of(side * half, half), half)
    out = local_ref[...] + dot(c_ref[...], enter_ref[...]) * scale_ref[:, lanes]
    if keeps:
        refs[0][...] = out.astype(BF16)
    else:
        own_ref, out_ref = refs
        out_ref[:, lanes] = out.astype(BF16)
        out_ref[:, pl.ds(pl.multiple_of(mine * half, half), half)] = own_ref[...]


def add_kernel(a_ref, b_ref, out_ref):
    out_ref[...] = a_ref[...] + b_ref[...]


def half_of(ref, side):
    half = ref.shape[1] // 2
    return ref[:, pl.ds(pl.multiple_of(side * half, half), half)]


def chip_kernel(keep_ref, got_ref, tot_ref, early_ref, ahead_ref, low_ref, *refs):
    mine = lax.axis_index("seq") % 2
    late = mine == 1
    keep, here = keep_ref[...], half_of(tot_ref, mine)
    got, there = unpack_state(got_ref)
    early = jnp.where(late, got, keep)
    total = jnp.where(late, here, there) * early + jnp.where(late, keep, got)
    early_ref[...] = early
    ahead_ref[...] = jnp.where(late, there, here)
    pack_state(low_ref, total, here * there)
    if refs:
        refs[0][...] = total
        refs[1][...] = here * there


def stage_kernel(bit, first, total_ref, mine_ref, theirs_ref, *refs):
    upper = (lax.axis_index("seq") >> bit) % 2 == 1
    enter_ref, carried_ref, low_ref, next_ref, running_ref = refs[-5:]
    theirs, decay = unpack_state(theirs_ref)
    total, mine = total_ref[...], mine_ref[...]
    if first:
        enter_ref[...] = jnp.where(upper, theirs, 0.0)
        carried_ref[...] = jnp.where(upper, decay, 1.0)
    else:
        carried = refs[1][...]
        enter_ref[...] = refs[0][...] + jnp.where(upper, carried * theirs, 0.0)
        carried_ref[...] = jnp.where(upper, carried * decay, carried)
    total = jnp.where(upper, mine * theirs + total, decay * total + theirs)
    pack_state(low_ref, total, mine * decay)
    next_ref[...] = total
    running_ref[...] = mine * decay


def last_kernel(shift, inner_ref, outer_ref, both_ref, early_ref, ahead_ref, *refs):
    own_ref, give_ref = refs[-2:]
    me = lax.axis_index("seq")
    quarter, late = me >> shift, me % 2 == 1
    beside, by_inner = unpack_state(inner_ref)
    across, by_outer = unpack_state(outer_ref)
    diagonal, _ = unpack_state(both_ref)
    third, fourth = quarter == 2, quarter == 3
    one, zero = jnp.ones_like(by_inner), jnp.zeros_like(by_inner)
    enter = jnp.where(quarter > 0, one, zero) * beside
    enter = enter + jnp.where(third | fourth, by_inner, zero) * across
    enter = enter + jnp.where(fourth, by_inner * by_outer, zero) * diagonal
    if len(refs) == 4:
        enter = refs[0][...] + refs[1][...] * enter
    after = ahead_ref[...] * enter + early_ref[...]
    own_ref[...] = jnp.where(late, after, enter).astype(BF16)
    give_ref[...] = jnp.where(late, enter, after).astype(BF16)


def layer(query, keys, values, norm_gain, in_b, out_c, step, log_decay, skip):
    seq_count = lax.axis_size("seq")
    head_count = lax.axis_size("head")
    blk, feat = query.shape[1:]
    heads, toks = step.shape
    kv_width = keys.shape[2]
    pairs = heads // 2
    half = feat // 2
    every = range(seq_count)

    def swap(block, bit):
        return lax.ppermute(block, "seq", [(i, i ^ (1 << bit)) for i in every])

    width = 2 * kv_width
    half_kv = ((blk, kv_width), BF16)
    keep_k, keep_v, kv_send = call(
        pack_kv_kernel,
        [half_kv, half_kv, ((blk, width), BF16)],
        (keys, values),
        spaces=[pltpu.HBM] * 2,
    )
    q_keep, q_send = call(pack_q_kernel, [((blk, feat), BF16)] * 2, (query,), spaces=[pltpu.HBM])
    chips = seq_count // 2
    onward = [(i, i + 2) for i in range(seq_count - 2)] + [(seq_count - 2, 1), (seq_count - 1, 0)]
    kv_got = swap(kv_send, 0)
    old_keep = lax.ppermute(keep_k, "seq", onward)
    got_k, got_v, both_v = call(
        part_kernel, [half_kv, half_kv, ((blk, width), BF16)], (kv_got, keep_v)
    )
    old_k = lax.ppermute(got_k, "seq", onward)
    old_v = lax.ppermute(both_v, "seq", onward)
    q_got = swap(q_send, 0)

    mix, b_weighted, scale, tot, skip_row = call(
        prepare_kernel,
        [
            ((pairs, toks, 2 * toks), BF16),
            ((pairs, STATE, 2 * toks), BF16),
            ((toks, feat), F32),
            ((1, feat), F32),
            ((1, feat), F32),
        ],
        (step, log_decay, in_b, out_c, skip),
        flops=1 << 30,
        spaces=[pltpu.HBM] * 5,
    )
    bits = seq_count.bit_length() - 1
    rows_at_once = feat // kv_width * blk
    weights, scales = call(
        score_kernel,
        [((2 * kv_width // HDIM, rows_at_once, 3 * blk), BF16), ((2 * kv_width // HDIM, rows_at_once, HDIM), F32)],
        (q_keep, q_got, keep_k, got_k, old_keep, old_k),
        flops=1 << 28,
    )
    (own_sum,) = call(
        own_value_kernel,
        [((2 * kv_width // HDIM, rows_at_once, HDIM), F32)],
        (weights, keep_v, got_v),
        flops=1 << 27,
    )
    (attended,) = call(
        value_kernel, [((toks, feat), BF16)], (weights, scales, own_sum, old_v), flops=1 << 28
    )
    (sums,) = call(square_kernel, [((16, blk), F32)], (attended,), flops=1 << 22)
    to_home = [(i, i // 2 + (1 - i % 2) * chips) for i in every]
    rows = lax.ppermute(attended, "seq", to_home)
    for bit in range(head_count.bit_length() - 1):
        other = lax.ppermute(sums, "head", [(i, i ^ (1 << bit)) for i in range(head_count)])
        (sums,) = call(add_kernel, [((16, blk), F32)], (sums, other))
    sums = lax.ppermute(sums, "seq", to_home)
    quarter = 1 << (bits - 2)

    def hop(block, quarters):
        route = []
        for i in every:
            to = quarters[i // quarter]
            route.append((i, i ^ 1 if to is None else to * quarter + i % quarter))
        return lax.ppermute(block, "seq", route)

    gain = norm_gain[None, :]
    state, row, packed = ((STATE, half), F32), ((1, half), F32), ((STATE + TAIL, half), BF16)
    x_send, send = call(
        functools.partial(home_kernel, False),
        [((toks, half), BF16), packed],
        (rows, sums, gain, b_weighted, tot),
        flops=1 << 27,
    )
    x_keep, keep = call(
        functools.partial(home_kernel, True),
        [((toks, half), BF16), state],
        (rows, sums, gain, b_weighted, tot),
        flops=1 << 27,
    )
    local_keep, local_send = call(
        local_kernel, [((toks, half), F32)] * 2, (x_keep, x_send, mix, skip_row), flops=1 << 29
    )
    got = swap(send, 0)
    stages = range(1, bits - 2)
    early, ahead, low, *held = call(
        chip_kernel, [state, row, packed] + [state, row] * bool(stages), (keep, got, tot)
    )
    entered = ()
    for bit in stages:
        theirs = swap(low, bit)
        *entered, low, total, running = call(
            functools.partial(stage_kernel, bit, bit == 1),
            [state, row, packed, state, row],
            (*held, theirs, *entered),
        )
        held = (total, running)
    both = hop(low, (3, 0, None, 1))
    inner = hop(low, (1, 2, 3, 0))
    outer = hop(low, (2, 3, 0, 1))
    own, give = call(
        functools.partial(last_kernel, bits - 2),
        [((STATE, half), BF16)] * 2,
        (inner, outer, both, early, ahead, *entered),
    )
    other = swap(give, 0)
    (kept,) = call(
        functools.partial(finish_kernel, True),
        [((toks, half), BF16)],
        (local_keep, scale, out_c, own),
        flops=1 << 27,
    )
    (out,) = call(
        functools.partial(finish_kernel, False),
        [((toks, feat), BF16)],
        (local_send, scale, out_c, other, kept),
        flops=1 << 27,
    )
    return out


def solution(mesh):
    placed = (
        P(None, "seq", "head"),
        P(None, "seq", "head"),
        P(None, "seq", "head"),
        P("head"),
        P("seq", None),
        P("seq", None),
        P("head", "seq"),
        P("head", "seq"),
        P("head"),
    )
    return jax.shard_map(
        layer, mesh=mesh, in_specs=placed, out_specs=P("seq", "head"), check_vma=False
    )
```

```python
import functools
import math

import jax
import jax.numpy as jnp
from jax import lax
from jax.experimental import pallas as pl
from jax.experimental.pallas import tpu as pltpu
from jax.sharding import PartitionSpec as P


HEADS = 32
HDIM = 128
SDIM = 64
STATE = 128
TAIL = 8

F32 = jnp.float32
BF16 = jnp.bfloat16
VMEM = pltpu.VMEM
GRANT = 12 << 20


def dot(a, b, contract=(1, 0), precision=None):
    return lax.dot_general(
        a,
        b,
        (((contract[0],), (contract[1],)), ((), ())),
        precision=precision,
        preferred_element_type=F32,
    )


def call(kernel, outs, args, flops=1, spaces=None):
    spaces = spaces or [VMEM] * len(args)
    return pl.pallas_call(
        kernel,
        out_shape=[jax.ShapeDtypeStruct(s, d) for s, d in outs],
        in_specs=[pl.BlockSpec(memory_space=m) for m in spaces],
        out_specs=[pl.BlockSpec(memory_space=VMEM)] * len(outs),
        compiler_params=pltpu.CompilerParams(vmem_limit_bytes=GRANT),
        cost_estimate=pl.CostEstimate(flops=flops, bytes_accessed=1 << 20, transcendentals=0),
    )(*[pltpu.with_memory_space_constraint(a, m) if m == pltpu.HBM else a for a, m in zip(args, spaces)])


def gather(copies, sems):
    started = [pltpu.make_async_copy(a, b, sems.at[i]) for i, (a, b) in enumerate(copies)]
    for copy in started:
        copy.start()
    for copy in started:
        copy.wait()


def part_kernel(got_ref, keep_v_ref, k_ref, v_ref, both_ref):
    width = k_ref.shape[1]
    k_ref[...] = got_ref[:, :width]
    v_ref[...] = got_ref[:, width:]
    both_ref[:, :width] = keep_v_ref[...]
    both_ref[:, width:] = got_ref[:, width:]


def pack_kv_kernel(k_ref, v_ref, keep_k_ref, keep_v_ref, send_ref):
    width = k_ref.shape[2]
    mine = lax.axis_index("seq") % 2
    copies = [
        (k_ref.at[1 - mine], keep_k_ref),
        (k_ref.at[mine], send_ref.at[:, :width]),
        (v_ref.at[mine], send_ref.at[:, width:]),
        (v_ref.at[1 - mine], keep_v_ref),
    ]
    pl.run_scoped(functools.partial(gather, copies), pltpu.SemaphoreType.DMA((4,)))


def pack_q_kernel(q_ref, keep_ref, send_ref):
    mine = lax.axis_index("seq") % 2
    copies = [(q_ref.at[1 - mine], keep_ref), (q_ref.at[mine], send_ref)]
    pl.run_scoped(functools.partial(gather, copies), pltpu.SemaphoreType.DMA((2,)))


def prepare_kernel(*refs):
    def inner(sems, *inside):
        copies = [
            pltpu.make_async_copy(src, dst, sems.at[i])
            for i, (src, dst) in enumerate(zip(refs[:5], inside))
        ]
        for copy in copies:
            copy.start()
        for copy in copies:
            copy.wait()
        prepare(*inside, *refs[5:])

    pl.run_scoped(
        inner,
        pltpu.SemaphoreType.DMA((5,)),
        *[VMEM(r.shape, r.dtype) for r in refs[:4]],
        pltpu.SMEM(refs[4].shape, refs[4].dtype),
    )


def prepare(step_ref, log_ref, b_ref, c_ref, skip_ref, mix_ref, bw_ref, scale_ref, tot_ref, pass_ref):
    heads, toks = step_ref.shape
    half = toks // 2
    highest = lax.Precision.HIGHEST
    log = log_ref[...]
    step = step_ref[...]
    rows = lax.broadcasted_iota(jnp.int32, (toks, toks), 0)
    cols = lax.broadcasted_iota(jnp.int32, (toks, toks), 1)
    lower = (rows >= cols).astype(F32)
    cum = dot(log, lower, (1, 1), highest)
    cum_cols = dot(lower, log, (1, 1), highest)
    total = cum[:, toks - 1 :]
    weight = jnp.exp(total - cum) * step
    cross = dot(c_ref[...], b_ref[...], (1, 1))
    b_t = jnp.transpose(b_ref[...].astype(F32))
    causal = (
        lax.broadcasted_iota(jnp.int32, (half, half), 0)
        >= lax.broadcasted_iota(jnp.int32, (half, half), 1)
    )
    lanes = lax.broadcasted_iota(jnp.int32, (toks, HDIM), 1)
    for pair in range(heads // 2):
        for side in range(2):
            k = 2 * pair + side
            at = side * toks
            for r in range(2):
                for c in range(2):
                    dst = (pair, slice(r * half, (r + 1) * half), slice(at + c * half, at + (c + 1) * half))
                    if c > r:
                        mix_ref[dst] = jnp.zeros((half, half), BF16)
                        continue
                    rs, cs = slice(r * half, (r + 1) * half), slice(c * half, (c + 1) * half)
                    gap = cum_cols[rs, k : k + 1] - cum[k : k + 1, cs]
                    if r == c:
                        gap = jnp.where(causal, gap, -jnp.inf)
                    mix_ref[dst] = (jnp.exp(gap) * cross[rs, cs] * step[k : k + 1, cs]).astype(BF16)
            bw_ref[pair, :, at : at + toks] = (b_t * weight[k : k + 1, :]).astype(BF16)
        both = jnp.where(
            lanes < SDIM,
            cum_cols[:, 2 * pair : 2 * pair + 1],
            cum_cols[:, 2 * pair + 1 : 2 * pair + 2],
        )
        both = jnp.exp(both)
        scale_ref[:, pair * HDIM : (pair + 1) * HDIM] = both
        tot_ref[:, pair * HDIM : (pair + 1) * HDIM] = both[toks - 1 :, :]
        pass_ref[:, pair * HDIM : (pair + 1) * HDIM] = jnp.where(
            lanes[:1] < SDIM, skip_ref[2 * pair], skip_ref[2 * pair + 1]
        )


def pick(keep_ref, got_ref, swapped, column, got_column=None):
    keep, got = [
        ref[:, c * HDIM : (c + 1) * HDIM]
        for ref, c in ((keep_ref, column), (got_ref, column if got_column is None else got_column))
    ]
    return jnp.where(swapped, got, keep), jnp.where(swapped, keep, got)


def places():
    me = lax.axis_index("seq")
    late = me % 2 == 1
    return late, jnp.where(me < 2, me % 2 == 0, late), me != 1


def score_kernel(
    q_keep_ref, q_got_ref, keep_ref, got_ref, old_keep_ref, old_got_ref, weight_ref, scale_ref
):
    blk, feat = q_keep_ref.shape
    kv_local = keep_ref.shape[1] // HDIM
    group = feat // HDIM // kv_local
    late, old_late, has_old = places()
    rows = lax.broadcasted_iota(jnp.int32, (group * blk, blk), 0) % blk
    cols = lax.broadcasted_iota(jnp.int32, (group * blk, blk), 1)
    own_ok = cols <= rows
    far_ok = (cols > rows) & has_old
    near_ok = (cols >= 0) & has_old
    factor = math.log2(math.e) / math.sqrt(HDIM)
    for g in range(kv_local):
        keys = pick(old_keep_ref, old_got_ref, old_late, g) + pick(keep_ref, got_ref, late, g)
        heads = [pick(q_keep_ref, q_got_ref, late, g * group + i) for i in range(group)]
        for part in range(2):
            query = jnp.concatenate([h[part] for h in heads], 0)
            score = dot(query, jnp.concatenate(keys[part : part + 3], 0), (1, 1))
            near = score[:, blk : 2 * blk]
            if part == 0:
                near = jnp.where(near_ok, near, -jnp.inf)
            far = jnp.where(far_ok, score[:, :blk], -jnp.inf)
            score = jnp.concatenate([far, near, jnp.where(own_ok, score[:, 2 * blk :], -jnp.inf)], 1)
            peak = jnp.max(score, axis=1, keepdims=True)
            terms = jnp.exp2((score - peak) * factor)
            total = pl.reciprocal(jnp.sum(terms, axis=1, keepdims=True))
            weight_ref[2 * g + part] = terms.astype(BF16)
            scale_ref[2 * g + part] = jnp.broadcast_to(total, (group * blk, HDIM))


def own_value_kernel(weight_ref, keep_ref, got_ref, sum_ref):
    blk = keep_ref.shape[0]
    late = places()[0]
    for g in range(keep_ref.shape[1] // HDIM):
        vals = pick(keep_ref, got_ref, late, g)
        for part in range(2):
            values = jnp.concatenate(vals[: part + 1], 0)
            sum_ref[2 * g + part] = dot(weight_ref[2 * g + part, :, (2 - part) * blk :], values)


def value_kernel(weight_ref, scale_ref, sum_ref, old_ref, out_ref):
    blk = old_ref.shape[0]
    kv_local = old_ref.shape[1] // (2 * HDIM)
    group = out_ref.shape[1] // HDIM // kv_local
    old_late = places()[1]
    for g in range(kv_local):
        vals = pick(old_ref, old_ref, old_late, g, kv_local + g)
        for part in range(2):
            at = 2 * g + part
            result = dot(weight_ref[at, :, : (2 - part) * blk], jnp.concatenate(vals[part:], 0))
            result = ((result + sum_ref[at]) * scale_ref[at]).astype(BF16)
            for i in range(group):
                lanes = slice((g * group + i) * HDIM, (g * group + i + 1) * HDIM)
                out_ref[part * blk : (part + 1) * blk, lanes] = result[i * blk : (i + 1) * blk]


def square_kernel(rows_ref, sums_ref):
    blk = rows_ref.shape[0] // 2
    for part in range(2):
        rows = rows_ref[part * blk : (part + 1) * blk].astype(F32)
        total = jnp.sum(rows * rows, axis=1, keepdims=True)
        turned = jnp.transpose(jnp.broadcast_to(total, (blk, blk)))
        sums_ref[part * 8 : part * 8 + 8] = turned[:8]


def spread(x):
    lanes = lax.broadcasted_iota(jnp.int32, x.shape, 1)
    zero = jnp.zeros_like(x)
    return jnp.concatenate([jnp.where(lanes < SDIM, x, zero), jnp.where(lanes < SDIM, zero, x)], 0)


def pack_state(ref, state, decay, at=slice(None)):
    ref[:STATE, at] = state.astype(BF16)
    high = decay.astype(BF16).astype(F32)
    row = lax.broadcasted_iota(jnp.int32, (TAIL, decay.shape[1]), 0)
    ref[STATE:, at] = jnp.where(row == 0, high, decay - high).astype(BF16)


def unpack_state(ref):
    tail = ref[STATE:].astype(F32)
    return ref[:STATE].astype(F32), tail[:1] + tail[1:2]


def home_kernel(keeps, rows_ref, sums_ref, gain_ref, bw_ref, tot_ref, x_ref, state_ref):
    mine = lax.axis_index("seq") % 2
    side = mine if keeps else 1 - mine
    toks, half = x_ref.shape
    blk = toks // 2
    pairs = half // HDIM
    lanes = pl.ds(pl.multiple_of(side * half, half), half)
    gain = gain_ref[:, lanes]
    for part in range(2):
        at = slice(part * blk, (part + 1) * blk)
        sums = sums_ref[part * 8 : part * 8 + 1]
        mean = jnp.transpose(jnp.broadcast_to(sums, (HDIM, blk))) / (HEADS * HDIM)
        inv = lax.rsqrt(mean + 1e-06)
        rows = rows_ref[at, lanes].astype(F32) * gain
        for p in range(pairs):
            tile = slice(p * HDIM, (p + 1) * HDIM)
            x_ref[at, tile] = (rows[:, tile] * inv).astype(BF16)
    for p in range(pairs):
        at = slice(p * HDIM, (p + 1) * HDIM)
        state = dot(bw_ref[side * pairs + p], spread(x_ref[:, at]))
        if keeps:
            state_ref[:, at] = state
        else:
            decay = tot_ref[:, pl.ds(pl.multiple_of(side * half + p * HDIM, HDIM), HDIM)]
            pack_state(state_ref, state, decay, at)


def local_kernel(x_keep_ref, x_send_ref, mix_ref, skip_ref, keep_ref, send_ref):
    mine = lax.axis_index("seq") % 2
    half = x_keep_ref.shape[1]
    pairs = half // HDIM
    for x_ref, out_ref, side in ((x_keep_ref, keep_ref, mine), (x_send_ref, send_ref, 1 - mine)):
        skip = skip_ref[:, pl.ds(pl.multiple_of(side * half, half), half)]
        for p in range(pairs):
            at = slice(p * HDIM, (p + 1) * HDIM)
            x = x_ref[:, at]
            out_ref[:, at] = dot(mix_ref[side * pairs + p], spread(x)) + skip[:, at] * x.astype(F32)


def finish_kernel(keeps, local_ref, scale_ref, c_ref, enter_ref, *refs):
    mine = lax.axis_index("seq") % 2
    half = local_ref.shape[1]
    side = mine if keeps else 1 - mine
    lanes = pl.ds(pl.multiple_of(side * half, half), half)
    out = local_ref[...] + dot(c_ref[...], enter_ref[...]) * scale_ref[:, lanes]
    if keeps:
        refs[0][...] = out.astype(BF16)
    else:
        own_ref, out_ref = refs
        out_ref[:, lanes] = out.astype(BF16)
        out_ref[:, pl.ds(pl.multiple_of(mine * half, half), half)] = own_ref[...]


def add_kernel(a_ref, b_ref, out_ref):
    out_ref[...] = a_ref[...] + b_ref[...]


def half_of(ref, side):
    half = ref.shape[1] // 2
    return ref[:, pl.ds(pl.multiple_of(side * half, half), half)]


def chip_kernel(keep_ref, got_ref, tot_ref, early_ref, ahead_ref, low_ref, plain_ref, *refs):
    mine = lax.axis_index("seq") % 2
    late = mine == 1
    keep, here = keep_ref[...], half_of(tot_ref, mine)
    got, there = unpack_state(got_ref)
    early = jnp.where(late, got, keep)
    total = jnp.where(late, here, there) * early + jnp.where(late, keep, got)
    early_ref[...] = early
    ahead_ref[...] = jnp.where(late, there, here)
    pack_state(low_ref, total, here * there)
    plain_ref[...] = total.astype(BF16)
    if refs:
        refs[0][...] = total
        refs[1][...] = here * there


def stage_kernel(bit, first, total_ref, mine_ref, theirs_ref, *refs):
    upper = (lax.axis_index("seq") >> bit) % 2 == 1
    enter_ref, carried_ref, low_ref, plain_ref, next_ref, running_ref = refs[-6:]
    theirs, decay = unpack_state(theirs_ref)
    total, mine = total_ref[...], mine_ref[...]
    if first:
        enter_ref[...] = jnp.where(upper, theirs, 0.0)
        carried_ref[...] = jnp.where(upper, decay, 1.0)
    else:
        carried = refs[1][...]
        enter_ref[...] = refs[0][...] + jnp.where(upper, carried * theirs, 0.0)
        carried_ref[...] = jnp.where(upper, carried * decay, carried)
    total = jnp.where(upper, mine * theirs + total, decay * total + theirs)
    pack_state(low_ref, total, mine * decay)
    plain_ref[...] = total.astype(BF16)
    next_ref[...] = total
    running_ref[...] = mine * decay


def last_kernel(shift, inner_ref, outer_ref, both_ref, early_ref, ahead_ref, *refs):
    own_ref, give_ref = refs[-2:]
    me = lax.axis_index("seq")
    quarter, late = me >> shift, me % 2 == 1
    beside, by_inner = unpack_state(inner_ref)
    across, by_outer = unpack_state(outer_ref)
    diagonal = both_ref[...].astype(F32)
    third, fourth = quarter == 2, quarter == 3
    one, zero = jnp.ones_like(by_inner), jnp.zeros_like(by_inner)
    enter = jnp.where(quarter > 0, one, zero) * beside
    enter = enter + jnp.where(third | fourth, by_inner, zero) * across
    enter = enter + jnp.where(fourth, by_inner * by_outer, zero) * diagonal
    if len(refs) == 4:
        enter = refs[0][...] + refs[1][...] * enter
    after = ahead_ref[...] * enter + early_ref[...]
    own_ref[...] = jnp.where(late, after, enter).astype(BF16)
    give_ref[...] = jnp.where(late, enter, after).astype(BF16)


def layer(query, keys, values, norm_gain, in_b, out_c, step, log_decay, skip):
    seq_count = lax.axis_size("seq")
    head_count = lax.axis_size("head")
    blk, feat = query.shape[1:]
    heads, toks = step.shape
    kv_width = keys.shape[2]
    pairs = heads // 2
    half = feat // 2
    every = range(seq_count)

    def swap(block, bit):
        return lax.ppermute(block, "seq", [(i, i ^ (1 << bit)) for i in every])

    width = 2 * kv_width
    half_kv = ((blk, kv_width), BF16)
    keep_k, keep_v, kv_send = call(
        pack_kv_kernel,
        [half_kv, half_kv, ((blk, width), BF16)],
        (keys, values),
        spaces=[pltpu.HBM] * 2,
    )
    q_keep, q_send = call(pack_q_kernel, [((blk, feat), BF16)] * 2, (query,), spaces=[pltpu.HBM])
    chips = seq_count // 2
    onward = [(i, i + 2) for i in range(seq_count - 2)] + [(seq_count - 2, 1), (seq_count - 1, 0)]
    kv_got = swap(kv_send, 0)
    old_keep = lax.ppermute(keep_k, "seq", onward)
    got_k, got_v, both_v = call(
        part_kernel, [half_kv, half_kv, ((blk, width), BF16)], (kv_got, keep_v)
    )
    old_k = lax.ppermute(got_k, "seq", onward)
    old_v = lax.ppermute(both_v, "seq", onward)
    q_got = swap(q_send, 0)

    mix, b_weighted, scale, tot, skip_row = call(
        prepare_kernel,
        [
            ((pairs, toks, 2 * toks), BF16),
            ((pairs, STATE, 2 * toks), BF16),
            ((toks, feat), F32),
            ((1, feat), F32),
            ((1, feat), F32),
        ],
        (step, log_decay, in_b, out_c, skip),
        flops=1 << 30,
        spaces=[pltpu.HBM] * 5,
    )
    bits = seq_count.bit_length() - 1
    rows_at_once = feat // kv_width * blk
    weights, scales = call(
        score_kernel,
        [((2 * kv_width // HDIM, rows_at_once, 3 * blk), BF16), ((2 * kv_width // HDIM, rows_at_once, HDIM), F32)],
        (q_keep, q_got, keep_k, got_k, old_keep, old_k),
        flops=1 << 28,
    )
    (own_sum,) = call(
        own_value_kernel,
        [((2 * kv_width // HDIM, rows_at_once, HDIM), F32)],
        (weights, keep_v, got_v),
        flops=1 << 27,
    )
    (attended,) = call(
        value_kernel, [((toks, feat), BF16)], (weights, scales, own_sum, old_v), flops=1 << 28
    )
    (sums,) = call(square_kernel, [((16, blk), F32)], (attended,), flops=1 << 22)
    to_home = [(i, i // 2 + (1 - i % 2) * chips) for i in every]
    rows = lax.ppermute(attended, "seq", to_home)
    for bit in range(head_count.bit_length() - 1):
        other = lax.ppermute(sums, "head", [(i, i ^ (1 << bit)) for i in range(head_count)])
        (sums,) = call(add_kernel, [((16, blk), F32)], (sums, other))
    sums = lax.ppermute(sums, "seq", to_home)
    quarter = 1 << (bits - 2)

    def hop(block, quarters):
        route = []
        for i in every:
            to = quarters[i // quarter]
            route.append((i, i ^ 1 if to is None else to * quarter + i % quarter))
        return lax.ppermute(block, "seq", route)

    gain = norm_gain[None, :]
    state, row, packed = ((STATE, half), F32), ((1, half), F32), ((STATE + TAIL, half), BF16)
    x_send, send = call(
        functools.partial(home_kernel, False),
        [((toks, half), BF16), packed],
        (rows, sums, gain, b_weighted, tot),
        flops=1 << 27,
    )
    x_keep, keep = call(
        functools.partial(home_kernel, True),
        [((toks, half), BF16), state],
        (rows, sums, gain, b_weighted, tot),
        flops=1 << 27,
    )
    local_keep, local_send = call(
        local_kernel, [((toks, half), F32)] * 2, (x_keep, x_send, mix, skip_row), flops=1 << 29
    )
    got = swap(send, 0)
    stages = range(1, bits - 2)
    plain_state = ((STATE, half), BF16)
    early, ahead, low, plain, *held = call(
        chip_kernel, [state, row, packed, plain_state] + [state, row] * bool(stages), (keep, got, tot)
    )
    entered = ()
    for bit in stages:
        theirs = swap(low, bit)
        *entered, low, plain, total, running = call(
            functools.partial(stage_kernel, bit, bit == 1),
            [state, row, packed, plain_state, state, row],
            (*held, theirs, *entered),
        )
        held = (total, running)
    both = hop(plain, (3, 0, None, 1))
    inner = hop(low, (1, 2, 3, 0))
    outer = hop(low, (2, 3, 0, 1))
    own, give = call(
        functools.partial(last_kernel, bits - 2),
        [((STATE, half), BF16)] * 2,
        (inner, outer, both, early, ahead, *entered),
    )
    other = swap(give, 0)
    (kept,) = call(
        functools.partial(finish_kernel, True),
        [((toks, half), BF16)],
        (local_keep, scale, out_c, own),
        flops=1 << 27,
    )
    (out,) = call(
        functools.partial(finish_kernel, False),
        [((toks, feat), BF16)],
        (local_send, scale, out_c, other, kept),
        flops=1 << 27,
    )
    return out


def solution(mesh):
    placed = (
        P(None, "seq", "head"),
        P(None, "seq", "head"),
        P(None, "seq", "head"),
        P("head"),
        P("seq", None),
        P("seq", None),
        P("head", "seq"),
        P("head", "seq"),
        P("head"),
    )
    return jax.shard_map(
        layer, mesh=mesh, in_specs=placed, out_specs=P("seq", "head"), check_vma=False
    )
```
